32 devices in a mesh: gz: 8 (over y, x, core), gy: 4 (over z).
Axes of the slice: x: 2, y: 2, z: 4, core: 2. Of those that a mesh axis runs over, the one named last changes fastest.
Arguments:
- source: float32 [128, 256, 256], P(('gz', 'gy')), may hold values from -8 to 8
- vertical: float32 [128], P(('gz', 'gy')), may hold values from 1 to 64
- reaction: float32 [128, 256, 256], P(('gz', 'gy')), may hold values from 0.05 to 2
Outputs:
- solution: float32 [128, 256, 256], P(('gz', 'gy'))
- norms: float32 [2], replicated
The draws below stay inside these ranges and needn't reach their ends.
All inputs are finite; a program needn't handle non-finite values.
Results may differ from the reference program's by a relative error of at most 0.0001.
Values sent between devices are 32-bit elements; how exact they have to be, the bound alone decides.
A program may use at most 192 MiB of HBM per device.

```python
import math
import jax
import jax.numpy as jnp

NX = 256
LEVELS = 5
SWITCH = 2
CYCLES = 2
SWEEPS = 2
COARSE = 4
NZ = 128


def draw_source(key, part):
    rough = jax.random.truncated_normal(key, -6.0, 6.0, (NZ, NX, NX), jnp.float32)
    return rough


def levels(key, dims, pieces, least, high):
    def one(position, parts):
        steps = jax.random.uniform(jax.random.fold_in(jax.random.fold_in(key, 6), position), (parts,), jnp.float32, least / len(pieces), high / len(pieces))
        return jnp.repeat(jnp.exp(steps), dims[position] // parts).reshape((-1,) + (1,) * (len(dims) - position - 1))

    level = one(*pieces[0])
    for cut in pieces[1:]:
        level = level * one(*cut)
    return level


def setup_inputs(seed: int = 0) -> dict:
    splits = jax.random.split(jax.random.key(seed), 4)
    return {
        "source": draw_source(jax.random.fold_in(splits[3], 71), 0),
        "vertical": jnp.clip(jnp.exp(math.log(64.0) - 4.158883 * jax.random.uniform(splits[1], (NZ,), jnp.float32) ** levels(splits[1], (NZ,), ((0, 32),), -0.2, 0.2)), 1.0, 64.0),
        "reaction": jnp.clip(jnp.exp(math.log(2.0) - 3.6888794 * jax.random.uniform(splits[2], (NZ, NX, NX), jnp.float32) ** levels(splits[2], (NZ, NX, NX), ((0, 32),), -0.2, 0.2)), 0.05, 2.0),
    }


DAMPING = 0.8
COUPLING = 1.0


def plane_sum(values):
    padded = jnp.pad(values, ((0, 0), (1, 1), (1, 1)))
    return padded[:, 2:, 1:-1] + padded[:, :-2, 1:-1] + padded[:, 1:-1, 2:] + padded[:, 1:-1, :-2]


def plane_residual(target, padded, vertical, diagonal, weight):
    centre = padded[1:-1]
    applied = diagonal * centre - vertical * (padded[2:] + padded[:-2]) - weight * plane_sum(centre)
    return target - applied


def around_sum(padded):
    return padded[2:, 1:-1] + padded[:-2, 1:-1] + padded[1:-1, 2:] + padded[1:-1, :-2]


def line_sum(values):
    return around_sum(jnp.pad(values, ((1, 1), (1, 1), (0, 0))))


def shift_left(values, filler):
    return jnp.concatenate([values[..., 1:], jnp.full_like(values[..., :1], filler)], axis=-1)


def shift_right(values, filler):
    return jnp.concatenate([jnp.full_like(values[..., :1], filler), values[..., :-1]], axis=-1)


def odd_even(lower, middle, upper, right):
    length = middle.shape[-1]
    if length == 1:
        return right / middle
    if length % 2 == 1:
        widths = [(0, 0)] * (middle.ndim - 1) + [(0, 1)]
        solved = odd_even(jnp.pad(lower, widths), jnp.pad(middle, widths, constant_values=1.0),
                          jnp.pad(upper, widths), jnp.pad(right, widths))
        return solved[..., :length]
    even_lower = lower[..., 0::2]
    even_middle = middle[..., 0::2]
    even_upper = upper[..., 0::2]
    even_right = right[..., 0::2]
    odd_lower = lower[..., 1::2]
    odd_middle = middle[..., 1::2]
    odd_upper = upper[..., 1::2]
    odd_right = right[..., 1::2]
    next_lower = shift_left(even_lower, 0.0)
    next_middle = shift_left(even_middle, 1.0)
    next_upper = shift_left(even_upper, 0.0)
    next_right = shift_left(even_right, 0.0)
    factor_left = -odd_lower / even_middle
    factor_right = -odd_upper / next_middle
    reduced = odd_even(factor_left * even_lower,
                       odd_middle + factor_left * even_upper + factor_right * next_lower,
                       factor_right * next_upper,
                       odd_right + factor_left * even_right + factor_right * next_right)
    before = shift_right(reduced, 0.0)
    evens = (even_right - even_lower * before - even_upper * reduced) / even_middle
    return jnp.stack([evens, reduced], axis=-1).reshape(middle.shape)


def line_relax(target, around, vertical, diagonal, weight):
    right = target + weight * around
    coupled = jnp.broadcast_to(-vertical, diagonal.shape)
    edge = jnp.zeros_like(coupled[..., :1])
    lower = jnp.concatenate([edge, coupled[..., 1:]], axis=-1)
    upper = jnp.concatenate([coupled[..., :-1], edge], axis=-1)
    return odd_even(lower, diagonal, upper, right)


def line_residual(target, values, around, vertical, diagonal, weight):
    padded = jnp.pad(values, ((0, 0), (0, 0), (1, 1)))
    applied = diagonal * values - vertical * (padded[..., 2:] + padded[..., :-2]) - weight * around
    return target - applied


def shrink_planes(values):
    depth, row_count, column_count = values.shape
    return values.reshape(depth, row_count // 2, 2, column_count // 2, 2).sum(axis=(2, 4)) * 0.25


def grow_planes(values):
    depth, row_count, column_count = values.shape
    spread = jnp.broadcast_to(values[:, :, None, :, None], (depth, row_count, 2, column_count, 2))
    return spread.reshape(depth, 2 * row_count, 2 * column_count)


def shrink_lines(values):
    row_count, column_count, depth = values.shape
    return values.reshape(row_count // 2, 2, column_count // 2, 2, depth).sum(axis=(1, 3)) * 0.25


def grow_lines(values):
    row_count, column_count, depth = values.shape
    spread = jnp.broadcast_to(values[:, None, :, None, :], (row_count, 2, column_count, 2, depth))
    return spread.reshape(2 * row_count, 2 * column_count, depth)


def pad_planes(values):
    return jnp.pad(values, ((1, 1), (0, 0), (0, 0)))


def reference(source, vertical, reaction):
    vertical_col = vertical.reshape(-1, 1, 1)
    reactions = [reaction]
    for height in range(1, LEVELS):
        if height < SWITCH:
            reactions.append(shrink_planes(reactions[-1]))
        elif height == SWITCH:
            reactions.append(jnp.transpose(shrink_planes(reactions[-1]), (1, 2, 0)))
        else:
            reactions.append(shrink_lines(reactions[-1]))
    weights = [COUPLING / 4.0 ** height for height in range(LEVELS)]
    diagonals = []
    for height in range(LEVELS):
        coefficient = vertical_col if height < SWITCH else vertical
        diagonals.append(2.0 * coefficient + 4.0 * weights[height] + reactions[height])

    def descend(height, values, target):
        weight = weights[height]
        diagonal = diagonals[height]
        if height < SWITCH:
            def sweep_plane(values):
                residual = plane_residual(target, pad_planes(values), vertical_col, diagonal, weight)
                return values + DAMPING * residual / diagonal

            for repeat in range(SWEEPS):
                values = sweep_plane(values)
            residual = plane_residual(target, pad_planes(values), vertical_col, diagonal, weight)
            coarse = shrink_planes(residual)
            if height + 1 == SWITCH:
                coarse = jnp.transpose(coarse, (1, 2, 0))
                correction = descend(height + 1, jnp.zeros_like(coarse), coarse)
                correction = jnp.transpose(correction, (2, 0, 1))
            else:
                correction = descend(height + 1, jnp.zeros_like(coarse), coarse)
            values = values + grow_planes(correction)
            for repeat in range(SWEEPS):
                values = sweep_plane(values)
            return values

        def relax_line(values):
            return line_relax(target, line_sum(values), vertical, diagonal, weight)

        if height == LEVELS - 1:
            for repeat in range(COARSE):
                values = relax_line(values)
            return values
        for repeat in range(SWEEPS):
            values = relax_line(values)
        residual = line_residual(target, values, line_sum(values), vertical, diagonal, weight)
        coarse = shrink_lines(residual)
        correction = descend(height + 1, jnp.zeros_like(coarse), coarse)
        values = values + grow_lines(correction)
        for repeat in range(SWEEPS):
            values = relax_line(values)
        return values

    solution = jnp.zeros_like(source)
    scores = []
    for cycle_index in range(CYCLES):
        solution = descend(0, solution, source)
        residual = plane_residual(source, pad_planes(solution), vertical_col, diagonals[0], weights[0])
        scores.append(jnp.mean(residual * residual))
    return solution, jnp.stack(scores)
```

```python
import functools

import jax
import jax.numpy as jnp
import numpy as np
from jax import lax
from jax.experimental import pallas as pl
from jax.experimental.pallas import tpu as pltpu
from jax.sharding import PartitionSpec as P

LEVELS = 5
SWITCH = 2
CYCLES = 2
SWEEPS = 2
COARSE = 4
DAMPING = 0.8
COUPLING = 1.0
CHUNK = 32
MESH = pl.DeviceIdType.MESH


def dot(a, b):
    return lax.dot_general(
        a,
        b,
        (((1,), (0,)), ((), ())),
        precision=lax.Precision.HIGHEST,
        preferred_element_type=jnp.float32,
    )


def parts_of(x):
    first = x.astype(jnp.bfloat16)
    rest = x - first.astype(jnp.float32)
    second = rest.astype(jnp.bfloat16)
    third = (rest - second.astype(jnp.float32)).astype(jnp.bfloat16)
    return (third, second, first)


def dot_right(x, m):
    m = m.astype(jnp.bfloat16)
    total = None
    for x in parts_of(x):
        term = jnp.dot(x, m, preferred_element_type=jnp.float32)
        total = term if total is None else total + term
    return total


def dot_left(m, x):
    m = m.astype(jnp.bfloat16)
    total = None
    for x in parts_of(x):
        term = jnp.dot(m, x, preferred_element_type=jnp.float32)
        total = term if total is None else total + term
    return total


def kernel(
    dims,
    source, reaction, vert_s, vert_b, down0, downt0, down1, cols, mask, group, ups, groupt, colst,
    out, norms,
    v0, v1, w0, d1, w1, g1, r1, tmp0, res1, corr1, send_a, recv_a, send_v, recv_v, recv_b,
    send_n, recv_n, lines, diag, factor, target, around, halo, rowbuf, acc,
    plane_send, plane_recv, line_send, line_recv, a2a_send, a2a_recv,
):
    gz, gy, depth, cp = dims
    nd = gz * gy
    zall = nd * depth
    n0 = source.shape[1]
    n1 = n0 // 2
    a_me = lax.axis_index("gz")
    b_me = lax.axis_index("gy")
    me = a_me * gy + b_me
    h = [COUPLING / 4.0**k for k in range(LEVELS)]

    @pl.when(me == 0)
    def _():
        for p in range(2):
            v0[p, 0] = jnp.zeros((n0, n0), jnp.float32)
            v1[p, 0] = jnp.zeros((n1, n1), jnp.float32)

    @pl.when(me == nd - 1)
    def _():
        for p in range(2):
            v0[p, depth + 1] = jnp.zeros((n0, n0), jnp.float32)
            v1[p, depth + 1] = jnp.zeros((n1, n1), jnp.float32)

    edges = [a_me == 0, a_me == gz - 1, b_me == 0, b_me == gy - 1]
    for k in range(4):
        @pl.when(edges[k])
        def _(k=k):
            for p in range(2):
                halo[p, k] = jnp.zeros((zall, cp), jnp.float32)

    def flat(d):
        return (d // gy, d % gy)

    def plane_copy(v, p, level, up):
        if up:
            src, dst, to = v.at[p, depth], v.at[p, 0], flat(me + 1)
        else:
            src, dst, to = v.at[p, 1], v.at[p, depth + 1], flat(me + nd - 1 - nd * ((me + nd - 1) // nd))
        if up:
            to = flat((me + 1) % nd)
        k = 0 if up else 1
        return pltpu.make_async_remote_copy(
            src_ref=src, dst_ref=dst,
            send_sem=plane_send.at[level, p, k], recv_sem=plane_recv.at[level, p, k],
            device_id=to, device_id_type=MESH,
        )

    def plane_start(v, p, level):
        @pl.when(me < nd - 1)
        def _():
            plane_copy(v, p, level, True).start()

        @pl.when(me > 0)
        def _():
            plane_copy(v, p, level, False).start()

    def plane_wait(v, p, level):
        @pl.when(me < nd - 1)
        def _():
            plane_copy(v, p, level, True).wait_send()
            plane_copy(v, p, level, False).wait_recv()

        @pl.when(me > 0)
        def _():
            plane_copy(v, p, level, False).wait_send()
            plane_copy(v, p, level, True).wait_recv()

    def residual_chunk(v, p, z, r, n, target_ref, diag_of, weight):
        centre = v[p, z, pl.ds(r, CHUNK), :]
        rows = lax.broadcasted_iota(jnp.int32, (CHUNK, n), 0)
        lanes = lax.broadcasted_iota(jnp.int32, (CHUNK, n), 1)
        if r == 0:
            above = jnp.where(rows == 0, 0.0, pltpu.roll(centre, 1, 0))
        else:
            above = v[p, z, pl.ds(r - 1, CHUNK), :]
        if r + CHUNK == n:
            below = jnp.where(rows == CHUNK - 1, 0.0, pltpu.roll(centre, CHUNK - 1, 0))
        else:
            below = v[p, z, pl.ds(r + 1, CHUNK), :]
        left = jnp.where(lanes == 0, 0.0, pltpu.roll(centre, 1, 1))
        right = jnp.where(lanes == n - 1, 0.0, pltpu.roll(centre, n - 1, 1))
        vert = vert_s[z - 1]
        applied = (
            diag_of(z - 1, r, vert) * centre
            - vert * (v[p, z - 1, pl.ds(r, CHUNK), :] + v[p, z + 1, pl.ds(r, CHUNK), :])
            - weight * (above + below + left + right)
        )
        return centre, target_ref[z - 1, pl.ds(r, CHUNK), :] - applied

    def diag0(z, r, vert):
        return 2.0 * vert + 4.0 * h[0] + reaction[z, pl.ds(r, CHUNK), :]

    def diag1(z, r, vert):
        return d1[z, pl.ds(r, CHUNK), :]

    def over_planes(v, p, level, body):
        plane_start(v, p, level)

        def inner(z, c):
            body(z)
            return c

        lax.fori_loop(2, depth, inner, 0)
        plane_wait(v, p, level)

        def outer(i, c):
            body(1 + i * (depth - 1))
            return c

        lax.fori_loop(0, 2, outer, 0)

    def level_parts(level):
        if level == 0:
            return v0, source, diag0, w0, n0
        return v1, g1, diag1, w1, n1

    def sweep(level, p, record=None):
        v, tgt, dg, w, n = level_parts(level)

        def body(z):
            for r in range(0, n, CHUNK):
                centre, res = residual_chunk(v, p, z, r, n, tgt, dg, h[level])
                v[1 - p, z, pl.ds(r, CHUNK), :] = centre + w[z - 1, pl.ds(r, CHUNK), :] * res
                if record is not None:
                    sq = (res * res).reshape(CHUNK // 8, 8, n).sum(axis=0)
                    acc[record, :, :] += sq

        over_planes(v, p, level, body)
        return 1 - p

    def first_sweep(level):
        v, tgt, dg, w, n = level_parts(level)

        def body(z, c):
            v[0, z + 1] = w[z] * tgt[z]
            return c

        lax.fori_loop(0, depth, body, 0)
        return 0

    def restrict0(read_chunk, store):
        def body(z):
            for r in range(0, n0, CHUNK):
                tmp0[pl.ds(r, CHUNK), :] = dot_right(read_chunk(z, r), downt0[...])
            store(z, dot_left(down0[...], tmp0[...]))
        return body

    def restrict1(z, plane):
        half = dot(down1[...], plane)
        for b in range(gy):
            spread = dot(half, cols[b]) * mask[...]
            packed = dot(group[...], spread)
            for a in range(gz):
                send_a[b, a, z : z + 1, :] = packed[a : a + 1, :]

    def exchange_all(kind, src_of, recv):
        def copy(k):
            dst = (me + k) % nd
            a, b = dst // gy, dst % gy
            return pltpu.make_async_remote_copy(
                src_ref=src_of(a, b), dst_ref=recv.at[b_me, a_me],
                send_sem=a2a_send.at[kind, k], recv_sem=a2a_recv.at[kind, me],
                device_id=(a, b), device_id_type=MESH,
            )

        def start(k, c):
            copy(k).start()
            return c

        def finish(k, c):
            copy(k).wait_send()
            src = (me + k) % nd
            a, b = src // gy, src % gy
            pltpu.make_async_remote_copy(
                src_ref=recv.at[b, a], dst_ref=recv.at[b, a],
                send_sem=a2a_send.at[kind, k], recv_sem=a2a_recv.at[kind, src],
                device_id=(a, b), device_id_type=MESH,
            ).wait_recv()
            return c

        def begin():
            lax.fori_loop(1, nd, start, 0)

        def end():
            lax.fori_loop(1, nd, finish, 0)

        return begin, end

    def to_lines(recv, dest):
        for a in range(gz):
            for b in range(gy):
                s = (a * gy + b) * depth
                dest[s : s + depth, :] = recv[b, a]

    bx2, by2 = (n1 // 2 // gz, n1 // 2 // gy)
    steps = []
    s = 1
    while s < zall:
        steps.append(s)
        s *= 2
    ns = len(steps)

    def setup_lines(offset):
        rows = lax.broadcasted_iota(jnp.int32, (zall, cp), 0)
        vert = lines[...]
        a = jnp.where(rows == 0, 0.0, -vert)
        c = jnp.where(rows == zall - 1, 0.0, -vert)
        b = diag[offset]
        for k, s in enumerate(steps):
            alpha = -a / pltpu.roll(b, s, 0)
            gamma = -c / pltpu.roll(b, zall - s, 0)
            b = b + alpha * pltpu.roll(c, s, 0) + gamma * pltpu.roll(a, zall - s, 0)
            a = alpha * pltpu.roll(a, s, 0)
            c = gamma * pltpu.roll(c, zall - s, 0)
            factor[offset, 2 * k] = alpha
            factor[offset, 2 * k + 1] = gamma
        factor[offset, 2 * ns] = 1.0 / b

    def solve(offset, right):
        for k, s in enumerate(steps):
            right = (
                right
                + factor[offset, 2 * k] * pltpu.roll(right, s, 0)
                + factor[offset, 2 * k + 1] * pltpu.roll(right, zall - s, 0)
            )
        return right * factor[offset, 2 * ns]

    count = [0]
    def line_copy(p, k):
        if k == 0:
            to, slot = ((a_me + gz - 1) % gz, b_me), 1
        elif k == 1:
            to, slot = ((a_me + 1) % gz, b_me), 0
        elif k == 2:
            to, slot = (a_me, (b_me + gy - 1) % gy), 3
        else:
            to, slot = (a_me, (b_me + 1) % gy), 2
        return pltpu.make_async_remote_copy(
            src_ref=around.at[p], dst_ref=halo.at[p, slot],
            send_sem=line_send.at[p, k], recv_sem=line_recv.at[p, slot],
            device_id=to, device_id_type=MESH,
        )

    def line_landed(p, k):
        return pltpu.make_async_remote_copy(
            src_ref=around.at[p], dst_ref=halo.at[p, k],
            send_sem=line_send.at[p, k], recv_sem=line_recv.at[p, k],
            device_id=(a_me, b_me), device_id_type=MESH,
        )

    def neighbours(offset, values):
        bx, by = bx2 >> offset, by2 >> offset
        cells = bx * by
        p = count[0] % 2
        count[0] += 1
        around[p] = values
        for k in range(4):
            @pl.when(jnp.logical_not(edges[k]))
            def _(k=k):
                line_copy(p, k).start()
        for k in range(4):
            @pl.when(jnp.logical_not(edges[k]))
            def _(k=k):
                line_copy(p, k).wait_send()
                line_landed(p, k).wait_recv()
        lane = lax.broadcasted_iota(jnp.int32, (zall, cp), 1)

        def roll(x, amount):
            amount = amount % cp
            return x if amount == 0 else pltpu.roll(x, amount, 1)

        total = jnp.where(lane < by, roll(halo[p, 0], by - cells), roll(values, by))
        total += jnp.where(lane >= cells - by, roll(halo[p, 1], cells - by), roll(values, -by))
        inrow = lane & (by - 1)
        total += jnp.where(inrow == 0, roll(halo[p, 2], 1 - by), roll(values, 1))
        total += jnp.where(inrow == by - 1, roll(halo[p, 3], by - 1), roll(values, -1))
        return total

    def line_descend(offset):
        weight = h[SWITCH + offset]
        values = solve(offset, target[offset])
        repeats = COARSE if offset == LEVELS - 1 - SWITCH else SWEEPS
        for _ in range(1, repeats):
            values = solve(offset, target[offset] + weight * neighbours(offset, values))
        if offset == LEVELS - 1 - SWITCH:
            return values
        near = neighbours(offset, values)
        rows = lax.broadcasted_iota(jnp.int32, (zall, cp), 0)
        before = jnp.where(rows == 0, 0.0, pltpu.roll(values, 1, 0))
        after = jnp.where(rows == zall - 1, 0.0, pltpu.roll(values, zall - 1, 0))
        res = target[offset] - (
            diag[offset] * values - lines[...] * (before + after) - weight * near
        )
        target[offset + 1] = dot(res, ups[2 * offset])
        tmp = values
        lower = line_descend(offset + 1)
        values = tmp + dot(lower, ups[2 * offset + 1])
        for _ in range(SWEEPS):
            values = solve(offset, target[offset] + weight * neighbours(offset, values))
        return values

    def fill0(z, c):
        w0[z] = DAMPING / (2.0 * vert_s[z] + 4.0 * h[0] + reaction[z])
        return c

    lax.fori_loop(0, depth, fill0, 0)

    def keep_r1(z, value):
        r1[z] = value
        dv = 2.0 * vert_s[z] + 4.0 * h[1] + value
        d1[z] = dv
        w1[z] = DAMPING / dv

    body = restrict0(lambda z, r: reaction[z, pl.ds(r, CHUNK), :], keep_r1)
    lax.fori_loop(0, depth, lambda z, c: (body(z), c)[1], 0)
    for z in range(depth):
        restrict1(z, r1[z])
    send_v[...] = send_a[...]
    begin_v, end_v = exchange_all(0, lambda a, b: vert_b, recv_v)
    begin_r, end_r = exchange_all(1, lambda a, b: send_v.at[b, a], recv_a)
    begin_v()
    begin_r()
    recv_v[b_me, a_me] = vert_b[...]
    recv_a[b_me, a_me] = send_v[b_me, a_me]
    acc[...] = jnp.zeros_like(acc)

    begin_a, end_a = exchange_all(2, lambda a, b: send_a.at[b, a], recv_b.at[0])
    begin_b, end_b = exchange_all(3, lambda a, b: send_n.at[b, a], recv_b.at[1])

    p0 = first_sweep(0)
    for cycle in range(CYCLES):
        for k in range(SWEEPS):
            if cycle == 0 and k == 0:
                continue
            p0 = sweep(0, p0, record=cycle - 1 if cycle > 0 and k == 0 else None)

        def read0(z, r, p0=p0):
            return residual_chunk(v0, p0, z, r, n0, source, diag0, h[0])[1]

        def keep_g1(z, value):
            g1[z - 1] = value

        over_planes(v0, p0, 0, restrict0(read0, keep_g1))
        p1 = first_sweep(1)
        for k in range(1, SWEEPS):
            p1 = sweep(1, p1)

        def keep_res(z, p1=p1):
            for r in range(0, n1, CHUNK):
                res1[z - 1, pl.ds(r, CHUNK), :] = residual_chunk(
                    v1, p1, z, r, n1, g1, diag1, h[1]
                )[1]

        over_planes(v1, p1, 1, keep_res)
        for z in range(depth):
            restrict1(z, res1[z])
        begin_a()
        recv_b[0, b_me, a_me] = send_a[b_me, a_me]
        if cycle == 0:
            end_v()
            end_r()
            to_lines(recv_v, lines)
            to_lines(recv_a, target.at[0])
            coarse = target[0]
            for offset in range(LEVELS - SWITCH):
                if offset > 0:
                    coarse = dot(coarse, ups[2 * offset - 2])
                diag[offset] = 2.0 * lines[...] + 4.0 * h[SWITCH + offset] + coarse
            for offset in range(LEVELS - SWITCH):
                setup_lines(offset)
        end_a()
        to_lines(recv_b.at[0], target.at[0])
        rowbuf[...] = line_descend(0)
        for a in range(gz):
            for b in range(gy):
                s = (a * gy + b) * depth
                send_n[b, a] = rowbuf[s : s + depth, :]
        begin_b()
        recv_b[1, b_me, a_me] = send_n[b_me, a_me]
        end_b()
        for z in range(depth):
            wide = None
            for b in range(gy):
                for a in range(gz):
                    corr1[a : a + 1, :] = recv_b[1, b, a, z : z + 1, :]
                part = dot(dot(groupt[...], corr1[...]) * mask[...], colst[b])
                wide = part if wide is None else wide + part
            v1[1 - p1, z + 1] = v1[p1, z + 1] + dot(down1[...].T * 2.0, wide)
        p1 = 1 - p1
        for _ in range(SWEEPS):
            p1 = sweep(1, p1)

        def correct0(z, c, p0=p0, p1=p1):
            tmp0[...] = dot_left(downt0[...] * 2.0, v1[p1, z])
            for r in range(0, n0, CHUNK):
                v0[1 - p0, z, pl.ds(r, CHUNK), :] = v0[p0, z, pl.ds(r, CHUNK), :] + dot_right(
                    tmp0[pl.ds(r, CHUNK), :], down0[...] * 2.0
                )
            return c

        lax.fori_loop(1, depth + 1, correct0, 0)
        p0 = 1 - p0
        for _ in range(SWEEPS):
            p0 = sweep(0, p0)

    def last(z, p0=p0):
        for r in range(0, n0, CHUNK):
            centre, res = residual_chunk(v0, p0, z, r, n0, source, diag0, h[0])
            out[z - 1, pl.ds(r, CHUNK), :] = centre
            acc[CYCLES - 1, :, :] += (res * res).reshape(CHUNK // 8, 8, n0).sum(axis=0)

    over_planes(v0, p0, 0, last)
    ridx = lax.broadcasted_iota(jnp.int32, (8, 128), 0)
    part = jnp.zeros((8, 128), jnp.float32)
    for k in range(CYCLES):
        part = jnp.where(ridx == k, jnp.sum(acc[k]), part)
    rowbuf_n = tmp_n = send_n
    target_n = recv_n
    w_n = acc
    acc[0, :, 0:128] = part
    begin_n, end_n = exchange_all(4, lambda a, b: acc.at[0, :, pl.ds(0, 128)], recv_n)
    begin_n()
    recv_n[b_me, a_me] = part
    end_n()
    total = jnp.zeros((8, 128), jnp.float32)
    for a in range(gz):
        for b in range(gy):
            total = total + recv_n[b, a]
    norms[...] = total * (1.0 / (zall * n0 * n0))


def pair_matrix(n, value):
    return (np.arange(n)[None, :] // 2 == np.arange(n // 2)[:, None]).astype(np.float32) * value


def shards(gz, gy, source, vertical, reaction):
    depth, n0 = source.shape[0], source.shape[1]
    nd = gz * gy
    zall = nd * depth
    n1, n2 = n0 // 2, n0 // 4
    bx, by = n2 // gz, n2 // gy
    cells = bx * by
    cp = -(-cells // 128) * 128
    down0 = pair_matrix(n0, 0.5)
    down1 = pair_matrix(n1, 0.5)
    lane = np.arange(cp)
    cols = np.zeros((gy, n1, cp), np.float32)
    colst = np.zeros((gy, cp, n1), np.float32)
    for b in range(gy):
        hit = (np.arange(n1)[:, None] // 2 == b * by + lane[None, :] % by) & (lane[None, :] < cells)
        cols[b] = hit * 0.5
        colst[b] = hit.T
    mask = ((lane[None, :] // by == np.arange(n2)[:, None] % bx) & (lane[None, :] < cells)).astype(np.float32)
    group = (np.arange(n2)[None, :] // bx == np.arange(gz)[:, None]).astype(np.float32)
    ups = []
    for offset in range(LEVELS - SWITCH - 1):
        fx, fy = bx >> offset, by >> offset
        cy = fy // 2
        matrix = np.zeros((cp, cp), np.float32)
        for i in range(fx):
            for j in range(fy):
                matrix[i * fy + j, (i // 2) * cy + j // 2] = 1.0
        ups += [matrix * 0.25, matrix.T]
    ups = np.stack(ups)
    steps = (zall - 1).bit_length()
    f32 = jnp.float32
    nl = LEVELS - SWITCH
    vm = pl.BlockSpec(memory_space=pltpu.VMEM)
    consts = [down0, down0.T.copy(), down1, cols, mask, group, ups, group.T.copy(), colst]
    solution, norms = pl.pallas_call(
        functools.partial(kernel, (gz, gy, depth, cp)),
        out_shape=(
            jax.ShapeDtypeStruct(source.shape, f32),
            jax.ShapeDtypeStruct((8, 128), f32),
        ),
        in_specs=[vm, vm, pl.BlockSpec(memory_space=pltpu.SMEM), vm] + [vm] * len(consts),
        out_specs=(vm, vm),
        scratch_shapes=[
            pltpu.VMEM((2, depth + 2, n0, n0), f32),
            pltpu.VMEM((2, depth + 2, n1, n1), f32),
            pltpu.VMEM((depth, n0, n0), f32),
            pltpu.VMEM((depth, n1, n1), f32),
            pltpu.VMEM((depth, n1, n1), f32),
            pltpu.VMEM((depth, n1, n1), f32),
            pltpu.VMEM((depth, n1, n1), f32),
            pltpu.VMEM((n0, n1), f32),
            pltpu.VMEM((depth, n1, n1), f32),
            pltpu.VMEM((gz, cp), f32),
            pltpu.VMEM((gy, gz, depth, cp), f32),
            pltpu.VMEM((gy, gz, depth, cp), f32),
            pltpu.VMEM((gy, gz, depth, cp), f32),
            pltpu.VMEM((gy, gz, depth, cp), f32),
            pltpu.VMEM((2, gy, gz, depth, cp), f32),
            pltpu.VMEM((gy, gz, depth, cp), f32),
            pltpu.VMEM((gy, gz, 8, 128), f32),
            pltpu.VMEM((zall, cp), f32),
            pltpu.VMEM((nl, zall, cp), f32),
            pltpu.VMEM((nl, 2 * steps + 1, zall, cp), f32),
            pltpu.VMEM((nl, zall, cp), f32),
            pltpu.VMEM((2, zall, cp), f32),
            pltpu.VMEM((2, 4, zall, cp), f32),
            pltpu.VMEM((zall, cp), f32),
            pltpu.VMEM((CYCLES, 8, n0), f32),
            pltpu.SemaphoreType.DMA((2, 2, 2)),
            pltpu.SemaphoreType.DMA((2, 2, 2)),
            pltpu.SemaphoreType.DMA((2, 4)),
            pltpu.SemaphoreType.DMA((2, 4)),
            pltpu.SemaphoreType.DMA((5, nd)),
            pltpu.SemaphoreType.DMA((5, nd)),
        ],
        compiler_params=pltpu.CompilerParams(
            has_side_effects=True, vmem_limit_bytes=64000 * 1024
        ),
    )(
        source,
        reaction,
        vertical,
        jnp.broadcast_to(vertical[:, None], (depth, cp)),
        *[jnp.asarray(c) for c in consts],
    )
    return solution, norms[:CYCLES, 0]


CROWS = 32
PAD = 8


def dot_parts(x, m, parts=2):
    total = None
    rest = x
    for k in range(parts):
        piece = rest.astype(jnp.bfloat16)
        if k + 1 < parts:
            rest = rest - piece.astype(jnp.float32)
        term = jnp.dot(piece, m, preferred_element_type=jnp.float32)
        total = term if total is None else total + term
    return total


def chain_kernel(
    dims,
    source, reaction, vertical, downy, upy, down2, up2, down3, down4, up3, up4,
    out, norms,
    v0, g0, w0, d0, v1, g1, w1, d1, raw_r, raw_s, stage, turn, lines, vsend, vrecv,
    gx, cx, dx, win3, win4, v2, v3, v4, g3, g4, diag, fac, mask, acc, nsend, nrecv,
    a2a_send, a2a_recv, x_send, x_recv, w3_send, w3_recv, w4_send, w4_recv,
):
    gz, gy, depth = dims
    nd = gz * gy
    zall = nd * depth
    n0 = source.shape[1]
    n1, n2, n3, n4 = n0 // 2, n0 // 4, n0 // 8, n0 // 16
    r0, r1 = n0 // nd, n0 // 2 // nd
    nt0 = n0 // 128
    h = [COUPLING / 4.0**k for k in range(LEVELS)]
    f32 = jnp.float32
    a_me, b_me = lax.axis_index("gz"), lax.axis_index("gy")
    me = a_me * gy + b_me
    nchip = gz // 2

    def bend(c):
        return c + c // 2 - 2 * (c // 3) if nchip == 4 else c

    def place(i):
        k, core = i // 2, i % 2
        b, q = k // nchip, k % nchip
        q = q + (b % 2) * (nchip - 1 - 2 * q)
        return (bend(q) * 2 + core, b)

    q_me = bend(a_me // 2)
    q_me = q_me + (b_me % 2) * (nchip - 1 - 2 * q_me)
    p = (b_me * nchip + q_me) * 2 + a_me % 2
    chip, par = p // 2, p % 2

    def loop(lo, hi, body):
        def step(i, c):
            body(i)
            return c
        lax.fori_loop(lo, hi, step, 0)

    def remote(src, dst, ss, rs, to):
        return pltpu.make_async_remote_copy(
            src_ref=src, dst_ref=dst, send_sem=ss, recv_sem=rs, device_id=to, device_id_type=MESH
        )

    def target(k):
        return (p + nd + (k // 2 + k % 2) * (1 - 2 * (k % 2))) % nd

    def flat(i):
        a, b = place(i)
        return a * gy + b

    def spread(kind, src_of, dst_mine, dst_from):
        def start(k):
            t = target(k)
            remote(src_of(t), dst_mine, a2a_send.at[kind, k], a2a_recv.at[kind, me], place(t)).start()

        def end_send(k):
            t = target(k)
            remote(src_of(t), dst_mine, a2a_send.at[kind, k], a2a_recv.at[kind, me], place(t)).wait_send()

        def landed(s):
            r = dst_from(s)
            remote(r, r, a2a_send.at[kind, 0], a2a_recv.at[kind, s], place(p)).wait_recv()

        return (
            lambda: loop(1, nd, start),
            lambda: loop(1, nd, end_send),
            landed,
        )

    def piece(ref, t):
        return ref.at[:, pl.ds(r0 * t, r0), :]

    def zrows(ref, s):
        return ref.at[pl.ds(depth * s, depth)]

    start_v, done_v, landed_v = spread(0, lambda t: vsend, vrecv.at[me], lambda s: vrecv.at[s])
    start_r, done_r, landed_r = spread(
        1, lambda t: piece(reaction, t), zrows(raw_r, me), lambda s: zrows(raw_r, s))
    start_s, done_s, landed_s = spread(
        2, lambda t: piece(source, t), zrows(raw_s, me), lambda s: zrows(raw_s, s))
    start_o, done_o, landed_o = spread(
        3, lambda t: zrows(stage, flat(t)), piece(out, p), lambda s: zrows(stage, s))
    start_n, done_n, landed_n = spread(4, lambda t: nsend, nrecv.at[me], lambda s: nrecv.at[s])

    for i in range(depth):
        vsend[i : i + 1, :] = jnp.full((1, 128), vertical[i], f32)
    start_v()
    start_r()
    start_s()

    first, last = p == 0, p == nd - 1

    def xchg(kind, lo_src, lo_dst, hi_src, hi_dst):
        def down():
            return remote(lo_src, hi_dst, x_send.at[kind, 0], x_recv.at[kind, 0], place((p + nd - 1) % nd))

        def up():
            return remote(hi_src, lo_dst, x_send.at[kind, 1], x_recv.at[kind, 1], place((p + 1) % nd))

        def begin():
            @pl.when(jnp.logical_not(first))
            def _():
                down().start()

            @pl.when(jnp.logical_not(last))
            def _():
                up().start()

        def end():
            @pl.when(jnp.logical_not(first))
            def _():
                down().wait_send()
                up().wait_recv()

            @pl.when(jnp.logical_not(last))
            def _():
                up().wait_send()
                down().wait_recv()

        return begin, end

    def planes0(m, dep):
        def at(lo):
            return v0.at[m, pl.ds(lo, dep), pl.ds(PAD, zall), :]
        return xchg(m, at(2), at(2 - dep), at(2 + r0 - dep), at(2 + r0))

    def planes1(ref, kind):
        return xchg(kind, ref.at[pl.ds(2, 2)], ref.at[pl.ds(0, 2)],
                    ref.at[pl.ds(r1, 2)], ref.at[pl.ds(r1 + 2, 2)])

    def planes1v(m):
        def at(lo):
            return v1.at[m, pl.ds(lo, 2), pl.ds(PAD, zall), :]
        return xchg(4, at(2), at(0), at(r1), at(r1 + 2))

    def blocks(ref, kind):
        return xchg(kind, ref.at[1], ref.at[0], ref.at[1], ref.at[2])

    def halo_d0():
        return xchg(5, d0.at[1], d0.at[0], d0.at[r0], d0.at[r0 + 1])

    offs3 = [-1, 1, -2, 2, -3, 3]

    def window3(kind):
        buf = win3.at[kind]

        def each(fn):
            for o in offs3:
                @pl.when(jnp.logical_and(p + o >= 0, p + o < nd))
                def _(o=o):
                    fn(o)

        def out_of(o):
            return remote(buf.at[3], buf.at[3 - o], w3_send.at[kind, 3 + o], w3_recv.at[kind, 3 - o],
                          place((p + o + nd) % nd))

        def begin():
            each(lambda o: out_of(o).start())

        def end():
            def fn(o):
                out_of(o).wait_send()
                remote(buf.at[3 + o], buf.at[3 + o], w3_send.at[kind, 3 + o], w3_recv.at[kind, 3 + o],
                       place(p)).wait_recv()
            each(fn)

        return begin, end

    offs4 = [(o, c) for o in (0, -1, 1, -2, 2, -3, 3, -4, 4) for c in range(2)]

    def window4(kind):
        buf = win4.at[kind]

        def each(fn):
            for o, c in offs4:
                good = par != c if o == 0 else jnp.logical_and(chip + o >= 0, chip + o < nd // 2)

                @pl.when(good)
                def _(o=o, c=c):
                    fn(o, c)

        def out_of(o, c):
            slot = 8 + par - 2 * o
            return remote(buf.at[8 + par], buf.at[slot], w4_send.at[kind, 8 + 2 * o + c],
                          w4_recv.at[kind, slot], place((2 * (chip + o) + c + nd) % nd))

        def begin():
            each(lambda o, c: out_of(o, c).start())

        def end():
            def fn(o, c):
                s = 8 + 2 * o + c
                out_of(o, c).wait_send()
                remote(buf.at[s], buf.at[s], w4_send.at[kind, s], w4_recv.at[kind, s], place(p)).wait_recv()
            each(fn)

        return begin, end

    zpad = jnp.zeros((PAD, n0), f32)
    for m in range(3):
        def zero0(x, m=m):
            v0[m, x, 0:PAD, :] = zpad
            v0[m, x, PAD + zall : 2 * PAD + zall, :] = zpad
        loop(0, r0 + 4, zero0)

        def zero1(x, m=m):
            v1[m, x, 0:PAD, :] = zpad[:, :n1]
            v1[m, x, PAD + zall : 2 * PAD + zall, :] = zpad[:, :n1]
        loop(0, r1 + 4, zero1)

    tile0 = jnp.zeros((zall, 128), f32)
    plane0 = jnp.zeros((zall, n0), f32)

    def blank(lo0, x0, lo1, b):
        for q in range(2):
            for m in (0, 2):
                v0[m, lo0 + q, PAD : PAD + zall, :] = plane0
            v1[2, lo1 + q, PAD : PAD + zall, :] = tile0
            g1[lo1 + q] = tile0
            d1[lo1 + q] = tile0
            w1[lo1 + q] = tile0
        d0[x0] = plane0
        w0[x0] = plane0
        for k in range(CYCLES):
            gx[k, b] = tile0
            cx[k, b] = tile0
        dx[b] = tile0

    @pl.when(first)
    def _():
        blank(0, 0, 0, 0)

    @pl.when(last)
    def _():
        blank(r0 + 2, r0 + 1, r1 + 2, 2)

    for k in range(CYCLES + 1):
        for o in offs3:
            @pl.when(jnp.logical_or(p + o < 0, p + o >= nd))
            def _(o=o, k=k):
                win3[k, 3 + o] = jnp.zeros((n3 * zall // 128, 128), f32)
        for o, c in offs4:
            if o:
                @pl.when(jnp.logical_or(chip + o < 0, chip + o >= nd // 2))
                def _(o=o, c=c, k=k):
                    win4[k, 8 + 2 * o + c] = jnp.zeros((n4 * zall // 128, 128), f32)
    for q in range(2):
        v2[q, 0] = tile0
        v2[q, 4] = tile0
        v3[q, 0] = tile0
        v3[q, 3] = tile0
        v4[q, 0] = tile0
        v4[q, 3] = tile0
    v4[1, 2] = tile0
    acc[...] = jnp.zeros_like(acc)

    lane = lax.broadcasted_iota(jnp.int32, (zall, 128), 1)
    rows = lax.broadcasted_iota(jnp.int32, (zall, 128), 0)

    for t in range(3):
        good = [p > 0, None, p < nd - 1][t]
        one = jnp.ones((zall, 128), f32)
        mask[t] = one if good is None else one * good.astype(f32)
    for t in range(2):
        row = p - 3 + 4 * t + lane // n3
        mask[3 + t] = jnp.where((row >= 0) & (row < nd) & (row < p + 4), 1.0, 0.0)
        row = chip - 4 + 8 * t + lane // n4
        mask[5 + t] = jnp.where((row >= 0) & (row < nd // 2) & (row < chip + 5), 1.0, 0.0)

    def pack(rep, width):
        k = 128 // width
        zb = zall // k
        part = lane[:zb]
        got = rep[0:zb]
        for j in range(1, k):
            got = jnp.where(part // width == j, rep[zb * j : zb * (j + 1)], got)
        return got

    def unpack(slots, width):
        k = 128 // width
        zb = zall // k
        part = lane[:zb] // width
        parts = []
        for j in range(k):
            got = jnp.zeros((zb, 128), f32)
            for s, x in enumerate(slots):
                turn = (width * (s - j)) % 128
                x = x if turn == 0 else pltpu.roll(x, turn, 1)
                got = jnp.where(part == s, x, got)
            parts.append(got)
        return parts

    def unpack3(kind, dest, add=None):
        for t in range(2):
            slots = [win3[kind, 4 * t + k] for k in range(4) if 4 * t + k < 7]
            zb = zall // 4
            for j, x in enumerate(unpack(slots, n3)):
                if add is not None:
                    x = x + add(j * zb, zb)
                dest[t, j * zb : (j + 1) * zb] = x

    def unpack4(kind, dest, add=None):
        for t in range(2):
            slots = [win4[kind, 2 * r] + win4[kind, 2 * r + 1] for r in range(8 * t, min(8 * t + 8, 9))]
            zb = zall // 8
            for j, x in enumerate(unpack(slots, n4)):
                if add is not None:
                    x = x + add(j * zb, zb)
                dest[t, j * zb : (j + 1) * zb] = x

    rawr = raw_r.reshape(zall * r0, n0)
    raws = raw_s.reshape(zall * r0, n0)
    staged = stage.reshape(zall * r0, n0)

    def unfold(raw, j):
        at = pl.ds(pl.multiple_of(PAD * r0 * j, PAD * r0), PAD * r0)
        for t in range(nt0):
            turn[t, at, :] = raw[at, 128 * t : 128 * (t + 1)]
    raw_r[pl.ds(depth * me, depth)] = reaction[:, pl.ds(r0 * p, r0), :]
    raw_s[pl.ds(depth * me, depth)] = source[:, pl.ds(r0 * p, r0), :]
    vrecv[me] = vsend[...]
    group = PAD // depth

    def each_rows(landed, body):
        def step(i):
            j = (me // group + i) % (zall // PAD)
            for k in range(group):
                s = group * j + k

                @pl.when(s != me)
                def _():
                    landed(s)
            body(j)
        loop(0, zall // PAD, step)

    loop(0, nd, lambda s: pl.when(s != me)(lambda: landed_v(s)))
    for s in range(nd):
        lines[depth * s : depth * (s + 1), :] = vrecv[s]

    def take_r(j):
        z = pl.multiple_of(PAD * j, PAD)
        unfold(rawr, j)
        for x in range(r0):
            for t in range(nt0):
                d0[x + 1, pl.ds(z, PAD), 128 * t : 128 * (t + 1)] = turn[
                    t, pl.ds(PAD * r0 * j + x, PAD, stride=r0), :]

    each_rows(landed_r, take_r)

    def shrink_r(i):
        for r in range(0, zall, CROWS):
            at = pl.ds(r, CROWS)
            a, b = d0[2 * i + 1, at, :], d0[2 * i + 2, at, :]
            got = dot_parts(a + b, downy[...], 3)
            vert = lines[at, :]
            base = 2.0 * vert + 4.0 * h[1]
            w1[i + 2, at, :] = got
            d = base + got
            d1[i + 2, at, :] = d
            base = jnp.concatenate([2.0 * vert + 4.0 * h[0]] * nt0, axis=1)
            for k, x in ((1, a), (2, b)):
                x = base + x
                d0[2 * i + k, at, :] = x
                w0[2 * i + k, at, :] = DAMPING / x

    loop(0, r1, shrink_r)
    begin_d0, end_d0 = halo_d0()
    begin_d0()
    begin_d1, end_d1 = planes1(d1, 6)
    begin_d1()
    rx2 = dot_parts(jnp.concatenate([w1[2] + w1[3], w1[4] + w1[5]], axis=1), down2[...], 3)
    dx[1] = rx2
    begin_dx, end_dx = blocks(dx, 7)
    begin_dx()
    rx3 = dot_parts(rx2, down3[...], 3)
    win3[CYCLES, 3] = pack(rx3, n3)
    begin_w3, end_w3 = window3(CYCLES)
    begin_w3()
    win4[CYCLES, 8 + par] = pack(dot_parts(rx3, down4[...], 3), n4)
    begin_w4, end_w4 = window4(CYCLES)
    begin_w4()
    loop(2, r1 + 2, lambda x: w1.__setitem__(x, DAMPING / d1[x]))

    def take_s(j):
        z = pl.multiple_of(PAD * j, PAD)
        unfold(raws, j)
        for x in range(r0):
            for t in range(nt0):
                cut = slice(128 * t, 128 * (t + 1))
                got = turn[t, pl.ds(PAD * r0 * j + x, PAD, stride=r0), :]
                g0[x + 1, pl.ds(z, PAD), cut] = got
                v0[0, x + 2, pl.ds(z + PAD, PAD), cut] = w0[x + 1, pl.ds(z, PAD), cut] * got

    each_rows(landed_s, take_s)

    ns = (zall - 1).bit_length()

    def factors(f):
        vert = lines[...]
        a = jnp.where(rows == 0, 0.0, -vert)
        c = jnp.where(rows == zall - 1, 0.0, -vert)
        b = diag[f]
        for k in range(ns):
            s = 1 << k
            inv = 1.0 / b
            alpha = -a * pltpu.roll(inv, s, 0)
            gamma = -c * pltpu.roll(inv, zall - s, 0)
            b = b + alpha * pltpu.roll(c, s, 0) + gamma * pltpu.roll(a, zall - s, 0)
            a = alpha * pltpu.roll(a, s, 0)
            c = gamma * pltpu.roll(c, zall - s, 0)
            fac[f, 2 * k] = alpha
            fac[f, 2 * k + 1] = gamma
        fac[f, 2 * ns] = mask[f] / b

    def solve(f, right):
        for k in range(ns):
            s = 1 << k
            right = (
                right
                + fac[f, 2 * k] * pltpu.roll(right, s, 0)
                + fac[f, 2 * k + 1] * pltpu.roll(right, zall - s, 0)
            )
        return right * fac[f, 2 * ns]

    def near(v, q, b, width):
        t = v[q, b]
        below = pltpu.roll(jnp.where(lane >= 128 - width, v[q, b - 1], t), width, 1)
        above = pltpu.roll(jnp.where(lane < width, v[q, b + 1], t), 128 - width, 1)
        inrow = lane % width
        left = jnp.where(inrow == 0, 0.0, pltpu.roll(t, 1, 1))
        right = jnp.where(inrow == width - 1, 0.0, pltpu.roll(t, 127, 1))
        return (below + above) + (left + right)

    edge = lax.broadcasted_iota(jnp.int32, (CROWS, 128), 1)
    level0 = (v0, g0, w0, d0, nt0, h[0], 1)
    level1 = (v1, g1, w1, d1, 1, h[1], 2)

    def stencil(level, m, x, r):
        v, g, w, d, nt, weight, go = level
        centre, turn_r, turn_l = [], [], []
        for t in range(nt):
            cut = slice(128 * t, 128 * (t + 1))
            c = v[m, x + 2, PAD + r : PAD + r + CROWS, cut]
            centre.append(c)
            turn_r.append(pltpu.roll(c, 1, 1))
            turn_l.append(pltpu.roll(c, 127, 1))
        vert = lines[r : r + CROWS, :]
        got = []
        for t in range(nt):
            cut = slice(128 * t, 128 * (t + 1))
            left = jnp.where(edge == 0, turn_r[t - 1] if t else 0.0, turn_r[t])
            right = jnp.where(edge == 127, turn_l[t + 1] if t + 1 < nt else 0.0, turn_l[t])
            side = (v[m, x + 1, PAD + r : PAD + r + CROWS, cut] + v[m, x + 3, PAD + r : PAD + r + CROWS, cut]) + (left + right)
            if weight != 1.0:
                side = weight * side
            ends = v[m, x + 2, PAD + r - 1 : PAD + r - 1 + CROWS, cut] + v[m, x + 2, PAD + r + 1 : PAD + r + 1 + CROWS, cut]
            got.append(g[x + go, r : r + CROWS, cut] + side + vert * ends)
        return centre, got

    def sweep_plane(level, m, q, x, record=None, put=None):
        v, g, w, d, nt, weight, go = level
        for r in range(0, zall, CROWS):
            centre, got = stencil(level, m, x, r)
            for t in range(nt):
                cut = slice(128 * t, 128 * (t + 1))
                wt = w[x + go, r : r + CROWS, cut]
                if record is None:
                    new = (1.0 - DAMPING) * centre[t] + wt * got[t]
                else:
                    res = got[t] - d[x + go, r : r + CROWS, cut] * centre[t]
                    new = centre[t] + wt * res
                    acc[record] += (res * res).reshape(CROWS // 8, 8, 128).sum(axis=0)
                v[q, x + 2, PAD + r : PAD + r + CROWS, cut] = new
                if put is not None:
                    for e in range(0, CROWS, 8):
                        put(x, r + e, t, new[e : e + 8])

    def residual(level, m, x, r):
        v, g, w, d, nt, weight, go = level
        centre, got = stencil(level, m, x, r)
        res = [
            got[t] - d[x + go, r : r + CROWS, 128 * t : 128 * (t + 1)] * centre[t] for t in range(nt)]
        return res

    def sweeps(level, m, q, xs, record=None, put=None):
        lo, hi, fn = xs
        loop(lo, hi, lambda i: sweep_plane(level, m, q, fn(i), record, put))

    def restrict0(m, lo, hi, fn):
        def body(i):
            i = fn(i)
            for r in range(0, zall, CROWS):
                a = residual(level0, m, 2 * i, r)
                b = residual(level0, m, 2 * i + 1, r)
                both = jnp.concatenate([s + t for s, t in zip(a, b)], axis=1)
                g1[i + 2, r : r + CROWS, :] = dot_parts(both, downy[...])
        loop(lo, hi, body)

    def same(i):
        return i

    def rim(size, wide):
        return lambda i: i + (i // wide) * (size - 2 * wide)

    def outer(size):
        return lambda i: -1 + i * (size + 1)

    def pair0(m, q, record=None, hook=None, put=None, restrict=False):
        begin, end = planes0(m, 2)
        begin()
        if hook is not None:
            hook[0]()
        sweeps(level0, m, 1, (1, r0 - 1, same), record)
        if restrict:
            restrict0(1, 1, r1 - 1, same)
        else:
            sweeps(level0, 1, q, (2, r0 - 2, same), None, put)
        end()
        if hook is not None:
            hook[1]()
        sweeps(level0, m, 1, (0, 2, outer(r0)))
        sweeps(level0, m, 1, (0, 2, rim(r0, 1)), record)
        if restrict:
            restrict0(1, 0, 2, lambda i: i * (r1 - 1))
        else:
            sweeps(level0, 1, q, (0, 4, rim(r0, 2)), None, put)

    def halo_factors():
        end_dx()
        for t in range(3):
            diag[t] = 2.0 * lines[...] + 4.0 * h[2] + dx[t]
        loop(0, 3, factors)

    def window_factors():
        end_w3()
        end_w4()

        def add(level):
            return lambda r, n: 2.0 * lines[r : r + n, :] + 4.0 * h[level]
        unpack3(CYCLES, diag.at[pl.ds(3, 2)], add(3))
        unpack4(CYCLES, diag.at[pl.ds(5, 2)], add(4))
        loop(3, 7, factors)

    def halo_level0():
        end_d0()
        for x, inside in ((0, jnp.logical_not(first)), (r0 + 1, jnp.logical_not(last))):
            @pl.when(inside)
            def _(x=x):
                w0[x] = DAMPING / d0[x]
            g0[x] = v0[0, x + 1, PAD : PAD + zall, :] * d0[x] * (1.0 / DAMPING)

    def halo_level1():
        end_d1()
        for x, inside in ((0, jnp.logical_not(first)), (r1 + 2, jnp.logical_not(last))):
            @pl.when(inside)
            def _(x=x):
                for q in range(2):
                    w1[x + q] = DAMPING / d1[x + q]

    def coarse(cycle):
        begin, end = planes1(g1, 3)
        begin()
        if cycle == 0:
            window_factors()
        loop(2, r1 + 2, lambda x: v1.__setitem__((0, x, pl.ds(PAD, zall)), w1[x] * g1[x]))
        end()
        if cycle == 0:
            halo_level1()
        for x in (0, 1, r1 + 2, r1 + 3):
            v1[0, x, PAD : PAD + zall] = w1[x] * g1[x]
        sweeps(level1, 0, 1, (-1, r1 + 1, same))

        pairs = []
        for i in range(r1 // 2):
            cuts = []
            for r in range(0, zall, CROWS):
                a = residual(level1, 1, 2 * i, r)[0]
                b = residual(level1, 1, 2 * i + 1, r)[0]
                cuts.append(a + b)
            pairs.append(jnp.concatenate(cuts, axis=0))
        gx[cycle, 1] = dot_parts(jnp.concatenate(pairs, axis=1), down2[...])
        e2 = lines2(cycle)

        for i in range(r1 // 2):
            e = dot_parts(e2, up2[i])
            for x in (2 * i, 2 * i + 1):
                v1[2, x + 2, PAD : PAD + zall] = v1[1, x + 2, PAD : PAD + zall] + e
        begin, end = planes1v(2)
        begin()
        sweeps(level1, 2, 1, (1, r1 - 1, same))
        end()
        sweeps(level1, 2, 1, (0, 2, outer(r1)))
        sweeps(level1, 2, 1, (0, 2, rim(r1, 1)))
        sweeps(level1, 1, 0, (0, r1, same))

    def lines_sweep(v, q, s, lo, hi, right, f, weight, width):
        loop(lo, hi, lambda b: v.__setitem__(
            (s, b), solve(f + b - 1, right[b - 1] + weight * near(v, q, b, width))))

    def line_residual(v, q, b, right, f, weight, width):
        values = v[q, b]
        before = jnp.where(rows == 0, 0.0, pltpu.roll(values, 1, 0))
        after = jnp.where(rows == zall - 1, 0.0, pltpu.roll(values, zall - 1, 0))
        return right[b - 1] + weight * near(v, q, b, width) + lines[...] * (before + after) - diag[f + b - 1] * values

    def lines2(cycle):
        right = gx.at[cycle]
        begin, end = blocks(right, 8 + cycle)
        begin()
        v2[0, 2] = solve(1, right[1])
        end()
        loop(0, 2, lambda i: v2.__setitem__((0, 1 + 2 * i), solve(2 * i, right[2 * i])))
        lines_sweep(v2, 0, 1, 1, 4, right, 0, h[2], n2)
        res = line_residual(v2, 1, 2, right, 0, h[2], n2)
        win3[cycle, 3] = pack(dot_parts(res, down3[...]), n3)
        e3 = lines3(cycle)
        cx[cycle, 1] = v2[1, 2] + dot_parts(e3, up3[...])
        begin, end = blocks(cx.at[cycle], 8 + CYCLES + cycle)
        begin()
        end()
        for b in range(3):
            v2[0, b + 1] = cx[cycle, b]
        lines_sweep(v2, 0, 1, 1, 4, right, 0, h[2], n2)
        return solve(1, right[1] + h[2] * near(v2, 1, 2, n2))

    def lines3(cycle):
        begin, end = window3(cycle)
        begin()
        end()
        unpack3(cycle, g3)
        loop(1, 3, lambda b: v3.__setitem__((0, b), solve(3 + b - 1, g3[b - 1])))
        lines_sweep(v3, 0, 1, 1, 3, g3, 3, h[3], n3)
        res = line_residual(v3, 1, 1, g3, 3, h[3], n3)
        win4[cycle, 8 + par] = pack(dot_parts(res, down4[...]), n4)
        e4 = lines4(cycle)
        for t in range(2):
            v3[0, t + 1] = v3[1, t + 1] + dot_parts(e4, up4[par, t])
        lines_sweep(v3, 0, 1, 1, 3, g3, 3, h[3], n3)
        return solve(3, g3[0] + h[3] * near(v3, 1, 1, n3))

    def lines4(cycle):
        begin, end = window4(cycle)
        begin()
        end()
        unpack4(cycle, g4)
        loop(1, 3, lambda b: v4.__setitem__((0, b), solve(5 + b - 1, g4[b - 1])))
        q = 0
        for k in range(1, COARSE - 1):
            v4[1 - q, 1] = solve(5, g4[0] + h[4] * near(v4, q, 1, n4))
            q = 1 - q
        return solve(5, g4[0] + h[4] * near(v4, q, 1, n4))

    def correct0(m, q, lo, hi, fn):
        def body(i):
            i = fn(i)
            for r in range(0, zall, CROWS):
                e = dot_parts(v1[0, i + 2, PAD + r : PAD + r + CROWS, :], upy[...])
                for x in (2 * i + 2, 2 * i + 3):
                    v0[q, x, PAD + r : PAD + r + CROWS, :] = v0[m, x, PAD + r : PAD + r + CROWS, :] + e
        loop(lo, hi, body)

    def put(x, z, t, value):
        turn[t, pl.ds(z * r0 + x, 8, stride=r0), :] = value

    def fold(j):
        at = pl.ds(pl.multiple_of(PAD * r0 * j, PAD * r0), PAD * r0)
        for t in range(nt0):
            staged[at, 128 * t : 128 * (t + 1)] = turn[t, at, :]

    pair0(0, 1, hook=(halo_factors, halo_level0), restrict=True)
    coarse(0)
    correct0(1, 2, 0, r1, same)
    pair0(2, 0)
    pair0(0, 2, record=0)
    begin, end = planes0(2, 1)
    begin()
    restrict0(2, 1, r1 - 1, same)
    end()
    restrict0(2, 0, 2, lambda i: i * (r1 - 1))
    coarse(1)
    correct0(2, 0, 0, r1, same)
    pair0(0, 2, put=put)
    loop(0, zall // PAD, fold)
    begin, end = planes0(2, 1)
    begin()
    start_o()
    out[:, pl.ds(r0 * p, r0), :] = stage[pl.ds(depth * me, depth)]

    def last_norm(x):
        for r in range(0, zall, CROWS):
            for res in residual(level0, 2, x, r):
                acc[CYCLES - 1] += (res * res).reshape(CROWS // 8, 8, 128).sum(axis=0)

    loop(1, r0 - 1, last_norm)
    end()
    loop(0, 2, lambda i: last_norm(i * (r0 - 1)))
    ridx = lax.broadcasted_iota(jnp.int32, (8, 128), 0)
    part = jnp.zeros((8, 128), f32)
    for k in range(CYCLES):
        part = jnp.where(ridx == k, jnp.sum(acc[k]), part)
    nsend[...] = part
    start_n()
    total = part
    done_v()
    done_r()
    done_s()

    def finish(s):
        @pl.when(s != me)
        def _():
            landed_n(s)
            remote(zrows(stage, 0), zrows(stage, 0), a2a_send.at[3, 0], a2a_recv.at[3, s], place(p)).wait_recv()
    loop(0, nd, finish)
    nrecv[me] = part
    total = jnp.sum(nrecv[...], axis=0)
    norms[...] = total * (1.0 / (zall * n0 * n0))
    done_o()
    done_n()


def chain_shards(gz, gy, source, vertical, reaction):
    depth, n0 = source.shape[0], source.shape[1]
    nd = gz * gy
    zall = nd * depth
    n1, n2, n3, n4 = n0 // 2, n0 // 4, n0 // 8, n0 // 16
    r0, r1 = n0 // nd, n1 // nd
    f32 = jnp.float32
    bf16 = jnp.bfloat16

    def halve(n, k):
        return np.tile((np.arange(n)[:, None] // 2 == np.arange(n // 2)[None, :]).astype(np.float32) * 0.25, (1, k))

    downy = halve(n0, 1)
    upy = halve(n0, 1).T * 4.0
    down2 = np.zeros((r1 // 2 * n1, 128), np.float32)
    up2 = np.zeros((r1 // 2, 128, n1), np.float32)
    down3 = np.zeros((128, 128), np.float32)
    up3 = np.zeros((128, 128), np.float32)
    for i in range(r1 // 2):
        down2[i * n1 : (i + 1) * n1, i * n2 : (i + 1) * n2] = halve(n1, 1)
        up2[i, i * n2 : (i + 1) * n2, :] = halve(n1, 1).T * 4.0
        down3[i * n2 : (i + 1) * n2] = halve(n2, 128 // n3)
        up3[3 * n3 : 4 * n3, i * n2 : (i + 1) * n2] = halve(n2, 1).T * 4.0
    down4 = np.zeros((128, 128), np.float32)
    down4[3 * n3 : 4 * n3] = halve(n3, 128 // n4)
    up4 = np.zeros((2, 2, 128, 128), np.float32)
    for par in range(2):
        for s in range(1, 6):
            r = 4 + (par - 3 + s) // 2
            up4[par, s // 4, r * n4 : (r + 1) * n4, s % 4 * n3 : (s % 4 + 1) * n3] = halve(n3, 1).T * 4.0
    consts = [jnp.asarray(c, bf16) for c in (downy, upy, down2, up2, down3, down4, up3, up4)]
    vm = pl.BlockSpec(memory_space=pltpu.VMEM)
    sm = pl.BlockSpec(memory_space=pltpu.SMEM)
    ns = (zall - 1).bit_length()
    dma = pltpu.SemaphoreType.DMA
    solution, norms = pl.pallas_call(
        functools.partial(chain_kernel, (gz, gy, depth)),
        out_shape=(
            jax.ShapeDtypeStruct(source.shape, f32),
            jax.ShapeDtypeStruct((8, 128), f32),
        ),
        in_specs=[vm, vm, sm] + [vm] * len(consts),
        out_specs=(vm, vm),
        scratch_shapes=[
            pltpu.VMEM((3, r0 + 4, zall + 2 * PAD, n0), f32),
            pltpu.VMEM((r0 + 2, zall, n0), f32),
            pltpu.VMEM((r0 + 2, zall, n0), f32),
            pltpu.VMEM((r0 + 2, zall, n0), f32),
            pltpu.VMEM((3, r1 + 4, zall + 2 * PAD, n1), f32),
            pltpu.VMEM((r1 + 4, zall, n1), f32),
            pltpu.VMEM((r1 + 4, zall, n1), f32),
            pltpu.VMEM((r1 + 4, zall, n1), f32),
            pltpu.VMEM((zall, r0, n0), f32),
            pltpu.VMEM((zall, r0, n0), f32),
            pltpu.VMEM((zall, r0, n0), f32),
            pltpu.VMEM((n0 // 128, zall * r0, 128), f32),
            pltpu.VMEM((zall, 128), f32),
            pltpu.VMEM((depth, 128), f32),
            pltpu.VMEM((nd, depth, 128), f32),
            pltpu.VMEM((CYCLES, 3, zall, 128), f32),
            pltpu.VMEM((CYCLES, 3, zall, 128), f32),
            pltpu.VMEM((3, zall, 128), f32),
            pltpu.VMEM((CYCLES + 1, 7, n3 * zall // 128, 128), f32),
            pltpu.VMEM((CYCLES + 1, 18, n4 * zall // 128, 128), f32),
            pltpu.VMEM((2, 5, zall, 128), f32),
            pltpu.VMEM((2, 4, zall, 128), f32),
            pltpu.VMEM((2, 4, zall, 128), f32),
            pltpu.VMEM((2, zall, 128), f32),
            pltpu.VMEM((2, zall, 128), f32),
            pltpu.VMEM((7, zall, 128), f32),
            pltpu.VMEM((7, 2 * ns + 1, zall, 128), f32),
            pltpu.VMEM((7, zall, 128), f32),
            pltpu.VMEM((CYCLES, 8, 128), f32),
            pltpu.VMEM((8, 128), f32),
            pltpu.VMEM((nd, 8, 128), f32),
            dma((5, nd)),
            dma((5, nd)),
            dma((8 + 2 * CYCLES, 2)),
            dma((8 + 2 * CYCLES, 2)),
            dma((CYCLES + 1, 7)),
            dma((CYCLES + 1, 7)),
            dma((CYCLES + 1, 18)),
            dma((CYCLES + 1, 18)),
        ],
        compiler_params=pltpu.CompilerParams(
            has_side_effects=True, vmem_limit_bytes=64000 * 1024
        ),
    )(source, reaction, vertical, *consts)
    return solution, norms[:CYCLES, 0]


def shards_of(gz, gy, source, vertical, reaction):
    depth, n0 = source.shape[0], source.shape[1]
    nd = gz * gy
    fits = (
        gz % 2 == 0 and n0 % (8 * nd) == 0 and n0 // nd == 8 and n0 % 256 == 0 and n0 // 4 * 2 == 128
        and PAD % depth == 0 and nd * depth % 128 == 0 and (LEVELS, SWITCH, SWEEPS, COARSE, CYCLES) == (5, 2, 2, 4, 2)
    )
    return (chain_shards if fits else shards)(gz, gy, source, vertical, reaction)


def solution(mesh):
    return jax.shard_map(
        functools.partial(shards_of, mesh.shape["gz"], mesh.shape["gy"]),
        mesh=mesh,
        in_specs=(P(("gz", "gy"), None, None), P(("gz", "gy")), P(("gz", "gy"), None, None)),
        out_specs=(P(("gz", "gy"), None, None), P()),
        check_vma=False,
    )
```

```python
import functools

import jax
import jax.numpy as jnp
import numpy as np
from jax import lax
from jax.experimental import pallas as pl
from jax.experimental.pallas import tpu as pltpu
from jax.sharding import PartitionSpec as P

LEVELS = 5
SWITCH = 2
CYCLES = 2
SWEEPS = 2
COARSE = 4
DAMPING = 0.8
COUPLING = 1.0
CHUNK = 32
MESH = pl.DeviceIdType.MESH


def dot(a, b):
    return lax.dot_general(
        a,
        b,
        (((1,), (0,)), ((), ())),
        precision=lax.Precision.HIGHEST,
        preferred_element_type=jnp.float32,
    )


def parts_of(x):
    first = x.astype(jnp.bfloat16)
    rest = x - first.astype(jnp.float32)
    second = rest.astype(jnp.bfloat16)
    third = (rest - second.astype(jnp.float32)).astype(jnp.bfloat16)
    return (third, second, first)


def dot_right(x, m):
    m = m.astype(jnp.bfloat16)
    total = None
    for x in parts_of(x):
        term = jnp.dot(x, m, preferred_element_type=jnp.float32)
        total = term if total is None else total + term
    return total


def dot_left(m, x):
    m = m.astype(jnp.bfloat16)
    total = None
    for x in parts_of(x):
        term = jnp.dot(m, x, preferred_element_type=jnp.float32)
        total = term if total is None else total + term
    return total


def kernel(
    dims,
    source, reaction, vert_s, vert_b, down0, downt0, down1, cols, mask, group, ups, groupt, colst,
    out, norms,
    v0, v1, w0, d1, w1, g1, r1, tmp0, res1, corr1, send_a, recv_a, send_v, recv_v, recv_b,
    send_n, recv_n, lines, diag, factor, target, around, halo, rowbuf, acc,
    plane_send, plane_recv, line_send, line_recv, a2a_send, a2a_recv,
):
    gz, gy, depth, cp = dims
    nd = gz * gy
    zall = nd * depth
    n0 = source.shape[1]
    n1 = n0 // 2
    a_me = lax.axis_index("gz")
    b_me = lax.axis_index("gy")
    me = a_me * gy + b_me
    h = [COUPLING / 4.0**k for k in range(LEVELS)]

    @pl.when(me == 0)
    def _():
        for p in range(2):
            v0[p, 0] = jnp.zeros((n0, n0), jnp.float32)
            v1[p, 0] = jnp.zeros((n1, n1), jnp.float32)

    @pl.when(me == nd - 1)
    def _():
        for p in range(2):
            v0[p, depth + 1] = jnp.zeros((n0, n0), jnp.float32)
            v1[p, depth + 1] = jnp.zeros((n1, n1), jnp.float32)

    edges = [a_me == 0, a_me == gz - 1, b_me == 0, b_me == gy - 1]
    for k in range(4):
        @pl.when(edges[k])
        def _(k=k):
            for p in range(2):
                halo[p, k] = jnp.zeros((zall, cp), jnp.float32)

    def flat(d):
        return (d // gy, d % gy)

    def plane_copy(v, p, level, up):
        if up:
            src, dst, to = v.at[p, depth], v.at[p, 0], flat(me + 1)
        else:
            src, dst, to = v.at[p, 1], v.at[p, depth + 1], flat(me + nd - 1 - nd * ((me + nd - 1) // nd))
        if up:
            to = flat((me + 1) % nd)
        k = 0 if up else 1
        return pltpu.make_async_remote_copy(
            src_ref=src, dst_ref=dst,
            send_sem=plane_send.at[level, p, k], recv_sem=plane_recv.at[level, p, k],
            device_id=to, device_id_type=MESH,
        )

    def plane_start(v, p, level):
        @pl.when(me < nd - 1)
        def _():
            plane_copy(v, p, level, True).start()

        @pl.when(me > 0)
        def _():
            plane_copy(v, p, level, False).start()

    def plane_wait(v, p, level):
        @pl.when(me < nd - 1)
        def _():
            plane_copy(v, p, level, True).wait_send()
            plane_copy(v, p, level, False).wait_recv()

        @pl.when(me > 0)
        def _():
            plane_copy(v, p, level, False).wait_send()
            plane_copy(v, p, level, True).wait_recv()

    def residual_chunk(v, p, z, r, n, target_ref, diag_of, weight):
        centre = v[p, z, pl.ds(r, CHUNK), :]
        rows = lax.broadcasted_iota(jnp.int32, (CHUNK, n), 0)
        lanes = lax.broadcasted_iota(jnp.int32, (CHUNK, n), 1)
        if r == 0:
            above = jnp.where(rows == 0, 0.0, pltpu.roll(centre, 1, 0))
        else:
            above = v[p, z, pl.ds(r - 1, CHUNK), :]
        if r + CHUNK == n:
            below = jnp.where(rows == CHUNK - 1, 0.0, pltpu.roll(centre, CHUNK - 1, 0))
        else:
            below = v[p, z, pl.ds(r + 1, CHUNK), :]
        left = jnp.where(lanes == 0, 0.0, pltpu.roll(centre, 1, 1))
        right = jnp.where(lanes == n - 1, 0.0, pltpu.roll(centre, n - 1, 1))
        vert = vert_s[z - 1]
        applied = (
            diag_of(z - 1, r, vert) * centre
            - vert * (v[p, z - 1, pl.ds(r, CHUNK), :] + v[p, z + 1, pl.ds(r, CHUNK), :])
            - weight * (above + below + left + right)
        )
        return centre, target_ref[z - 1, pl.ds(r, CHUNK), :] - applied

    def diag0(z, r, vert):
        return 2.0 * vert + 4.0 * h[0] + reaction[z, pl.ds(r, CHUNK), :]

    def diag1(z, r, vert):
        return d1[z, pl.ds(r, CHUNK), :]

    def over_planes(v, p, level, body):
        plane_start(v, p, level)

        def inner(z, c):
            body(z)
            return c

        lax.fori_loop(2, depth, inner, 0)
        plane_wait(v, p, level)

        def outer(i, c):
            body(1 + i * (depth - 1))
            return c

        lax.fori_loop(0, 2, outer, 0)

    def level_parts(level):
        if level == 0:
            return v0, source, diag0, w0, n0
        return v1, g1, diag1, w1, n1

    def sweep(level, p, record=None):
        v, tgt, dg, w, n = level_parts(level)

        def body(z):
            for r in range(0, n, CHUNK):
                centre, res = residual_chunk(v, p, z, r, n, tgt, dg, h[level])
                v[1 - p, z, pl.ds(r, CHUNK), :] = centre + w[z - 1, pl.ds(r, CHUNK), :] * res
                if record is not None:
                    sq = (res * res).reshape(CHUNK // 8, 8, n).sum(axis=0)
                    acc[record, :, :] += sq

        over_planes(v, p, level, body)
        return 1 - p

    def first_sweep(level):
        v, tgt, dg, w, n = level_parts(level)

        def body(z, c):
            v[0, z + 1] = w[z] * tgt[z]
            return c

        lax.fori_loop(0, depth, body, 0)
        return 0

    def restrict0(read_chunk, store):
        def body(z):
            for r in range(0, n0, CHUNK):
                tmp0[pl.ds(r, CHUNK), :] = dot_right(read_chunk(z, r), downt0[...])
            store(z, dot_left(down0[...], tmp0[...]))
        return body

    def restrict1(z, plane):
        half = dot(down1[...], plane)
        for b in range(gy):
            spread = dot(half, cols[b]) * mask[...]
            packed = dot(group[...], spread)
            for a in range(gz):
                send_a[b, a, z : z + 1, :] = packed[a : a + 1, :]

    def exchange_all(kind, src_of, recv):
        def copy(k):
            dst = (me + k) % nd
            a, b = dst // gy, dst % gy
            return pltpu.make_async_remote_copy(
                src_ref=src_of(a, b), dst_ref=recv.at[b_me, a_me],
                send_sem=a2a_send.at[kind, k], recv_sem=a2a_recv.at[kind, me],
                device_id=(a, b), device_id_type=MESH,
            )

        def start(k, c):
            copy(k).start()
            return c

        def finish(k, c):
            copy(k).wait_send()
            src = (me + k) % nd
            a, b = src // gy, src % gy
            pltpu.make_async_remote_copy(
                src_ref=recv.at[b, a], dst_ref=recv.at[b, a],
                send_sem=a2a_send.at[kind, k], recv_sem=a2a_recv.at[kind, src],
                device_id=(a, b), device_id_type=MESH,
            ).wait_recv()
            return c

        def begin():
            lax.fori_loop(1, nd, start, 0)

        def end():
            lax.fori_loop(1, nd, finish, 0)

        return begin, end

    def to_lines(recv, dest):
        for a in range(gz):
            for b in range(gy):
                s = (a * gy + b) * depth
                dest[s : s + depth, :] = recv[b, a]

    bx2, by2 = (n1 // 2 // gz, n1 // 2 // gy)
    steps = []
    s = 1
    while s < zall:
        steps.append(s)
        s *= 2
    ns = len(steps)

    def setup_lines(offset):
        rows = lax.broadcasted_iota(jnp.int32, (zall, cp), 0)
        vert = lines[...]
        a = jnp.where(rows == 0, 0.0, -vert)
        c = jnp.where(rows == zall - 1, 0.0, -vert)
        b = diag[offset]
        for k, s in enumerate(steps):
            alpha = -a / pltpu.roll(b, s, 0)
            gamma = -c / pltpu.roll(b, zall - s, 0)
            b = b + alpha * pltpu.roll(c, s, 0) + gamma * pltpu.roll(a, zall - s, 0)
            a = alpha * pltpu.roll(a, s, 0)
            c = gamma * pltpu.roll(c, zall - s, 0)
            factor[offset, 2 * k] = alpha
            factor[offset, 2 * k + 1] = gamma
        factor[offset, 2 * ns] = 1.0 / b

    def solve(offset, right):
        for k, s in enumerate(steps):
            right = (
                right
                + factor[offset, 2 * k] * pltpu.roll(right, s, 0)
                + factor[offset, 2 * k + 1] * pltpu.roll(right, zall - s, 0)
            )
        return right * factor[offset, 2 * ns]

    count = [0]
    def line_copy(p, k):
        if k == 0:
            to, slot = ((a_me + gz - 1) % gz, b_me), 1
        elif k == 1:
            to, slot = ((a_me + 1) % gz, b_me), 0
        elif k == 2:
            to, slot = (a_me, (b_me + gy - 1) % gy), 3
        else:
            to, slot = (a_me, (b_me + 1) % gy), 2
        return pltpu.make_async_remote_copy(
            src_ref=around.at[p], dst_ref=halo.at[p, slot],
            send_sem=line_send.at[p, k], recv_sem=line_recv.at[p, slot],
            device_id=to, device_id_type=MESH,
        )

    def line_landed(p, k):
        return pltpu.make_async_remote_copy(
            src_ref=around.at[p], dst_ref=halo.at[p, k],
            send_sem=line_send.at[p, k], recv_sem=line_recv.at[p, k],
            device_id=(a_me, b_me), device_id_type=MESH,
        )

    def neighbours(offset, values):
        bx, by = bx2 >> offset, by2 >> offset
        cells = bx * by
        p = count[0] % 2
        count[0] += 1
        around[p] = values
        for k in range(4):
            @pl.when(jnp.logical_not(edges[k]))
            def _(k=k):
                line_copy(p, k).start()
        for k in range(4):
            @pl.when(jnp.logical_not(edges[k]))
            def _(k=k):
                line_copy(p, k).wait_send()
                line_landed(p, k).wait_recv()
        lane = lax.broadcasted_iota(jnp.int32, (zall, cp), 1)

        def roll(x, amount):
            amount = amount % cp
            return x if amount == 0 else pltpu.roll(x, amount, 1)

        total = jnp.where(lane < by, roll(halo[p, 0], by - cells), roll(values, by))
        total += jnp.where(lane >= cells - by, roll(halo[p, 1], cells - by), roll(values, -by))
        inrow = lane & (by - 1)
        total += jnp.where(inrow == 0, roll(halo[p, 2], 1 - by), roll(values, 1))
        total += jnp.where(inrow == by - 1, roll(halo[p, 3], by - 1), roll(values, -1))
        return total

    def line_descend(offset):
        weight = h[SWITCH + offset]
        values = solve(offset, target[offset])
        repeats = COARSE if offset == LEVELS - 1 - SWITCH else SWEEPS
        for _ in range(1, repeats):
            values = solve(offset, target[offset] + weight * neighbours(offset, values))
        if offset == LEVELS - 1 - SWITCH:
            return values
        near = neighbours(offset, values)
        rows = lax.broadcasted_iota(jnp.int32, (zall, cp), 0)
        before = jnp.where(rows == 0, 0.0, pltpu.roll(values, 1, 0))
        after = jnp.where(rows == zall - 1, 0.0, pltpu.roll(values, zall - 1, 0))
        res = target[offset] - (
            diag[offset] * values - lines[...] * (before + after) - weight * near
        )
        target[offset + 1] = dot(res, ups[2 * offset])
        tmp = values
        lower = line_descend(offset + 1)
        values = tmp + dot(lower, ups[2 * offset + 1])
        for _ in range(SWEEPS):
            values = solve(offset, target[offset] + weight * neighbours(offset, values))
        return values

    def fill0(z, c):
        w0[z] = DAMPING / (2.0 * vert_s[z] + 4.0 * h[0] + reaction[z])
        return c

    lax.fori_loop(0, depth, fill0, 0)

    def keep_r1(z, value):
        r1[z] = value
        dv = 2.0 * vert_s[z] + 4.0 * h[1] + value
        d1[z] = dv
        w1[z] = DAMPING / dv

    body = restrict0(lambda z, r: reaction[z, pl.ds(r, CHUNK), :], keep_r1)
    lax.fori_loop(0, depth, lambda z, c: (body(z), c)[1], 0)
    for z in range(depth):
        restrict1(z, r1[z])
    send_v[...] = send_a[...]
    begin_v, end_v = exchange_all(0, lambda a, b: vert_b, recv_v)
    begin_r, end_r = exchange_all(1, lambda a, b: send_v.at[b, a], recv_a)
    begin_v()
    begin_r()
    recv_v[b_me, a_me] = vert_b[...]
    recv_a[b_me, a_me] = send_v[b_me, a_me]
    acc[...] = jnp.zeros_like(acc)

    begin_a, end_a = exchange_all(2, lambda a, b: send_a.at[b, a], recv_b.at[0])
    begin_b, end_b = exchange_all(3, lambda a, b: send_n.at[b, a], recv_b.at[1])

    p0 = first_sweep(0)
    for cycle in range(CYCLES):
        for k in range(SWEEPS):
            if cycle == 0 and k == 0:
                continue
            p0 = sweep(0, p0, record=cycle - 1 if cycle > 0 and k == 0 else None)

        def read0(z, r, p0=p0):
            return residual_chunk(v0, p0, z, r, n0, source, diag0, h[0])[1]

        def keep_g1(z, value):
            g1[z - 1] = value

        over_planes(v0, p0, 0, restrict0(read0, keep_g1))
        p1 = first_sweep(1)
        for k in range(1, SWEEPS):
            p1 = sweep(1, p1)

        def keep_res(z, p1=p1):
            for r in range(0, n1, CHUNK):
                res1[z - 1, pl.ds(r, CHUNK), :] = residual_chunk(
                    v1, p1, z, r, n1, g1, diag1, h[1]
                )[1]

        over_planes(v1, p1, 1, keep_res)
        for z in range(depth):
            restrict1(z, res1[z])
        begin_a()
        recv_b[0, b_me, a_me] = send_a[b_me, a_me]
        if cycle == 0:
            end_v()
            end_r()
            to_lines(recv_v, lines)
            to_lines(recv_a, target.at[0])
            coarse = target[0]
            for offset in range(LEVELS - SWITCH):
                if offset > 0:
                    coarse = dot(coarse, ups[2 * offset - 2])
                diag[offset] = 2.0 * lines[...] + 4.0 * h[SWITCH + offset] + coarse
            for offset in range(LEVELS - SWITCH):
                setup_lines(offset)
        end_a()
        to_lines(recv_b.at[0], target.at[0])
        rowbuf[...] = line_descend(0)
        for a in range(gz):
            for b in range(gy):
                s = (a * gy + b) * depth
                send_n[b, a] = rowbuf[s : s + depth, :]
        begin_b()
        recv_b[1, b_me, a_me] = send_n[b_me, a_me]
        end_b()
        for z in range(depth):
            wide = None
            for b in range(gy):
                for a in range(gz):
                    corr1[a : a + 1, :] = recv_b[1, b, a, z : z + 1, :]
                part = dot(dot(groupt[...], corr1[...]) * mask[...], colst[b])
                wide = part if wide is None else wide + part
            v1[1 - p1, z + 1] = v1[p1, z + 1] + dot(down1[...].T * 2.0, wide)
        p1 = 1 - p1
        for _ in range(SWEEPS):
            p1 = sweep(1, p1)

        def correct0(z, c, p0=p0, p1=p1):
            tmp0[...] = dot_left(downt0[...] * 2.0, v1[p1, z])
            for r in range(0, n0, CHUNK):
                v0[1 - p0, z, pl.ds(r, CHUNK), :] = v0[p0, z, pl.ds(r, CHUNK), :] + dot_right(
                    tmp0[pl.ds(r, CHUNK), :], down0[...] * 2.0
                )
            return c

        lax.fori_loop(1, depth + 1, correct0, 0)
        p0 = 1 - p0
        for _ in range(SWEEPS):
            p0 = sweep(0, p0)

    def last(z, p0=p0):
        for r in range(0, n0, CHUNK):
            centre, res = residual_chunk(v0, p0, z, r, n0, source, diag0, h[0])
            out[z - 1, pl.ds(r, CHUNK), :] = centre
            acc[CYCLES - 1, :, :] += (res * res).reshape(CHUNK // 8, 8, n0).sum(axis=0)

    over_planes(v0, p0, 0, last)
    ridx = lax.broadcasted_iota(jnp.int32, (8, 128), 0)
    part = jnp.zeros((8, 128), jnp.float32)
    for k in range(CYCLES):
        part = jnp.where(ridx == k, jnp.sum(acc[k]), part)
    rowbuf_n = tmp_n = send_n
    target_n = recv_n
    w_n = acc
    acc[0, :, 0:128] = part
    begin_n, end_n = exchange_all(4, lambda a, b: acc.at[0, :, pl.ds(0, 128)], recv_n)
    begin_n()
    recv_n[b_me, a_me] = part
    end_n()
    total = jnp.zeros((8, 128), jnp.float32)
    for a in range(gz):
        for b in range(gy):
            total = total + recv_n[b, a]
    norms[...] = total * (1.0 / (zall * n0 * n0))


def pair_matrix(n, value):
    return (np.arange(n)[None, :] // 2 == np.arange(n // 2)[:, None]).astype(np.float32) * value


def shards(gz, gy, source, vertical, reaction):
    depth, n0 = source.shape[0], source.shape[1]
    nd = gz * gy
    zall = nd * depth
    n1, n2 = n0 // 2, n0 // 4
    bx, by = n2 // gz, n2 // gy
    cells = bx * by
    cp = -(-cells // 128) * 128
    down0 = pair_matrix(n0, 0.5)
    down1 = pair_matrix(n1, 0.5)
    lane = np.arange(cp)
    cols = np.zeros((gy, n1, cp), np.float32)
    colst = np.zeros((gy, cp, n1), np.float32)
    for b in range(gy):
        hit = (np.arange(n1)[:, None] // 2 == b * by + lane[None, :] % by) & (lane[None, :] < cells)
        cols[b] = hit * 0.5
        colst[b] = hit.T
    mask = ((lane[None, :] // by == np.arange(n2)[:, None] % bx) & (lane[None, :] < cells)).astype(np.float32)
    group = (np.arange(n2)[None, :] // bx == np.arange(gz)[:, None]).astype(np.float32)
    ups = []
    for offset in range(LEVELS - SWITCH - 1):
        fx, fy = bx >> offset, by >> offset
        cy = fy // 2
        matrix = np.zeros((cp, cp), np.float32)
        for i in range(fx):
            for j in range(fy):
                matrix[i * fy + j, (i // 2) * cy + j // 2] = 1.0
        ups += [matrix * 0.25, matrix.T]
    ups = np.stack(ups)
    steps = (zall - 1).bit_length()
    f32 = jnp.float32
    nl = LEVELS - SWITCH
    vm = pl.BlockSpec(memory_space=pltpu.VMEM)
    consts = [down0, down0.T.copy(), down1, cols, mask, group, ups, group.T.copy(), colst]
    solution, norms = pl.pallas_call(
        functools.partial(kernel, (gz, gy, depth, cp)),
        out_shape=(
            jax.ShapeDtypeStruct(source.shape, f32),
            jax.ShapeDtypeStruct((8, 128), f32),
        ),
        in_specs=[vm, vm, pl.BlockSpec(memory_space=pltpu.SMEM), vm] + [vm] * len(consts),
        out_specs=(vm, vm),
        scratch_shapes=[
            pltpu.VMEM((2, depth + 2, n0, n0), f32),
            pltpu.VMEM((2, depth + 2, n1, n1), f32),
            pltpu.VMEM((depth, n0, n0), f32),
            pltpu.VMEM((depth, n1, n1), f32),
            pltpu.VMEM((depth, n1, n1), f32),
            pltpu.VMEM((depth, n1, n1), f32),
            pltpu.VMEM((depth, n1, n1), f32),
            pltpu.VMEM((n0, n1), f32),
            pltpu.VMEM((depth, n1, n1), f32),
            pltpu.VMEM((gz, cp), f32),
            pltpu.VMEM((gy, gz, depth, cp), f32),
            pltpu.VMEM((gy, gz, depth, cp), f32),
            pltpu.VMEM((gy, gz, depth, cp), f32),
            pltpu.VMEM((gy, gz, depth, cp), f32),
            pltpu.VMEM((2, gy, gz, depth, cp), f32),
            pltpu.VMEM((gy, gz, depth, cp), f32),
            pltpu.VMEM((gy, gz, 8, 128), f32),
            pltpu.VMEM((zall, cp), f32),
            pltpu.VMEM((nl, zall, cp), f32),
            pltpu.VMEM((nl, 2 * steps + 1, zall, cp), f32),
            pltpu.VMEM((nl, zall, cp), f32),
            pltpu.VMEM((2, zall, cp), f32),
            pltpu.VMEM((2, 4, zall, cp), f32),
            pltpu.VMEM((zall, cp), f32),
            pltpu.VMEM((CYCLES, 8, n0), f32),
            pltpu.SemaphoreType.DMA((2, 2, 2)),
            pltpu.SemaphoreType.DMA((2, 2, 2)),
            pltpu.SemaphoreType.DMA((2, 4)),
            pltpu.SemaphoreType.DMA((2, 4)),
            pltpu.SemaphoreType.DMA((5, nd)),
            pltpu.SemaphoreType.DMA((5, nd)),
        ],
        compiler_params=pltpu.CompilerParams(
            has_side_effects=True, vmem_limit_bytes=64000 * 1024
        ),
    )(
        source,
        reaction,
        vertical,
        jnp.broadcast_to(vertical[:, None], (depth, cp)),
        *[jnp.asarray(c) for c in consts],
    )
    return solution, norms[:CYCLES, 0]


CROWS = 32
VMEM_LIMIT = 64000 * 1024
PAD = 8


def dot_parts(x, m, parts=2):
    total = None
    rest = x
    for k in range(parts):
        piece = rest.astype(jnp.bfloat16)
        if k + 1 < parts:
            rest = rest - piece.astype(jnp.float32)
        term = jnp.dot(piece, m, preferred_element_type=jnp.float32)
        total = term if total is None else total + term
    return total


def chain_kernel(
    dims,
    source_in, reaction_in, vertical,
    out, norms,
    source, reaction, downy, upy, up2, down3, down4, up3, up4, load,
    v0, g0, w0, d0, v1, g1, w1, d1, raw_r, raw_s, stage, turn, lines, vsend, vrecv,
    gx, cx, dx, win3, win4, v2, v3, v4, g3, g4, diag, fac, mask, acc, nsend, nrecv,
    a2a_send, a2a_recv, from_sem, x_send, x_recv, w3_send, w3_recv, w4_send, w4_recv,
):
    gz, gy, depth = dims
    nd = gz * gy
    zall = nd * depth
    n0 = source.shape[1]
    n1, n2, n3, n4 = n0 // 2, n0 // 4, n0 // 8, n0 // 16
    r0, r1 = n0 // nd, n0 // 2 // nd
    nt0 = n0 // 128
    h = [COUPLING / 4.0**k for k in range(LEVELS)]
    f32 = jnp.float32
    a_me, b_me = lax.axis_index("gz"), lax.axis_index("gy")
    me = a_me * gy + b_me
    nchip = gz // 2

    def bend(c):
        return c + c // 2 - 2 * (c // 3) if nchip == 4 else c

    def place(i):
        k, core = i // 2, i % 2
        b, q = k // nchip, k % nchip
        q = q + (b % 2) * (nchip - 1 - 2 * q)
        return (bend(q) * 2 + core, b)

    q_me = bend(a_me // 2)
    q_me = q_me + (b_me % 2) * (nchip - 1 - 2 * q_me)
    p = (b_me * nchip + q_me) * 2 + a_me % 2
    chip, par = p // 2, p % 2

    def loop(lo, hi, body):
        def step(i, c):
            body(i)
            return c
        lax.fori_loop(lo, hi, step, 0)

    def remote(src, dst, ss, rs, to):
        return pltpu.make_async_remote_copy(
            src_ref=src, dst_ref=dst, send_sem=ss, recv_sem=rs, device_id=to, device_id_type=MESH
        )

    def target(k):
        return (p + nd + (k // 2 + k % 2) * (1 - 2 * (k % 2))) % nd

    def flat(i):
        a, b = place(i)
        return a * gy + b

    def spread(kind, src_of, dst_mine, whole, each=None):
        def start(k):
            t = target(k)
            sem = a2a_recv.at[kind] if each is None else from_sem.at[me]
            remote(src_of(t), dst_mine, a2a_send.at[kind], sem, place(t)).start()

        def wait_all(recv):
            copy = remote(whole, whole, a2a_send.at[kind], a2a_recv.at[kind], place(p))
            copy.wait_recv() if recv else copy.wait_send()

        def landed(s):
            if each is None:
                wait_all(True)
            else:
                r = each(s)
                remote(r, r, a2a_send.at[kind], from_sem.at[s], place(p)).wait_recv()

        return lambda: loop(1, nd, start), lambda: wait_all(False), landed

    def piece(ref, t):
        return ref.at[:, pl.ds(r0 * t, r0), :]

    def zrows(ref, s):
        return ref.at[pl.ds(depth * s, depth)]

    zrest = pl.ds(0, depth * (nd - 1))
    rest = pl.ds(0, nd - 1)
    start_v, done_v, landed_v = spread(0, lambda t: vsend, vrecv.at[me], vrecv.at[rest])
    start_r, done_r, landed_r = spread(1, lambda t: piece(reaction, t), zrows(raw_r, me), raw_r.at[zrest])
    start_s, done_s, landed_s = spread(
        2, lambda t: piece(source, t), zrows(raw_s, me), raw_s.at[zrest], lambda s: zrows(raw_s, s))
    start_o, done_o, landed_o = spread(
        3, lambda t: zrows(stage, flat(t)), piece(out, p), stage.at[zrest], lambda s: zrows(stage, s))
    start_n, done_n, landed_n = spread(4, lambda t: nsend, nrecv.at[me], nrecv.at[rest])

    load_r = pltpu.make_async_copy(reaction_in, reaction, load.at[0])
    load_s = pltpu.make_async_copy(source_in, source, load.at[1])
    load_r.start()
    load_s.start()
    for i in range(depth):
        vsend[i : i + 1, :] = jnp.full((1, 128), vertical[i], f32)
    load_r.wait()
    start_r()
    start_v()
    load_s.wait()
    start_s()

    def fill(ref, at, value):
        shape = ref.shape[-2:]
        row = lax.broadcasted_iota(jnp.int32, shape, 0)
        col = lax.broadcasted_iota(jnp.int32, shape, 1)
        hit, scale = value(row, col)
        ref[at] = jnp.where(hit, scale, 0.0).astype(jnp.bfloat16)

    fill(downy, ..., lambda r, c: (r // 2 == c, 0.25))
    fill(upy, ..., lambda r, c: (r == c // 2, 1.0))
    for i in range(r1 // 2):
        fill(up2, i, lambda r, c: (r == n2 * i + c // 2, 1.0))
    fill(down3, ..., lambda r, c: (r % n2 // 2 == c % n3, 0.25))
    fill(down4, 0, lambda r, c: ((r >= 3 * n3) & ((r - 3 * n3) // 2 == c % n4), 0.25))
    fill(down4, 1, lambda r, c: ((r < n3) & (r // 2 == c % n4), 0.25))
    fill(up3, 0, lambda r, c: (r == 3 * n3 + c % n2 // 2, 1.0))
    fill(up3, 1, lambda r, c: (r == c % n2 // 2, 1.0))
    for t in range(2):
        fill(up4, t, lambda r, c: (r == n4 * (4 + (4 * t + c // n3 + 5) // 2 - 4) + c % n3 // 2, 1.0))

    first, last = p == 0, p == nd - 1

    def xchg(kind, lo_src, lo_dst, hi_src, hi_dst):
        def down():
            return remote(lo_src, hi_dst, x_send.at[kind, 0], x_recv.at[kind, 0], place((p + nd - 1) % nd))

        def up():
            return remote(hi_src, lo_dst, x_send.at[kind, 1], x_recv.at[kind, 1], place((p + 1) % nd))

        def begin():
            @pl.when(jnp.logical_not(first))
            def _():
                down().start()

            @pl.when(jnp.logical_not(last))
            def _():
                up().start()

        def end():
            @pl.when(jnp.logical_not(first))
            def _():
                down().wait_send()
                up().wait_recv()

            @pl.when(jnp.logical_not(last))
            def _():
                up().wait_send()
                down().wait_recv()

        return begin, end

    def planes0(m, dep):
        def at(lo):
            return v0.at[m, pl.ds(lo, dep), pl.ds(PAD, zall), :]
        return xchg(m, at(2), at(2 - dep), at(2 + r0 - dep), at(2 + r0))

    def planes1(ref, kind):
        return xchg(kind, ref.at[pl.ds(2, 2)], ref.at[pl.ds(0, 2)],
                    ref.at[pl.ds(r1, 2)], ref.at[pl.ds(r1 + 2, 2)])

    def planes1v(m):
        def at(lo):
            return v1.at[m, pl.ds(lo, 2), pl.ds(PAD, zall), :]
        return xchg(4, at(2), at(0), at(r1), at(r1 + 2))

    def blocks(ref, kind):
        return xchg(kind, ref.at[1], ref.at[0], ref.at[1], ref.at[2])

    def halo_d0():
        return xchg(5, d0.at[1], d0.at[0], d0.at[r0], d0.at[r0 + 1])

    offs3 = [(o, c) for o in (0, -1, 1, -2, 2) for c in range(2)]

    def window3(kind):
        buf = win3.at[kind]

        def out_of(o, c):
            slot = par + 3 - 2 * o
            return remote(buf.at[3 + par], buf.at[slot], w3_send.at[4 + 2 * o + c], w3_recv.at[kind // CYCLES, slot],
                          place((2 * (chip + o) + c + nd) % nd))

        def goes(o, c):
            there = jnp.logical_and(chip + o >= 0, chip + o < nd // 2)
            if o == 0:
                return par != c
            if o == -2:
                return jnp.logical_and(there, par == 0)
            if o == 2:
                return jnp.logical_and(there, par == 1)
            return there

        def begin():
            for o, c in offs3:
                @pl.when(goes(o, c))
                def _(o=o, c=c):
                    out_of(o, c).start()

        def end():
            for o, c in offs3:
                @pl.when(goes(o, c))
                def _(o=o, c=c):
                    out_of(o, c).wait_send()
            for q in range(8):
                row = 2 * chip - 3 + q
                inside = jnp.logical_and(row >= 0, row < nd)
                if q in (3, 4):
                    inside = par != q - 3

                @pl.when(inside)
                def _(q=q):
                    remote(buf.at[q], buf.at[q], w3_send.at[0], w3_recv.at[kind // CYCLES, q], place(p)).wait_recv()

        return begin, end

    offs4 = [-1, 1, -2, 2, -3, 3, -4, 4]

    def window4(kind):
        buf = win4.at[kind]

        def each(fn):
            for o in offs4:
                @pl.when(jnp.logical_and(chip + o >= 0, chip + o < nd // 2))
                def _(o=o):
                    fn(o)

        def out_of(o):
            return remote(buf.at[4], buf.at[4 - o], w4_send.at[4 + o], w4_recv.at[kind // CYCLES, 4 - o],
                          place((p + 2 * o + nd) % nd))

        def begin():
            each(lambda o: out_of(o).start())

        def end():
            def fn(o):
                out_of(o).wait_send()
                remote(buf.at[4 + o], buf.at[4 + o], w4_send.at[4 + o], w4_recv.at[kind // CYCLES, 4 + o],
                       place(p)).wait_recv()
            each(fn)

        return begin, end

    zpad = jnp.zeros((PAD, n0), f32)
    for m in range(3):
        def zero0(x, m=m):
            v0[m, x, 0:PAD, :] = zpad
            v0[m, x, PAD + zall : 2 * PAD + zall, :] = zpad
        loop(0, r0 + 4, zero0)

        def zero1(x, m=m):
            v1[m, x, 0:PAD, :] = zpad[:, :n1]
            v1[m, x, PAD + zall : 2 * PAD + zall, :] = zpad[:, :n1]
        loop(0, r1 + 4, zero1)

    tile0 = jnp.zeros((zall, 128), f32)
    plane0 = jnp.zeros((zall, n0), f32)

    def blank(lo0, x0, lo1, b):
        for q in range(2):
            for m in (0, 2):
                v0[m, lo0 + q, PAD : PAD + zall, :] = plane0
            v1[2, lo1 + q, PAD : PAD + zall, :] = tile0
            g1[lo1 + q] = tile0
            d1[lo1 + q] = tile0
            w1[lo1 + q] = tile0
        d0[x0] = plane0
        w0[x0] = plane0
        for k in range(CYCLES):
            gx[k, b] = tile0
            cx[k, b] = tile0
        dx[b] = tile0

    @pl.when(first)
    def _():
        blank(0, 0, 0, 0)

    @pl.when(last)
    def _():
        blank(r0 + 2, r0 + 1, r1 + 2, 2)

    for k in range(CYCLES + 1):
        for q in range(8):
            @pl.when(jnp.logical_or(2 * chip - 3 + q < 0, 2 * chip - 3 + q >= nd))
            def _(q=q, k=k):
                win3[k, q] = jnp.zeros((n3 * zall // 128, 128), f32)
        for o in offs4:
            @pl.when(jnp.logical_or(chip + o < 0, chip + o >= nd // 2))
            def _(o=o, k=k):
                win4[k, 4 + o] = jnp.zeros((n4 * zall // 128, 128), f32)
    for q in range(2):
        v2[q, 0] = tile0
        v2[q, 4] = tile0
        v3[q, 0] = tile0
        v3[q, 3] = tile0
        v4[q, 0] = tile0
        v4[q, 3] = tile0
    v4[1, 2] = tile0
    acc[...] = jnp.zeros_like(acc)

    lane = lax.broadcasted_iota(jnp.int32, (zall, 128), 1)
    rows = lax.broadcasted_iota(jnp.int32, (zall, 128), 0)

    for t in range(3):
        good = [p > 0, None, p < nd - 1][t]
        one = jnp.ones((zall, 128), f32)
        mask[t] = one if good is None else one * good.astype(f32)
    for t in range(2):
        row = 2 * chip - 3 + 4 * t + lane // n3
        mask[3 + t] = jnp.where((row >= 0) & (row < nd), 1.0, 0.0)
        row = chip - 4 + 8 * t + lane // n4
        mask[5 + t] = jnp.where((row >= 0) & (row < nd // 2) & (row < chip + 5), 1.0, 0.0)

    def pack(rep, width):
        k = 128 // width
        zb = zall // k
        part = lane[:zb]
        got = rep[0:zb]
        for j in range(1, k):
            got = jnp.where(part // width == j, rep[zb * j : zb * (j + 1)], got)
        return got

    def unpack(slots, width):
        k = 128 // width
        zb = zall // k
        part = lane[:zb] // width
        parts = []
        for j in range(k):
            got = jnp.zeros((zb, 128), f32)
            for s, x in enumerate(slots):
                turn = (width * (s - j)) % 128
                x = x if turn == 0 else pltpu.roll(x, turn, 1)
                got = jnp.where(part == s, x, got)
            parts.append(got)
        return parts

    def unpack3(kind, dest, add=None):
        for t in range(2):
            slots = [win3[kind, 4 * t + k] for k in range(4)]
            zb = zall // 4
            for j, x in enumerate(unpack(slots, n3)):
                if add is not None:
                    x = x + add(j * zb, zb)
                dest[t, j * zb : (j + 1) * zb] = x

    def unpack4(kind, dest, add=None):
        for t in range(2):
            slots = [win4[kind, r] for r in range(8 * t, min(8 * t + 8, 9))]
            zb = zall // 8
            for j, x in enumerate(unpack(slots, n4)):
                if add is not None:
                    x = x + add(j * zb, zb)
                dest[t, j * zb : (j + 1) * zb] = x

    rawr = raw_r.reshape(zall * r0, n0)
    raws = raw_s.reshape(zall * r0, n0)
    staged = stage.reshape(zall * r0, n0)

    def unfold(raw, j):
        at = pl.ds(pl.multiple_of(PAD * r0 * j, PAD * r0), PAD * r0)
        for t in range(nt0):
            turn[t, at, :] = raw[at, 128 * t : 128 * (t + 1)]
    raw_r[pl.ds(depth * me, depth)] = reaction[:, pl.ds(r0 * p, r0), :]
    raw_s[pl.ds(depth * me, depth)] = source[:, pl.ds(r0 * p, r0), :]
    vrecv[me] = vsend[...]
    group = PAD // depth

    def each_rows(landed, body):
        def step(i):
            j = (me // group + i) % (zall // PAD)
            for k in range(group if landed is not None else 0):
                s = group * j + k

                @pl.when(s != me)
                def _():
                    landed(s)
            body(j)
        loop(0, zall // PAD, step)

    landed_v(None)
    for s in range(nd):
        lines[depth * s : depth * (s + 1), :] = vrecv[s]

    def take_r(j):
        z = pl.multiple_of(PAD * j, PAD)
        unfold(rawr, j)
        for x in range(r0):
            for t in range(nt0):
                d0[x + 1, pl.ds(z, PAD), 128 * t : 128 * (t + 1)] = turn[
                    t, pl.ds(PAD * r0 * j + x, PAD, stride=r0), :]

    landed_r(None)
    each_rows(None, take_r)

    def shrink_r(i):
        for r in range(0, zall, CROWS):
            at = pl.ds(r, CROWS)
            a, b = d0[2 * i + 1, at, :], d0[2 * i + 2, at, :]
            got = dot_parts(a + b, downy[...], 3)
            vert = lines[at, :]
            base = 2.0 * vert + 4.0 * h[1]
            w1[i + 2, at, :] = got
            d = base + got
            d1[i + 2, at, :] = d
            base = jnp.concatenate([2.0 * vert + 4.0 * h[0]] * nt0, axis=1)
            for k, x in ((1, a), (2, b)):
                x = base + x
                d0[2 * i + k, at, :] = x
                w0[2 * i + k, at, :] = DAMPING / x

    loop(0, r1, shrink_r)
    begin_d0, end_d0 = halo_d0()
    begin_d0()
    begin_d1, end_d1 = planes1(d1, 6)
    begin_d1()
    rx2 = dot_parts(jnp.concatenate([w1[2] + w1[3], w1[4] + w1[5]], axis=1), downy[...], 3)
    dx[1] = rx2
    begin_dx, end_dx = blocks(dx, 7)
    begin_dx()
    rx3 = dot_parts(rx2, down3[...], 3)
    win3[CYCLES, 3 + par] = pack(rx3, n3)
    begin_w3, end_w3 = window3(CYCLES)
    begin_w3()
    begin_w4, end_w4 = window4(CYCLES)
    loop(2, r1 + 2, lambda x: w1.__setitem__(x, DAMPING / d1[x]))

    def take_s(j):
        z = pl.multiple_of(PAD * j, PAD)
        unfold(raws, j)
        for x in range(r0):
            for t in range(nt0):
                cut = slice(128 * t, 128 * (t + 1))
                got = turn[t, pl.ds(PAD * r0 * j + x, PAD, stride=r0), :]
                g0[x + 1, pl.ds(z, PAD), cut] = got
                v0[0, x + 2, pl.ds(z + PAD, PAD), cut] = w0[x + 1, pl.ds(z, PAD), cut] * got

    each_rows(landed_s, take_s)

    ns = (zall - 1).bit_length()

    def factors(f):
        vert = lines[...]
        a = jnp.where(rows == 0, 0.0, -vert)
        c = jnp.where(rows == zall - 1, 0.0, -vert)
        b = diag[f]
        for k in range(ns):
            s = 1 << k
            inv = 1.0 / b
            alpha = -a * pltpu.roll(inv, s, 0)
            gamma = -c * pltpu.roll(inv, zall - s, 0)
            b = b + alpha * pltpu.roll(c, s, 0) + gamma * pltpu.roll(a, zall - s, 0)
            a = alpha * pltpu.roll(a, s, 0)
            c = gamma * pltpu.roll(c, zall - s, 0)
            fac[f, 2 * k] = alpha
            fac[f, 2 * k + 1] = gamma
        fac[f, 2 * ns] = mask[f] / b

    def solve(f, right):
        for k in range(ns):
            s = 1 << k
            right = (
                right
                + fac[f, 2 * k] * pltpu.roll(right, s, 0)
                + fac[f, 2 * k + 1] * pltpu.roll(right, zall - s, 0)
            )
        return right * fac[f, 2 * ns]

    def near(v, q, b, width):
        t = v[q, b]
        below = pltpu.roll(jnp.where(lane >= 128 - width, v[q, b - 1], t), width, 1)
        above = pltpu.roll(jnp.where(lane < width, v[q, b + 1], t), 128 - width, 1)
        inrow = lane % width
        left = jnp.where(inrow == 0, 0.0, pltpu.roll(t, 1, 1))
        right = jnp.where(inrow == width - 1, 0.0, pltpu.roll(t, 127, 1))
        return (below + above) + (left + right)

    edge = lax.broadcasted_iota(jnp.int32, (CROWS, 128), 1)
    level0 = (v0, g0, w0, d0, nt0, h[0], 1)
    level1 = (v1, g1, w1, d1, 1, h[1], 2)

    def stencil(level, m, x, r):
        v, g, w, d, nt, weight, go = level
        centre, turn_r, turn_l = [], [], []
        for t in range(nt):
            cut = slice(128 * t, 128 * (t + 1))
            c = v[m, x + 2, PAD + r : PAD + r + CROWS, cut]
            centre.append(c)
            turn_r.append(pltpu.roll(c, 1, 1))
            turn_l.append(pltpu.roll(c, 127, 1))
        vert = lines[r : r + CROWS, :]
        got = []
        for t in range(nt):
            cut = slice(128 * t, 128 * (t + 1))
            left = jnp.where(edge == 0, turn_r[t - 1] if t else 0.0, turn_r[t])
            right = jnp.where(edge == 127, turn_l[t + 1] if t + 1 < nt else 0.0, turn_l[t])
            side = (v[m, x + 1, PAD + r : PAD + r + CROWS, cut] + v[m, x + 3, PAD + r : PAD + r + CROWS, cut]) + (left + right)
            if weight != 1.0:
                side = weight * side
            ends = v[m, x + 2, PAD + r - 1 : PAD + r - 1 + CROWS, cut] + v[m, x + 2, PAD + r + 1 : PAD + r + 1 + CROWS, cut]
            got.append(g[x + go, r : r + CROWS, cut] + side + vert * ends)
        return centre, got

    def sweep_plane(level, m, q, x, record=None, put=None):
        v, g, w, d, nt, weight, go = level
        for r in range(0, zall, CROWS):
            centre, got = stencil(level, m, x, r)
            for t in range(nt):
                cut = slice(128 * t, 128 * (t + 1))
                wt = w[x + go, r : r + CROWS, cut]
                if record is None:
                    new = (1.0 - DAMPING) * centre[t] + wt * got[t]
                else:
                    res = got[t] - d[x + go, r : r + CROWS, cut] * centre[t]
                    new = centre[t] + wt * res
                    acc[record] += (res * res).reshape(CROWS // 8, 8, 128).sum(axis=0)
                v[q, x + 2, PAD + r : PAD + r + CROWS, cut] = new
                if put is not None:
                    for e in range(0, CROWS, 8):
                        put(x, r + e, t, new[e : e + 8])

    def residual(level, m, x, r):
        v, g, w, d, nt, weight, go = level
        centre, got = stencil(level, m, x, r)
        res = [
            got[t] - d[x + go, r : r + CROWS, 128 * t : 128 * (t + 1)] * centre[t] for t in range(nt)]
        return res

    def sweeps(level, m, q, xs, record=None, put=None):
        lo, hi, fn = xs
        loop(lo, hi, lambda i: sweep_plane(level, m, q, fn(i), record, put))

    def restrict0(m, lo, hi, fn):
        def body(i):
            i = fn(i)
            for r in range(0, zall, CROWS):
                a = residual(level0, m, 2 * i, r)
                b = residual(level0, m, 2 * i + 1, r)
                both = jnp.concatenate([s + t for s, t in zip(a, b)], axis=1)
                g1[i + 2, r : r + CROWS, :] = dot_parts(both, downy[...])
        loop(lo, hi, body)

    def same(i):
        return i

    def rim(size, wide):
        return lambda i: i + (i // wide) * (size - 2 * wide)

    def outer(size):
        return lambda i: -1 + i * (size + 1)

    def pair0(m, q, record=None, hook=None, put=None, restrict=False, before=None):
        begin, end = planes0(m, 2)
        begin()
        if before is not None:
            before()
        if hook is not None:
            hook[0]()
        sweeps(level0, m, 1, (1, r0 - 1, same), record)
        if restrict:
            restrict0(1, 1, r1 - 1, same)
        else:
            sweeps(level0, 1, q, (2, r0 - 2, same), None, put)
        end()
        if hook is not None:
            hook[1]()
        sweeps(level0, m, 1, (0, 2, outer(r0)))
        sweeps(level0, m, 1, (0, 2, rim(r0, 1)), record)
        if restrict:
            restrict0(1, 0, 2, lambda i: i * (r1 - 1))
        else:
            sweeps(level0, 1, q, (0, 4, rim(r0, 2)), None, put)

    def halo_factors():
        end_dx()
        for t in range(3):
            diag[t] = 2.0 * lines[...] + 4.0 * h[2] + dx[t]
        loop(0, 3, factors)
        end_w3()
        unpack3(CYCLES, g3)
        win4[CYCLES, 4] = pack(
            dot_parts(g3[0], down4[0], 3) + dot_parts(g3[1], down4[1], 3), n4)
        begin_w4()

    def window_factors():
        def add(level):
            return lambda r, n: 2.0 * lines[r : r + n, :] + 4.0 * h[level]
        for t in range(2):
            diag[3 + t] = 2.0 * lines[...] + 4.0 * h[3] + g3[t]
        loop(3, 5, factors)
        end_w4()
        unpack4(CYCLES, diag.at[pl.ds(5, 2)], add(4))
        loop(5, 7, factors)

    def halo_level0():
        end_d0()
        for x, inside in ((0, jnp.logical_not(first)), (r0 + 1, jnp.logical_not(last))):
            @pl.when(inside)
            def _(x=x):
                w0[x] = DAMPING / d0[x]
            g0[x] = v0[0, x + 1, PAD : PAD + zall, :] * d0[x] * (1.0 / DAMPING)

    def halo_level1():
        end_d1()
        for x, inside in ((0, jnp.logical_not(first)), (r1 + 2, jnp.logical_not(last))):
            @pl.when(inside)
            def _(x=x):
                for q in range(2):
                    w1[x + q] = DAMPING / d1[x + q]

    def coarse(cycle):
        begin, end = planes1(g1, 3)
        begin()
        if cycle == 0:
            window_factors()
        loop(2, r1 + 2, lambda x: v1.__setitem__((0, x, pl.ds(PAD, zall)), w1[x] * g1[x]))
        end()
        if cycle == 0:
            halo_level1()
        for x in (0, 1, r1 + 2, r1 + 3):
            v1[0, x, PAD : PAD + zall] = w1[x] * g1[x]
        sweeps(level1, 0, 1, (-1, r1 + 1, same))

        pairs = []
        for i in range(r1 // 2):
            cuts = []
            for r in range(0, zall, CROWS):
                a = residual(level1, 1, 2 * i, r)[0]
                b = residual(level1, 1, 2 * i + 1, r)[0]
                cuts.append(a + b)
            pairs.append(jnp.concatenate(cuts, axis=0))
        gx[cycle, 1] = dot_parts(jnp.concatenate(pairs, axis=1), downy[...])
        e2 = lines2(cycle)

        for i in range(r1 // 2):
            e = dot_parts(e2, up2[i])
            for x in (2 * i, 2 * i + 1):
                v1[2, x + 2, PAD : PAD + zall] = v1[1, x + 2, PAD : PAD + zall] + e
        begin, end = planes1v(2)
        begin()
        sweeps(level1, 2, 1, (1, r1 - 1, same))
        end()
        sweeps(level1, 2, 1, (0, 2, outer(r1)))
        sweeps(level1, 2, 1, (0, 2, rim(r1, 1)))
        sweeps(level1, 1, 0, (0, r1, same))

    def lines_sweep(v, q, s, lo, hi, right, f, weight, width):
        loop(lo, hi, lambda b: v.__setitem__(
            (s, b), solve(f + b - 1, right[b - 1] + weight * near(v, q, b, width))))

    def line_residual(v, q, b, right, f, weight, width):
        values = v[q, b]
        before = jnp.where(rows == 0, 0.0, pltpu.roll(values, 1, 0))
        after = jnp.where(rows == zall - 1, 0.0, pltpu.roll(values, zall - 1, 0))
        return right[b - 1] + weight * near(v, q, b, width) + lines[...] * (before + after) - diag[f + b - 1] * values

    def lines2(cycle):
        right = gx.at[cycle]
        begin, end = blocks(right, 8)
        begin()
        v2[0, 2] = solve(1, right[1])
        end()
        loop(0, 2, lambda i: v2.__setitem__((0, 1 + 2 * i), solve(2 * i, right[2 * i])))
        lines_sweep(v2, 0, 1, 1, 4, right, 0, h[2], n2)
        res = line_residual(v2, 1, 2, right, 0, h[2], n2)
        win3[cycle, 3 + par] = pack(dot_parts(res, down3[...]), n3)
        e3 = lines3(cycle)
        cx[cycle, 1] = v2[1, 2] + dot_parts(e3, up3[par])
        begin, end = blocks(cx.at[cycle], 9)
        begin()
        end()
        for b in range(3):
            v2[0, b + 1] = cx[cycle, b]
        lines_sweep(v2, 0, 1, 1, 4, right, 0, h[2], n2)
        return solve(1, right[1] + h[2] * near(v2, 1, 2, n2))

    def lines3(cycle):
        begin, end = window3(cycle)
        begin()
        end()
        unpack3(cycle, g3)
        loop(1, 3, lambda b: v3.__setitem__((0, b), solve(3 + b - 1, g3[b - 1])))
        lines_sweep(v3, 0, 1, 1, 3, g3, 3, h[3], n3)
        both = None
        for t in range(2):
            part = dot_parts(line_residual(v3, 1, t + 1, g3, 3, h[3], n3), down4[t])
            both = part if both is None else both + part
        win4[cycle, 4] = pack(both, n4)
        e4 = lines4(cycle)
        for t in range(2):
            v3[0, t + 1] = v3[1, t + 1] + dot_parts(e4, up4[t])
        lines_sweep(v3, 0, 1, 1, 3, g3, 3, h[3], n3)
        return solve(3 + par, g3[par] + h[3] * near(v3, 1, 1 + par, n3))

    def lines4(cycle):
        begin, end = window4(cycle)
        begin()
        end()
        unpack4(cycle, g4)
        loop(1, 3, lambda b: v4.__setitem__((0, b), solve(5 + b - 1, g4[b - 1])))
        q = 0
        for k in range(1, COARSE - 1):
            v4[1 - q, 1] = solve(5, g4[0] + h[4] * near(v4, q, 1, n4))
            q = 1 - q
        return solve(5, g4[0] + h[4] * near(v4, q, 1, n4))

    def correct0(m, q, lo, hi, fn):
        def body(i):
            i = fn(i)
            for r in range(0, zall, CROWS):
                e = dot_parts(v1[0, i + 2, PAD + r : PAD + r + CROWS, :], upy[...])
                for x in (2 * i + 2, 2 * i + 3):
                    v0[q, x, PAD + r : PAD + r + CROWS, :] = v0[m, x, PAD + r : PAD + r + CROWS, :] + e
        loop(lo, hi, body)

    def put(x, z, t, value):
        turn[t, pl.ds(z * r0 + x, 8, stride=r0), :] = value

    def fold(j):
        at = pl.ds(pl.multiple_of(PAD * r0 * j, PAD * r0), PAD * r0)
        for t in range(nt0):
            staged[at, 128 * t : 128 * (t + 1)] = turn[t, at, :]

    pair0(0, 1, hook=(halo_factors, halo_level0), restrict=True)
    coarse(0)
    correct0(1, 2, 0, 2, lambda i: i * (r1 - 1))
    pair0(2, 0, before=lambda: correct0(1, 2, 1, r1 - 1, same))
    pair0(0, 2, record=0)
    begin, end = planes0(2, 1)
    begin()
    restrict0(2, 1, r1 - 1, same)
    end()
    restrict0(2, 0, 2, lambda i: i * (r1 - 1))
    coarse(1)
    correct0(2, 0, 0, 2, lambda i: i * (r1 - 1))
    pair0(0, 2, put=put, before=lambda: correct0(2, 0, 1, r1 - 1, same))
    loop(0, zall // PAD, fold)
    begin, end = planes0(2, 1)
    begin()
    start_o()
    keep = pltpu.make_async_copy(zrows(stage, me), piece(out, p), load.at[2])
    keep.start()

    def last_norm(x):
        for r in range(0, zall, CROWS):
            for res in residual(level0, 2, x, r):
                acc[CYCLES - 1] += (res * res).reshape(CROWS // 8, 8, 128).sum(axis=0)

    loop(1, r0 - 1, last_norm)
    end()
    loop(0, 2, lambda i: last_norm(i * (r0 - 1)))
    ridx = lax.broadcasted_iota(jnp.int32, (8, 128), 0)
    part = jnp.zeros((8, 128), f32)
    for k in range(CYCLES):
        part = jnp.where(ridx == k, jnp.sum(acc[k]), part)
    nsend[...] = part
    start_n()
    total = part
    done_v()
    done_r()
    done_s()

    def finish(s):
        @pl.when(s != me)
        def _():
            landed_o(s)
    loop(0, nd, finish)
    landed_n(None)
    nrecv[me] = part
    total = jnp.sum(nrecv[...], axis=0)
    for k in range(CYCLES):
        norms[k] = total[k, 0] * (1.0 / (zall * n0 * n0))
    keep.wait()
    done_o()
    done_n()


def chain_shards(gz, gy, source, vertical, reaction):
    depth, n0 = source.shape[0], source.shape[1]
    nd = gz * gy
    zall = nd * depth
    n1, n2, n3, n4 = n0 // 2, n0 // 4, n0 // 8, n0 // 16
    r0, r1 = n0 // nd, n1 // nd
    f32 = jnp.float32
    bf16 = jnp.bfloat16

    hbm = pl.BlockSpec(memory_space=pl.ANY)
    sm = pl.BlockSpec(memory_space=pltpu.SMEM)
    ns = (zall - 1).bit_length()
    dma = pltpu.SemaphoreType.DMA
    solution, norms = pl.pallas_call(
        functools.partial(chain_kernel, (gz, gy, depth)),
        out_shape=(
            jax.ShapeDtypeStruct(source.shape, f32),
            jax.ShapeDtypeStruct((CYCLES,), f32),
        ),
        in_specs=[pl.BlockSpec(memory_space=pltpu.HBM)] * 2 + [sm],
        out_specs=(hbm, sm),
        scratch_shapes=[
            pltpu.VMEM(source.shape, f32),
            pltpu.VMEM(source.shape, f32),
            pltpu.VMEM((n0, n1), bf16),
            pltpu.VMEM((n1, n0), bf16),
            pltpu.VMEM((r1 // 2, 128, n1), bf16),
            pltpu.VMEM((128, 128), bf16),
            pltpu.VMEM((2, 128, 128), bf16),
            pltpu.VMEM((2, 128, 128), bf16),
            pltpu.VMEM((2, 128, 128), bf16),
            pltpu.SemaphoreType.DMA((3,)),
            pltpu.VMEM((3, r0 + 4, zall + 2 * PAD, n0), f32),
            pltpu.VMEM((r0 + 2, zall, n0), f32),
            pltpu.VMEM((r0 + 2, zall, n0), f32),
            pltpu.VMEM((r0 + 2, zall, n0), f32),
            pltpu.VMEM((3, r1 + 4, zall + 2 * PAD, n1), f32),
            pltpu.VMEM((r1 + 4, zall, n1), f32),
            pltpu.VMEM((r1 + 4, zall, n1), f32),
            pltpu.VMEM((r1 + 4, zall, n1), f32),
            pltpu.VMEM((zall, r0, n0), f32),
            pltpu.VMEM((zall, r0, n0), f32),
            pltpu.VMEM((zall, r0, n0), f32),
            pltpu.VMEM((n0 // 128, zall * r0, 128), f32),
            pltpu.VMEM((zall, 128), f32),
            pltpu.VMEM((depth, 128), f32),
            pltpu.VMEM((nd, depth, 128), f32),
            pltpu.VMEM((CYCLES, 3, zall, 128), f32),
            pltpu.VMEM((CYCLES, 3, zall, 128), f32),
            pltpu.VMEM((3, zall, 128), f32),
            pltpu.VMEM((CYCLES + 1, 8, n3 * zall // 128, 128), f32),
            pltpu.VMEM((CYCLES + 1, 9, n4 * zall // 128, 128), f32),
            pltpu.VMEM((2, 5, zall, 128), f32),
            pltpu.VMEM((2, 4, zall, 128), f32),
            pltpu.VMEM((2, 4, zall, 128), f32),
            pltpu.VMEM((2, zall, 128), f32),
            pltpu.VMEM((2, zall, 128), f32),
            pltpu.VMEM((7, zall, 128), f32),
            pltpu.VMEM((7, 2 * ns + 1, zall, 128), f32),
            pltpu.VMEM((7, zall, 128), f32),
            pltpu.VMEM((CYCLES, 8, 128), f32),
            pltpu.VMEM((8, 128), f32),
            pltpu.VMEM((nd, 8, 128), f32),
            dma((5,)),
            dma((5,)),
            dma((nd,)),
            dma((10, 2)),
            dma((10, 2)),
            dma((10,)),
            dma((2, 8)),
            dma((9,)),
            dma((2, 9)),
        ],
        compiler_params=pltpu.CompilerParams(
            has_side_effects=True, vmem_limit_bytes=VMEM_LIMIT
        ),
    )(source, reaction, vertical)
    return solution, norms


def shards_of(gz, gy, source, vertical, reaction):
    depth, n0 = source.shape[0], source.shape[1]
    nd = gz * gy
    fits = (
        gz % 2 == 0 and n0 % (8 * nd) == 0 and n0 // nd == 8 and n0 % 256 == 0 and n0 // 4 * 2 == 128
        and PAD % depth == 0 and nd * depth % 128 == 0 and (LEVELS, SWITCH, SWEEPS, COARSE, CYCLES) == (5, 2, 2, 4, 2)
    )
    return (chain_shards if fits else shards)(gz, gy, source, vertical, reaction)


def solution(mesh):
    return jax.shard_map(
        functools.partial(shards_of, mesh.shape["gz"], mesh.shape["gy"]),
        mesh=mesh,
        in_specs=(P(("gz", "gy"), None, None), P(("gz", "gy")), P(("gz", "gy"), None, None)),
        out_specs=(P(("gz", "gy"), None, None), P()),
        check_vma=False,
    )
```

```python
import functools

import jax
import jax.numpy as jnp
import numpy as np
from jax import lax
from jax.experimental import pallas as pl
from jax.experimental.pallas import tpu as pltpu
from jax.sharding import PartitionSpec as P

LEVELS = 5
SWITCH = 2
CYCLES = 2
SWEEPS = 2
COARSE = 4
DAMPING = 0.8
COUPLING = 1.0
CHUNK = 32
MESH = pl.DeviceIdType.MESH


def dot(a, b):
    return lax.dot_general(
        a,
        b,
        (((1,), (0,)), ((), ())),
        precision=lax.Precision.HIGHEST,
        preferred_element_type=jnp.float32,
    )


def parts_of(x):
    first = x.astype(jnp.bfloat16)
    rest = x - first.astype(jnp.float32)
    second = rest.astype(jnp.bfloat16)
    third = (rest - second.astype(jnp.float32)).astype(jnp.bfloat16)
    return (third, second, first)


def dot_right(x, m):
    m = m.astype(jnp.bfloat16)
    total = None
    for x in parts_of(x):
        term = jnp.dot(x, m, preferred_element_type=jnp.float32)
        total = term if total is None else total + term
    return total


def dot_left(m, x):
    m = m.astype(jnp.bfloat16)
    total = None
    for x in parts_of(x):
        term = jnp.dot(m, x, preferred_element_type=jnp.float32)
        total = term if total is None else total + term
    return total


def kernel(
    dims,
    source, reaction, vert_s, vert_b, down0, downt0, down1, cols, mask, group, ups, groupt, colst,
    out, norms,
    v0, v1, w0, d1, w1, g1, r1, tmp0, res1, corr1, send_a, recv_a, send_v, recv_v, recv_b,
    send_n, recv_n, lines, diag, factor, target, around, halo, rowbuf, acc,
    plane_send, plane_recv, line_send, line_recv, a2a_send, a2a_recv,
):
    gz, gy, depth, cp = dims
    nd = gz * gy
    zall = nd * depth
    n0 = source.shape[1]
    n1 = n0 // 2
    a_me = lax.axis_index("gz")
    b_me = lax.axis_index("gy")
    me = a_me * gy + b_me
    h = [COUPLING / 4.0**k for k in range(LEVELS)]

    @pl.when(me == 0)
    def _():
        for p in range(2):
            v0[p, 0] = jnp.zeros((n0, n0), jnp.float32)
            v1[p, 0] = jnp.zeros((n1, n1), jnp.float32)

    @pl.when(me == nd - 1)
    def _():
        for p in range(2):
            v0[p, depth + 1] = jnp.zeros((n0, n0), jnp.float32)
            v1[p, depth + 1] = jnp.zeros((n1, n1), jnp.float32)

    edges = [a_me == 0, a_me == gz - 1, b_me == 0, b_me == gy - 1]
    for k in range(4):
        @pl.when(edges[k])
        def _(k=k):
            for p in range(2):
                halo[p, k] = jnp.zeros((zall, cp), jnp.float32)

    def flat(d):
        return (d // gy, d % gy)

    def plane_copy(v, p, level, up):
        if up:
            src, dst, to = v.at[p, depth], v.at[p, 0], flat(me + 1)
        else:
            src, dst, to = v.at[p, 1], v.at[p, depth + 1], flat(me + nd - 1 - nd * ((me + nd - 1) // nd))
        if up:
            to = flat((me + 1) % nd)
        k = 0 if up else 1
        return pltpu.make_async_remote_copy(
            src_ref=src, dst_ref=dst,
            send_sem=plane_send.at[level, p, k], recv_sem=plane_recv.at[level, p, k],
            device_id=to, device_id_type=MESH,
        )

    def plane_start(v, p, level):
        @pl.when(me < nd - 1)
        def _():
            plane_copy(v, p, level, True).start()

        @pl.when(me > 0)
        def _():
            plane_copy(v, p, level, False).start()

    def plane_wait(v, p, level):
        @pl.when(me < nd - 1)
        def _():
            plane_copy(v, p, level, True).wait_send()
            plane_copy(v, p, level, False).wait_recv()

        @pl.when(me > 0)
        def _():
            plane_copy(v, p, level, False).wait_send()
            plane_copy(v, p, level, True).wait_recv()

    def residual_chunk(v, p, z, r, n, target_ref, diag_of, weight):
        centre = v[p, z, pl.ds(r, CHUNK), :]
        rows = lax.broadcasted_iota(jnp.int32, (CHUNK, n), 0)
        lanes = lax.broadcasted_iota(jnp.int32, (CHUNK, n), 1)
        if r == 0:
            above = jnp.where(rows == 0, 0.0, pltpu.roll(centre, 1, 0))
        else:
            above = v[p, z, pl.ds(r - 1, CHUNK), :]
        if r + CHUNK == n:
            below = jnp.where(rows == CHUNK - 1, 0.0, pltpu.roll(centre, CHUNK - 1, 0))
        else:
            below = v[p, z, pl.ds(r + 1, CHUNK), :]
        left = jnp.where(lanes == 0, 0.0, pltpu.roll(centre, 1, 1))
        right = jnp.where(lanes == n - 1, 0.0, pltpu.roll(centre, n - 1, 1))
        vert = vert_s[z - 1]
        applied = (
            diag_of(z - 1, r, vert) * centre
            - vert * (v[p, z - 1, pl.ds(r, CHUNK), :] + v[p, z + 1, pl.ds(r, CHUNK), :])
            - weight * (above + below + left + right)
        )
        return centre, target_ref[z - 1, pl.ds(r, CHUNK), :] - applied

    def diag0(z, r, vert):
        return 2.0 * vert + 4.0 * h[0] + reaction[z, pl.ds(r, CHUNK), :]

    def diag1(z, r, vert):
        return d1[z, pl.ds(r, CHUNK), :]

    def over_planes(v, p, level, body):
        plane_start(v, p, level)

        def inner(z, c):
            body(z)
            return c

        lax.fori_loop(2, depth, inner, 0)
        plane_wait(v, p, level)

        def outer(i, c):
            body(1 + i * (depth - 1))
            return c

        lax.fori_loop(0, 2, outer, 0)

    def level_parts(level):
        if level == 0:
            return v0, source, diag0, w0, n0
        return v1, g1, diag1, w1, n1

    def sweep(level, p, record=None):
        v, tgt, dg, w, n = level_parts(level)

        def body(z):
            for r in range(0, n, CHUNK):
                centre, res = residual_chunk(v, p, z, r, n, tgt, dg, h[level])
                v[1 - p, z, pl.ds(r, CHUNK), :] = centre + w[z - 1, pl.ds(r, CHUNK), :] * res
                if record is not None:
                    sq = (res * res).reshape(CHUNK // 8, 8, n).sum(axis=0)
                    acc[record, :, :] += sq

        over_planes(v, p, level, body)
        return 1 - p

    def first_sweep(level):
        v, tgt, dg, w, n = level_parts(level)

        def body(z, c):
            v[0, z + 1] = w[z] * tgt[z]
            return c

        lax.fori_loop(0, depth, body, 0)
        return 0

    def restrict0(read_chunk, store):
        def body(z):
            for r in range(0, n0, CHUNK):
                tmp0[pl.ds(r, CHUNK), :] = dot_right(read_chunk(z, r), downt0[...])
            store(z, dot_left(down0[...], tmp0[...]))
        return body

    def restrict1(z, plane):
        half = dot(down1[...], plane)
        for b in range(gy):
            spread = dot(half, cols[b]) * mask[...]
            packed = dot(group[...], spread)
            for a in range(gz):
                send_a[b, a, z : z + 1, :] = packed[a : a + 1, :]

    def exchange_all(kind, src_of, recv):
        def copy(k):
            dst = (me + k) % nd
            a, b = dst // gy, dst % gy
            return pltpu.make_async_remote_copy(
                src_ref=src_of(a, b), dst_ref=recv.at[b_me, a_me],
                send_sem=a2a_send.at[kind, k], recv_sem=a2a_recv.at[kind, me],
                device_id=(a, b), device_id_type=MESH,
            )

        def start(k, c):
            copy(k).start()
            return c

        def finish(k, c):
            copy(k).wait_send()
            src = (me + k) % nd
            a, b = src // gy, src % gy
            pltpu.make_async_remote_copy(
                src_ref=recv.at[b, a], dst_ref=recv.at[b, a],
                send_sem=a2a_send.at[kind, k], recv_sem=a2a_recv.at[kind, src],
                device_id=(a, b), device_id_type=MESH,
            ).wait_recv()
            return c

        def begin():
            lax.fori_loop(1, nd, start, 0)

        def end():
            lax.fori_loop(1, nd, finish, 0)

        return begin, end

    def to_lines(recv, dest):
        for a in range(gz):
            for b in range(gy):
                s = (a * gy + b) * depth
                dest[s : s + depth, :] = recv[b, a]

    bx2, by2 = (n1 // 2 // gz, n1 // 2 // gy)
    steps = []
    s = 1
    while s < zall:
        steps.append(s)
        s *= 2
    ns = len(steps)

    def setup_lines(offset):
        rows = lax.broadcasted_iota(jnp.int32, (zall, cp), 0)
        vert = lines[...]
        a = jnp.where(rows == 0, 0.0, -vert)
        c = jnp.where(rows == zall - 1, 0.0, -vert)
        b = diag[offset]
        for k, s in enumerate(steps):
            alpha = -a / pltpu.roll(b, s, 0)
            gamma = -c / pltpu.roll(b, zall - s, 0)
            b = b + alpha * pltpu.roll(c, s, 0) + gamma * pltpu.roll(a, zall - s, 0)
            a = alpha * pltpu.roll(a, s, 0)
            c = gamma * pltpu.roll(c, zall - s, 0)
            factor[offset, 2 * k] = alpha
            factor[offset, 2 * k + 1] = gamma
        factor[offset, 2 * ns] = 1.0 / b

    def solve(offset, right):
        for k, s in enumerate(steps):
            right = (
                right
                + factor[offset, 2 * k] * pltpu.roll(right, s, 0)
                + factor[offset, 2 * k + 1] * pltpu.roll(right, zall - s, 0)
            )
        return right * factor[offset, 2 * ns]

    count = [0]
    def line_copy(p, k):
        if k == 0:
            to, slot = ((a_me + gz - 1) % gz, b_me), 1
        elif k == 1:
            to, slot = ((a_me + 1) % gz, b_me), 0
        elif k == 2:
            to, slot = (a_me, (b_me + gy - 1) % gy), 3
        else:
            to, slot = (a_me, (b_me + 1) % gy), 2
        return pltpu.make_async_remote_copy(
            src_ref=around.at[p], dst_ref=halo.at[p, slot],
            send_sem=line_send.at[p, k], recv_sem=line_recv.at[p, slot],
            device_id=to, device_id_type=MESH,
        )

    def line_landed(p, k):
        return pltpu.make_async_remote_copy(
            src_ref=around.at[p], dst_ref=halo.at[p, k],
            send_sem=line_send.at[p, k], recv_sem=line_recv.at[p, k],
            device_id=(a_me, b_me), device_id_type=MESH,
        )

    def neighbours(offset, values):
        bx, by = bx2 >> offset, by2 >> offset
        cells = bx * by
        p = count[0] % 2
        count[0] += 1
        around[p] = values
        for k in range(4):
            @pl.when(jnp.logical_not(edges[k]))
            def _(k=k):
                line_copy(p, k).start()
        for k in range(4):
            @pl.when(jnp.logical_not(edges[k]))
            def _(k=k):
                line_copy(p, k).wait_send()
                line_landed(p, k).wait_recv()
        lane = lax.broadcasted_iota(jnp.int32, (zall, cp), 1)

        def roll(x, amount):
            amount = amount % cp
            return x if amount == 0 else pltpu.roll(x, amount, 1)

        total = jnp.where(lane < by, roll(halo[p, 0], by - cells), roll(values, by))
        total += jnp.where(lane >= cells - by, roll(halo[p, 1], cells - by), roll(values, -by))
        inrow = lane & (by - 1)
        total += jnp.where(inrow == 0, roll(halo[p, 2], 1 - by), roll(values, 1))
        total += jnp.where(inrow == by - 1, roll(halo[p, 3], by - 1), roll(values, -1))
        return total

    def line_descend(offset):
        weight = h[SWITCH + offset]
        values = solve(offset, target[offset])
        repeats = COARSE if offset == LEVELS - 1 - SWITCH else SWEEPS
        for _ in range(1, repeats):
            values = solve(offset, target[offset] + weight * neighbours(offset, values))
        if offset == LEVELS - 1 - SWITCH:
            return values
        near = neighbours(offset, values)
        rows = lax.broadcasted_iota(jnp.int32, (zall, cp), 0)
        before = jnp.where(rows == 0, 0.0, pltpu.roll(values, 1, 0))
        after = jnp.where(rows == zall - 1, 0.0, pltpu.roll(values, zall - 1, 0))
        res = target[offset] - (
            diag[offset] * values - lines[...] * (before + after) - weight * near
        )
        target[offset + 1] = dot(res, ups[2 * offset])
        tmp = values
        lower = line_descend(offset + 1)
        values = tmp + dot(lower, ups[2 * offset + 1])
        for _ in range(SWEEPS):
            values = solve(offset, target[offset] + weight * neighbours(offset, values))
        return values

    def fill0(z, c):
        w0[z] = DAMPING / (2.0 * vert_s[z] + 4.0 * h[0] + reaction[z])
        return c

    lax.fori_loop(0, depth, fill0, 0)

    def keep_r1(z, value):
        r1[z] = value
        dv = 2.0 * vert_s[z] + 4.0 * h[1] + value
        d1[z] = dv
        w1[z] = DAMPING / dv

    body = restrict0(lambda z, r: reaction[z, pl.ds(r, CHUNK), :], keep_r1)
    lax.fori_loop(0, depth, lambda z, c: (body(z), c)[1], 0)
    for z in range(depth):
        restrict1(z, r1[z])
    send_v[...] = send_a[...]
    begin_v, end_v = exchange_all(0, lambda a, b: vert_b, recv_v)
    begin_r, end_r = exchange_all(1, lambda a, b: send_v.at[b, a], recv_a)
    begin_v()
    begin_r()
    recv_v[b_me, a_me] = vert_b[...]
    recv_a[b_me, a_me] = send_v[b_me, a_me]
    acc[...] = jnp.zeros_like(acc)

    begin_a, end_a = exchange_all(2, lambda a, b: send_a.at[b, a], recv_b.at[0])
    begin_b, end_b = exchange_all(3, lambda a, b: send_n.at[b, a], recv_b.at[1])

    p0 = first_sweep(0)
    for cycle in range(CYCLES):
        for k in range(SWEEPS):
            if cycle == 0 and k == 0:
                continue
            p0 = sweep(0, p0, record=cycle - 1 if cycle > 0 and k == 0 else None)

        def read0(z, r, p0=p0):
            return residual_chunk(v0, p0, z, r, n0, source, diag0, h[0])[1]

        def keep_g1(z, value):
            g1[z - 1] = value

        over_planes(v0, p0, 0, restrict0(read0, keep_g1))
        p1 = first_sweep(1)
        for k in range(1, SWEEPS):
            p1 = sweep(1, p1)

        def keep_res(z, p1=p1):
            for r in range(0, n1, CHUNK):
                res1[z - 1, pl.ds(r, CHUNK), :] = residual_chunk(
                    v1, p1, z, r, n1, g1, diag1, h[1]
                )[1]

        over_planes(v1, p1, 1, keep_res)
        for z in range(depth):
            restrict1(z, res1[z])
        begin_a()
        recv_b[0, b_me, a_me] = send_a[b_me, a_me]
        if cycle == 0:
            end_v()
            end_r()
            to_lines(recv_v, lines)
            to_lines(recv_a, target.at[0])
            coarse = target[0]
            for offset in range(LEVELS - SWITCH):
                if offset > 0:
                    coarse = dot(coarse, ups[2 * offset - 2])
                diag[offset] = 2.0 * lines[...] + 4.0 * h[SWITCH + offset] + coarse
            for offset in range(LEVELS - SWITCH):
                setup_lines(offset)
        end_a()
        to_lines(recv_b.at[0], target.at[0])
        rowbuf[...] = line_descend(0)
        for a in range(gz):
            for b in range(gy):
                s = (a * gy + b) * depth
                send_n[b, a] = rowbuf[s : s + depth, :]
        begin_b()
        recv_b[1, b_me, a_me] = send_n[b_me, a_me]
        end_b()
        for z in range(depth):
            wide = None
            for b in range(gy):
                for a in range(gz):
                    corr1[a : a + 1, :] = recv_b[1, b, a, z : z + 1, :]
                part = dot(dot(groupt[...], corr1[...]) * mask[...], colst[b])
                wide = part if wide is None else wide + part
            v1[1 - p1, z + 1] = v1[p1, z + 1] + dot(down1[...].T * 2.0, wide)
        p1 = 1 - p1
        for _ in range(SWEEPS):
            p1 = sweep(1, p1)

        def correct0(z, c, p0=p0, p1=p1):
            tmp0[...] = dot_left(downt0[...] * 2.0, v1[p1, z])
            for r in range(0, n0, CHUNK):
                v0[1 - p0, z, pl.ds(r, CHUNK), :] = v0[p0, z, pl.ds(r, CHUNK), :] + dot_right(
                    tmp0[pl.ds(r, CHUNK), :], down0[...] * 2.0
                )
            return c

        lax.fori_loop(1, depth + 1, correct0, 0)
        p0 = 1 - p0
        for _ in range(SWEEPS):
            p0 = sweep(0, p0)

    def last(z, p0=p0):
        for r in range(0, n0, CHUNK):
            centre, res = residual_chunk(v0, p0, z, r, n0, source, diag0, h[0])
            out[z - 1, pl.ds(r, CHUNK), :] = centre
            acc[CYCLES - 1, :, :] += (res * res).reshape(CHUNK // 8, 8, n0).sum(axis=0)

    over_planes(v0, p0, 0, last)
    ridx = lax.broadcasted_iota(jnp.int32, (8, 128), 0)
    part = jnp.zeros((8, 128), jnp.float32)
    for k in range(CYCLES):
        part = jnp.where(ridx == k, jnp.sum(acc[k]), part)
    rowbuf_n = tmp_n = send_n
    target_n = recv_n
    w_n = acc
    acc[0, :, 0:128] = part
    begin_n, end_n = exchange_all(4, lambda a, b: acc.at[0, :, pl.ds(0, 128)], recv_n)
    begin_n()
    recv_n[b_me, a_me] = part
    end_n()
    total = jnp.zeros((8, 128), jnp.float32)
    for a in range(gz):
        for b in range(gy):
            total = total + recv_n[b, a]
    norms[...] = total * (1.0 / (zall * n0 * n0))


def pair_matrix(n, value):
    return (np.arange(n)[None, :] // 2 == np.arange(n // 2)[:, None]).astype(np.float32) * value


def shards(gz, gy, source, vertical, reaction):
    depth, n0 = source.shape[0], source.shape[1]
    nd = gz * gy
    zall = nd * depth
    n1, n2 = n0 // 2, n0 // 4
    bx, by = n2 // gz, n2 // gy
    cells = bx * by
    cp = -(-cells // 128) * 128
    down0 = pair_matrix(n0, 0.5)
    down1 = pair_matrix(n1, 0.5)
    lane = np.arange(cp)
    cols = np.zeros((gy, n1, cp), np.float32)
    colst = np.zeros((gy, cp, n1), np.float32)
    for b in range(gy):
        hit = (np.arange(n1)[:, None] // 2 == b * by + lane[None, :] % by) & (lane[None, :] < cells)
        cols[b] = hit * 0.5
        colst[b] = hit.T
    mask = ((lane[None, :] // by == np.arange(n2)[:, None] % bx) & (lane[None, :] < cells)).astype(np.float32)
    group = (np.arange(n2)[None, :] // bx == np.arange(gz)[:, None]).astype(np.float32)
    ups = []
    for offset in range(LEVELS - SWITCH - 1):
        fx, fy = bx >> offset, by >> offset
        cy = fy // 2
        matrix = np.zeros((cp, cp), np.float32)
        for i in range(fx):
            for j in range(fy):
                matrix[i * fy + j, (i // 2) * cy + j // 2] = 1.0
        ups += [matrix * 0.25, matrix.T]
    ups = np.stack(ups)
    steps = (zall - 1).bit_length()
    f32 = jnp.float32
    nl = LEVELS - SWITCH
    vm = pl.BlockSpec(memory_space=pltpu.VMEM)
    consts = [down0, down0.T.copy(), down1, cols, mask, group, ups, group.T.copy(), colst]
    solution, norms = pl.pallas_call(
        functools.partial(kernel, (gz, gy, depth, cp)),
        out_shape=(
            jax.ShapeDtypeStruct(source.shape, f32),
            jax.ShapeDtypeStruct((8, 128), f32),
        ),
        in_specs=[vm, vm, pl.BlockSpec(memory_space=pltpu.SMEM), vm] + [vm] * len(consts),
        out_specs=(vm, vm),
        scratch_shapes=[
            pltpu.VMEM((2, depth + 2, n0, n0), f32),
            pltpu.VMEM((2, depth + 2, n1, n1), f32),
            pltpu.VMEM((depth, n0, n0), f32),
            pltpu.VMEM((depth, n1, n1), f32),
            pltpu.VMEM((depth, n1, n1), f32),
            pltpu.VMEM((depth, n1, n1), f32),
            pltpu.VMEM((depth, n1, n1), f32),
            pltpu.VMEM((n0, n1), f32),
            pltpu.VMEM((depth, n1, n1), f32),
            pltpu.VMEM((gz, cp), f32),
            pltpu.VMEM((gy, gz, depth, cp), f32),
            pltpu.VMEM((gy, gz, depth, cp), f32),
            pltpu.VMEM((gy, gz, depth, cp), f32),
            pltpu.VMEM((gy, gz, depth, cp), f32),
            pltpu.VMEM((2, gy, gz, depth, cp), f32),
            pltpu.VMEM((gy, gz, depth, cp), f32),
            pltpu.VMEM((gy, gz, 8, 128), f32),
            pltpu.VMEM((zall, cp), f32),
            pltpu.VMEM((nl, zall, cp), f32),
            pltpu.VMEM((nl, 2 * steps + 1, zall, cp), f32),
            pltpu.VMEM((nl, zall, cp), f32),
            pltpu.VMEM((2, zall, cp), f32),
            pltpu.VMEM((2, 4, zall, cp), f32),
            pltpu.VMEM((zall, cp), f32),
            pltpu.VMEM((CYCLES, 8, n0), f32),
            pltpu.SemaphoreType.DMA((2, 2, 2)),
            pltpu.SemaphoreType.DMA((2, 2, 2)),
            pltpu.SemaphoreType.DMA((2, 4)),
            pltpu.SemaphoreType.DMA((2, 4)),
            pltpu.SemaphoreType.DMA((5, nd)),
            pltpu.SemaphoreType.DMA((5, nd)),
        ],
        compiler_params=pltpu.CompilerParams(
            has_side_effects=True, vmem_limit_bytes=64000 * 1024
        ),
    )(
        source,
        reaction,
        vertical,
        jnp.broadcast_to(vertical[:, None], (depth, cp)),
        *[jnp.asarray(c) for c in consts],
    )
    return solution, norms[:CYCLES, 0]


CROWS = 32
GROUP = 2
VMEM_LIMIT = 64000 * 1024
PAD = 8


def dot_parts(x, m, parts=2):
    total = None
    rest = x
    for k in range(parts):
        piece = rest.astype(jnp.bfloat16)
        if k + 1 < parts:
            rest = rest - piece.astype(jnp.float32)
        term = jnp.dot(piece, m, preferred_element_type=jnp.float32)
        total = term if total is None else total + term
    return total


def chain_kernel(
    dims,
    source_in, reaction_in, vertical,
    out, norms,
    source, reaction, downy, upy, up2, down3, down4, up3, up4, load,
    v0, g0, w0, d0, v1, g1, w1, d1, raw_r, raw_s, stage, turn, lines, vsend, vrecv,
    gx, cx, dx, win3, win4, v2, v3, v4, g3, g4, diag, fac, mask, acc, nsend, nrecv,
    a2a_send, a2a_recv, from_sem, x_send, x_recv, w3_send, w3_recv, w4_send, w4_recv,
):
    gz, gy, depth = dims
    nd = gz * gy
    zall = nd * depth
    n0 = source.shape[1]
    n1, n2, n3, n4 = n0 // 2, n0 // 4, n0 // 8, n0 // 16
    r0, r1 = n0 // nd, n0 // 2 // nd
    nt0 = n0 // 128
    h = [COUPLING / 4.0**k for k in range(LEVELS)]
    f32 = jnp.float32
    a_me, b_me = lax.axis_index("gz"), lax.axis_index("gy")
    me = a_me * gy + b_me
    nchip = gz // 2

    def div(x, n):
        return lax.div(x, jnp.int32(n))

    def rem(x, n):
        return lax.rem(x, jnp.int32(n))

    def bend(c):
        return c + div(c, 2) - 2 * div(c, 3) if nchip == 4 else c

    def place(i):
        k, core = div(i, 2), rem(i, 2)
        b, q = div(k, nchip), rem(k, nchip)
        q = q + rem(b, 2) * (nchip - 1 - 2 * q)
        return (bend(q) * 2 + core, b)

    q_me = bend(a_me // 2)
    q_me = q_me + (b_me % 2) * (nchip - 1 - 2 * q_me)
    p = (b_me * nchip + q_me) * 2 + a_me % 2
    chip, par = p // 2, p % 2

    def loop(lo, hi, body):
        def step(i, c):
            body(i)
            return c
        lax.fori_loop(lo, hi, step, 0)

    def remote(src, dst, ss, rs, to):
        return pltpu.make_async_remote_copy(
            src_ref=src, dst_ref=dst, send_sem=ss, recv_sem=rs, device_id=to, device_id_type=MESH
        )

    def target(k):
        return rem(p + nd + (div(k, 2) + rem(k, 2)) * (1 - 2 * rem(k, 2)), nd)

    def flat(i):
        a, b = place(i)
        return a * gy + b

    def spread(kind, src_of, dst_mine, whole, each=None):
        def start(k):
            t = target(k)
            sem = a2a_recv.at[kind] if each is None else from_sem.at[me]
            remote(src_of(t), dst_mine, a2a_send.at[kind], sem, place(t)).start()

        def wait_all(recv):
            copy = remote(whole, whole, a2a_send.at[kind], a2a_recv.at[kind], place(p))
            copy.wait_recv() if recv else copy.wait_send()

        def landed(s):
            if each is None:
                wait_all(True)
            else:
                r = each(s)
                remote(r, r, a2a_send.at[kind], from_sem.at[s], place(p)).wait_recv()

        return lambda lo=1, hi=nd: loop(lo, hi, start), lambda: wait_all(False), landed

    def piece(ref, t):
        return ref.at[:, pl.ds(r0 * t, r0), :]

    def zrows(ref, s):
        return ref.at[pl.ds(depth * s, depth)]

    zrest = pl.ds(0, depth * (nd - 1))
    rest = pl.ds(0, nd - 1)
    start_v, done_v, landed_v = spread(0, lambda t: vsend, vrecv.at[me], vrecv.at[rest])
    start_r, done_r, landed_r = spread(1, lambda t: piece(reaction, t), zrows(raw_r, me), raw_r.at[zrest])
    start_s, done_s, landed_s = spread(
        2, lambda t: piece(source, t), zrows(raw_s, me), raw_s.at[zrest], lambda s: zrows(raw_s, s))
    start_o, done_o, landed_o = spread(
        3, lambda t: zrows(stage, flat(t)), piece(out, p), stage.at[zrest], lambda s: zrows(stage, s))
    start_n, done_n, landed_n = spread(4, lambda t: nsend, nrecv.at[me], nrecv.at[rest])

    load_r = pltpu.make_async_copy(reaction_in, reaction, load.at[0])
    load_s = pltpu.make_async_copy(source_in, source, load.at[1])
    load_r.start()
    load_s.start()
    for i in range(depth):
        vsend[i : i + 1, :] = jnp.full((1, 128), vertical[i], f32)
    load_r.wait()
    start_r()
    start_v()
    load_s.wait()
    start_s()

    def fill(ref, at, value):
        shape = ref.shape[-2:]
        row = lax.broadcasted_iota(jnp.int32, shape, 0)
        col = lax.broadcasted_iota(jnp.int32, shape, 1)
        hit, scale = value(row, col)
        ref[at] = jnp.where(hit, scale, 0.0).astype(jnp.bfloat16)

    fill(downy, ..., lambda r, c: (r // 2 == c, 0.25))
    fill(upy, ..., lambda r, c: (r == c // 2, 1.0))
    for i in range(r1 // 2):
        fill(up2, i, lambda r, c: (r == n2 * i + c // 2, 1.0))
    fill(down3, ..., lambda r, c: (r % n2 // 2 == c % n3, 0.25))
    fill(down4, 0, lambda r, c: ((r >= 3 * n3) & ((r - 3 * n3) // 2 == c % n4), 0.25))
    fill(down4, 1, lambda r, c: ((r < n3) & (r // 2 == c % n4), 0.25))
    fill(up3, 0, lambda r, c: (r == 3 * n3 + c % n2 // 2, 1.0))
    fill(up3, 1, lambda r, c: (r == c % n2 // 2, 1.0))
    for t in range(2):
        fill(up4, t, lambda r, c: (r == n4 * (4 + (4 * t + c // n3 + 5) // 2 - 4) + c % n3 // 2, 1.0))

    first, last = p == 0, p == nd - 1

    def xchg(kind, lo_src, lo_dst, hi_src, hi_dst):
        def down():
            return remote(lo_src, hi_dst, x_send.at[kind, 0], x_recv.at[kind, 0], place((p + nd - 1) % nd))

        def up():
            return remote(hi_src, lo_dst, x_send.at[kind, 1], x_recv.at[kind, 1], place((p + 1) % nd))

        def begin():
            @pl.when(jnp.logical_not(first))
            def _():
                down().start()

            @pl.when(jnp.logical_not(last))
            def _():
                up().start()

        def end():
            @pl.when(jnp.logical_not(first))
            def _():
                down().wait_send()
                up().wait_recv()

            @pl.when(jnp.logical_not(last))
            def _():
                up().wait_send()
                down().wait_recv()

        return begin, end

    def planes0(m, dep):
        def at(lo):
            return v0.at[m, pl.ds(lo, dep), pl.ds(PAD, zall), :]
        return xchg(m, at(2), at(2 - dep), at(2 + r0 - dep), at(2 + r0))

    def row1(kind, far):
        return xchg(kind, g1.at[2 + far], g1.at[1 - far], g1.at[r1 + 1 - far], g1.at[r1 + 2 + far])

    def planes1(ref, kind):
        return xchg(kind, ref.at[pl.ds(2, 2)], ref.at[pl.ds(0, 2)],
                    ref.at[pl.ds(r1, 2)], ref.at[pl.ds(r1 + 2, 2)])

    def planes1v(m):
        def at(lo):
            return v1.at[m, pl.ds(lo, 2), pl.ds(PAD, zall), :]
        return xchg(4, at(2), at(0), at(r1), at(r1 + 2))

    def blocks(ref, kind):
        return xchg(kind, ref.at[1], ref.at[0], ref.at[1], ref.at[2])

    def halo_d0():
        return xchg(5, d0.at[1], d0.at[0], d0.at[r0], d0.at[r0 + 1])

    offs3 = [(o, c) for o in (0, -1, 1, -2, 2) for c in range(2)]

    def window3(kind):
        buf = win3.at[kind]

        def out_of(o, c):
            slot = par + 3 - 2 * o
            return remote(buf.at[3 + par], buf.at[slot], w3_send.at[4 + 2 * o + c], w3_recv.at[kind // CYCLES, slot],
                          place((2 * (chip + o) + c + nd) % nd))

        def goes(o, c):
            there = jnp.logical_and(chip + o >= 0, chip + o < nd // 2)
            if o == 0:
                return par != c
            if o == -2:
                return jnp.logical_and(there, par == 0)
            if o == 2:
                return jnp.logical_and(there, par == 1)
            return there

        def begin():
            for o, c in offs3:
                @pl.when(goes(o, c))
                def _(o=o, c=c):
                    out_of(o, c).start()

        def end():
            for o, c in offs3:
                @pl.when(goes(o, c))
                def _(o=o, c=c):
                    out_of(o, c).wait_send()
            for q in range(8):
                row = 2 * chip - 3 + q
                inside = jnp.logical_and(row >= 0, row < nd)
                if q in (3, 4):
                    inside = par != q - 3

                @pl.when(inside)
                def _(q=q):
                    remote(buf.at[q], buf.at[q], w3_send.at[0], w3_recv.at[kind // CYCLES, q], place(p)).wait_recv()

        return begin, end

    offs4 = [-1, 1, -2, 2, -3, 3, -4, 4]

    def window4(kind):
        buf = win4.at[kind]

        def each(fn):
            for o in offs4:
                @pl.when(jnp.logical_and(chip + o >= 0, chip + o < nd // 2))
                def _(o=o):
                    fn(o)

        def out_of(o):
            return remote(buf.at[4], buf.at[4 - o], w4_send.at[4 + o], w4_recv.at[kind // CYCLES, 4 - o],
                          place((p + 2 * o + nd) % nd))

        def begin():
            each(lambda o: out_of(o).start())

        def end():
            def fn(o):
                out_of(o).wait_send()
                remote(buf.at[4 + o], buf.at[4 + o], w4_send.at[4 + o], w4_recv.at[kind // CYCLES, 4 + o],
                       place(p)).wait_recv()
            each(fn)

        return begin, end

    zpad = jnp.zeros((PAD, n0), f32)
    for m in range(3):
        def zero0(x, m=m):
            v0[m, x, 0:PAD, :] = zpad
            v0[m, x, PAD + zall : 2 * PAD + zall, :] = zpad
        loop(0, r0 + 4, zero0)

        def zero1(x, m=m):
            v1[m, x, 0:PAD, :] = zpad[:, :n1]
            v1[m, x, PAD + zall : 2 * PAD + zall, :] = zpad[:, :n1]
        loop(0, r1 + 4, zero1)

    tile0 = jnp.zeros((zall, 128), f32)
    plane0 = jnp.zeros((zall, n0), f32)

    def blank(lo0, x0, lo1, b):
        for q in range(2):
            for m in (0, 2):
                v0[m, lo0 + q, PAD : PAD + zall, :] = plane0
            v1[2, lo1 + q, PAD : PAD + zall, :] = tile0
            g1[lo1 + q] = tile0
            d1[lo1 + q] = tile0
            w1[lo1 + q] = tile0
        d0[x0] = plane0
        w0[x0] = plane0
        for k in range(CYCLES):
            gx[k, b] = tile0
            cx[k, b] = tile0
        dx[b] = tile0

    @pl.when(first)
    def _():
        blank(0, 0, 0, 0)

    @pl.when(last)
    def _():
        blank(r0 + 2, r0 + 1, r1 + 2, 2)

    for k in range(CYCLES + 1):
        for q in range(8):
            @pl.when(jnp.logical_or(2 * chip - 3 + q < 0, 2 * chip - 3 + q >= nd))
            def _(q=q, k=k):
                win3[k, q] = jnp.zeros((n3 * zall // 128, 128), f32)
        for o in offs4:
            @pl.when(jnp.logical_or(chip + o < 0, chip + o >= nd // 2))
            def _(o=o, k=k):
                win4[k, 4 + o] = jnp.zeros((n4 * zall // 128, 128), f32)
    for q in range(2):
        v3[q, 0] = tile0
        v3[q, 3] = tile0
        v4[q, 0] = tile0
        v4[q, 3] = tile0
    v4[1, 2] = tile0
    acc[...] = jnp.zeros_like(acc)

    lane = lax.broadcasted_iota(jnp.int32, (zall, 128), 1)
    rows = lax.broadcasted_iota(jnp.int32, (zall, 128), 0)

    for t in range(3):
        good = [p > 0, None, p < nd - 1][t]
        one = jnp.ones((zall, 128), f32)
        mask[t] = one if good is None else one * good.astype(f32)
    for t in range(2):
        row = 2 * chip - 3 + 4 * t + lane // n3
        mask[3 + t] = jnp.where((row >= 0) & (row < nd), 1.0, 0.0)
        row = chip - 4 + 8 * t + lane // n4
        mask[5 + t] = jnp.where((row >= 0) & (row < nd // 2) & (row < chip + 5), 1.0, 0.0)

    def pack(rep, width):
        k = 128 // width
        zb = zall // k
        part = lane[:zb]
        got = rep[0:zb]
        for j in range(1, k):
            got = jnp.where(part // width == j, rep[zb * j : zb * (j + 1)], got)
        return got

    def unpack(slots, width):
        k = 128 // width
        zb = zall // k
        part = lane[:zb] // width
        parts = []
        for j in range(k):
            got = jnp.zeros((zb, 128), f32)
            for s, x in enumerate(slots):
                turn = (width * (s - j)) % 128
                x = x if turn == 0 else pltpu.roll(x, turn, 1)
                got = jnp.where(part == s, x, got)
            parts.append(got)
        return parts

    def unpack3(kind, dest, add=None):
        for t in range(2):
            slots = [win3[kind, 4 * t + k] for k in range(4)]
            zb = zall // 4
            for j, x in enumerate(unpack(slots, n3)):
                if add is not None:
                    x = x + add(j * zb, zb)
                dest[t, j * zb : (j + 1) * zb] = x

    def unpack4(kind, dest, add=None):
        for t in range(2):
            slots = [win4[kind, r] for r in range(8 * t, min(8 * t + 8, 9))]
            zb = zall // 8
            for j, x in enumerate(unpack(slots, n4)):
                if add is not None:
                    x = x + add(j * zb, zb)
                dest[t, j * zb : (j + 1) * zb] = x

    rawr = raw_r.reshape(zall * r0, n0)
    raws = raw_s.reshape(zall * r0, n0)
    staged = stage.reshape(zall * r0, n0)

    def unfold(raw, j):
        at = pl.ds(pl.multiple_of(PAD * r0 * j, PAD * r0), PAD * r0)
        for t in range(nt0):
            turn[t, at, :] = raw[at, 128 * t : 128 * (t + 1)]
    raw_r[pl.ds(depth * me, depth)] = reaction[:, pl.ds(r0 * p, r0), :]
    raw_s[pl.ds(depth * me, depth)] = source[:, pl.ds(r0 * p, r0), :]
    vrecv[me] = vsend[...]
    group = PAD // depth

    def each_rows(landed, body):
        def step(i):
            j = (me // group + i) % (zall // PAD)
            for k in range(group if landed is not None else 0):
                s = group * j + k

                @pl.when(s != me)
                def _():
                    landed(s)
            body(j)
        loop(0, zall // PAD, step)

    landed_v(None)
    for s in range(nd):
        lines[depth * s : depth * (s + 1), :] = vrecv[s]

    def take_r(j):
        z = pl.multiple_of(PAD * j, PAD)
        unfold(rawr, j)
        for x in range(r0):
            for t in range(nt0):
                d0[x + 1, pl.ds(z, PAD), 128 * t : 128 * (t + 1)] = turn[
                    t, pl.ds(PAD * r0 * j + x, PAD, stride=r0), :]

    landed_r(None)
    each_rows(None, take_r)

    def shrink_r(i):
        for r in range(0, zall, CROWS):
            at = pl.ds(r, CROWS)
            a, b = d0[2 * i + 1, at, :], d0[2 * i + 2, at, :]
            got = dot_parts(a + b, downy[...], 3)
            vert = lines[at, :]
            base = 2.0 * vert + 4.0 * h[1]
            w1[i + 2, at, :] = got
            d = base + got
            d1[i + 2, at, :] = d
            base = jnp.concatenate([2.0 * vert + 4.0 * h[0]] * nt0, axis=1)
            for k, x in ((1, a), (2, b)):
                x = base + x
                d0[2 * i + k, at, :] = x
                w0[2 * i + k, at, :] = DAMPING / x

    loop(0, r1, shrink_r)
    begin_d0, end_d0 = halo_d0()
    begin_d0()
    begin_d1, end_d1 = planes1(d1, 6)
    begin_d1()
    rx2 = dot_parts(jnp.concatenate([w1[2] + w1[3], w1[4] + w1[5]], axis=1), downy[...], 3)
    dx[1] = rx2
    begin_dx, end_dx = blocks(dx, 7)
    begin_dx()
    rx3 = dot_parts(rx2, down3[...], 3)
    win3[CYCLES, 3 + par] = pack(rx3, n3)
    begin_w3, end_w3 = window3(CYCLES)
    begin_w3()
    begin_w4, end_w4 = window4(CYCLES)
    loop(2, r1 + 2, lambda x: w1.__setitem__(x, DAMPING / d1[x]))

    def take_s(j):
        z = pl.multiple_of(PAD * j, PAD)
        unfold(raws, j)
        for x in range(r0):
            for t in range(nt0):
                cut = slice(128 * t, 128 * (t + 1))
                got = turn[t, pl.ds(PAD * r0 * j + x, PAD, stride=r0), :]
                g0[x + 1, pl.ds(z, PAD), cut] = got
                v0[0, x + 2, pl.ds(z + PAD, PAD), cut] = w0[x + 1, pl.ds(z, PAD), cut] * got

    each_rows(landed_s, take_s)

    ns = (zall - 1).bit_length()

    def factors(f):
        vert = lines[...]
        a = jnp.where(rows == 0, 0.0, -vert)
        c = jnp.where(rows == zall - 1, 0.0, -vert)
        b = diag[f]
        for k in range(ns):
            s = 1 << k
            inv = 1.0 / b
            alpha = -a * pltpu.roll(inv, s, 0)
            gamma = -c * pltpu.roll(inv, zall - s, 0)
            b = b + alpha * pltpu.roll(c, s, 0) + gamma * pltpu.roll(a, zall - s, 0)
            a = alpha * pltpu.roll(a, s, 0)
            c = gamma * pltpu.roll(c, zall - s, 0)
            fac[f, 2 * k] = alpha
            fac[f, 2 * k + 1] = gamma
        fac[f, 2 * ns] = mask[f] / b

    def solve(f, right):
        for k in range(ns):
            s = 1 << k
            right = (
                right
                + fac[f, 2 * k] * pltpu.roll(right, s, 0)
                + fac[f, 2 * k + 1] * pltpu.roll(right, zall - s, 0)
            )
        return right * fac[f, 2 * ns]

    def near(v, q, b, width):
        t = v[q, b]
        below = pltpu.roll(jnp.where(lane >= 128 - width, v[q, b - 1], t), width, 1)
        above = pltpu.roll(jnp.where(lane < width, v[q, b + 1], t), 128 - width, 1)
        inrow = lane % width
        left = jnp.where(inrow == 0, 0.0, pltpu.roll(t, 1, 1))
        right = jnp.where(inrow == width - 1, 0.0, pltpu.roll(t, 127, 1))
        return (below + above) + (left + right)

    edge = lax.broadcasted_iota(jnp.int32, (CROWS, 128), 1)
    level0 = (v0, g0, w0, d0, nt0, h[0], 1)
    level1 = (v1, g1, w1, d1, 1, h[1], 2)

    def stencil(level, m, x, r):
        v, g, w, d, nt, weight, go = level
        centre, turn_r, turn_l = [], [], []
        for t in range(nt):
            cut = slice(128 * t, 128 * (t + 1))
            c = v[m, x + 2, PAD + r : PAD + r + CROWS, cut]
            centre.append(c)
            turn_r.append(pltpu.roll(c, 1, 1))
            turn_l.append(pltpu.roll(c, 127, 1))
        vert = lines[r : r + CROWS, :]
        got = []
        for t in range(nt):
            cut = slice(128 * t, 128 * (t + 1))
            left = jnp.where(edge == 0, turn_r[t - 1] if t else 0.0, turn_r[t])
            right = jnp.where(edge == 127, turn_l[t + 1] if t + 1 < nt else 0.0, turn_l[t])
            side = (v[m, x + 1, PAD + r : PAD + r + CROWS, cut] + v[m, x + 3, PAD + r : PAD + r + CROWS, cut]) + (left + right)
            if weight != 1.0:
                side = weight * side
            ends = v[m, x + 2, PAD + r - 1 : PAD + r - 1 + CROWS, cut] + v[m, x + 2, PAD + r + 1 : PAD + r + 1 + CROWS, cut]
            got.append(g[x + go, r : r + CROWS, cut] + side + vert * ends)
        return centre, got

    def sweep_plane(level, m, q, x, record=None, put=None):
        v, g, w, d, nt, weight, go = level
        for lo in range(0, zall, GROUP * CROWS):
            new = []
            for r in range(lo, lo + GROUP * CROWS, CROWS):
                centre, got = stencil(level, m, x, r)
                for t in range(nt):
                    cut = slice(128 * t, 128 * (t + 1))
                    wt = w[x + go, r : r + CROWS, cut]
                    if record is None:
                        value = (1.0 - DAMPING) * centre[t] + wt * got[t]
                    else:
                        res = got[t] - d[x + go, r : r + CROWS, cut] * centre[t]
                        value = centre[t] + wt * res
                        acc[record] += (res * res).reshape(CROWS // 8, 8, 128).sum(axis=0)
                    new.append((r, t, value))
            for r, t, value in new:
                v[q, x + 2, PAD + r : PAD + r + CROWS, 128 * t : 128 * (t + 1)] = value
                if put is not None:
                    for e in range(0, CROWS, 8):
                        put(x, r + e, t, value[e : e + 8])

    def residual(level, m, x, r):
        v, g, w, d, nt, weight, go = level
        centre, got = stencil(level, m, x, r)
        res = [
            got[t] - d[x + go, r : r + CROWS, 128 * t : 128 * (t + 1)] * centre[t] for t in range(nt)]
        return res

    def sweeps(level, m, q, xs, record=None, put=None):
        lo, hi, fn = xs
        loop(lo, hi, lambda i: sweep_plane(level, m, q, fn(i), record, put))

    def restrict0(m, lo, hi, fn):
        def body(i):
            i = fn(i)
            for r in range(0, zall, CROWS):
                a = residual(level0, m, 2 * i, r)
                b = residual(level0, m, 2 * i + 1, r)
                both = jnp.concatenate([s + t for s, t in zip(a, b)], axis=1)
                g1[i + 2, r : r + CROWS, :] = dot_parts(both, downy[...])
        loop(lo, hi, body)

    def same(i):
        return i

    def rim(size, wide):
        return lambda i: i + (i // wide) * (size - 2 * wide)

    def outer(size):
        return lambda i: -1 + i * (size + 1)

    def pair0(m, q, record=None, hook=None, put=None, restrict=False, before=None):
        begin, end = planes0(m, 2)
        begin()
        if before is not None:
            before()
        if hook is not None:
            hook[0]()
        sweeps(level0, m, 1, (1, r0 - 1, same), record)
        if restrict:
            restrict0(1, 1, r1 - 1, same)
            row1(3, 1)[0]()
        else:
            sweeps(level0, 1, q, (2, r0 - 2, same), None, put)
        end()
        if hook is not None:
            hook[1]()
        sweeps(level0, m, 1, (0, 2, outer(r0)))
        sweeps(level0, m, 1, (0, 2, rim(r0, 1)), record)
        if restrict:
            restrict0(1, 0, 2, lambda i: i * (r1 - 1))
        else:
            sweeps(level0, 1, q, (0, 4, rim(r0, 2)), None, put)

    def halo_factors():
        end_dx()
        for t in range(3):
            diag[t] = 2.0 * lines[...] + 4.0 * h[2] + dx[t]
        loop(0, 3, factors)
        for k in range(2 * ns + 1):
            fac[7, k] = jnp.where(lane >= n2, fac[0, k], fac[2, k])
        end_w3()
        unpack3(CYCLES, g3)
        win4[CYCLES, 4] = pack(
            dot_parts(g3[0], down4[0], 3) + dot_parts(g3[1], down4[1], 3), n4)
        begin_w4()

    def window_factors():
        def add(level):
            return lambda r, n: 2.0 * lines[r : r + n, :] + 4.0 * h[level]
        for t in range(2):
            diag[3 + t] = 2.0 * lines[...] + 4.0 * h[3] + g3[t]
        loop(3, 5, factors)
        end_w4()
        unpack4(CYCLES, diag.at[pl.ds(5, 2)], add(4))
        loop(5, 7, factors)

    def halo_level0():
        end_d0()
        for x, inside in ((0, jnp.logical_not(first)), (r0 + 1, jnp.logical_not(last))):
            @pl.when(inside)
            def _(x=x):
                w0[x] = DAMPING / d0[x]
            g0[x] = v0[0, x + 1, PAD : PAD + zall, :] * d0[x] * (1.0 / DAMPING)

    def halo_level1():
        end_d1()
        for x, inside in ((0, jnp.logical_not(first)), (r1 + 2, jnp.logical_not(last))):
            @pl.when(inside)
            def _(x=x):
                for q in range(2):
                    w1[x + q] = DAMPING / d1[x + q]

    def coarse(cycle):
        begin, end = row1(10, 0)
        begin()
        if cycle == 0:
            window_factors()
        loop(2, r1 + 2, lambda x: v1.__setitem__((0, x, pl.ds(PAD, zall)), w1[x] * g1[x]))
        row1(3, 1)[1]()
        end()
        if cycle == 0:
            halo_level1()
        for x in (0, 1, r1 + 2, r1 + 3):
            v1[0, x, PAD : PAD + zall] = w1[x] * g1[x]
        sweeps(level1, 0, 1, (-1, r1 + 1, same))

        pairs = []
        for i in range(r1 // 2):
            cuts = []
            for r in range(0, zall, CROWS):
                a = residual(level1, 1, 2 * i, r)[0]
                b = residual(level1, 1, 2 * i + 1, r)[0]
                cuts.append(a + b)
            pairs.append(jnp.concatenate(cuts, axis=0))
        gx[cycle, 1] = dot_parts(jnp.concatenate(pairs, axis=1), downy[...])
        e2 = lines2(cycle)

        for i in range(r1 // 2):
            e = dot_parts(e2, up2[i])
            for x in (2 * i, 2 * i + 1):
                v1[2, x + 2, PAD : PAD + zall] = v1[1, x + 2, PAD : PAD + zall] + e
        begin, end = planes1v(2)
        begin()
        sweeps(level1, 2, 1, (1, r1 - 1, same))
        end()
        sweeps(level1, 2, 1, (0, 2, outer(r1)))
        sweeps(level1, 2, 1, (0, 2, rim(r1, 1)))
        sweeps(level1, 1, 0, (0, r1, same))

    def lines_sweep(v, q, s, lo, hi, right, f, weight, width):
        for b in range(lo, hi):
            v[s, b] = solve(f + b - 1, right[b - 1] + weight * near(v, q, b, width))

    def line_residual(v, q, b, right, f, weight, width):
        values = v[q, b]
        before = jnp.where(rows == 0, 0.0, pltpu.roll(values, 1, 0))
        after = jnp.where(rows == zall - 1, 0.0, pltpu.roll(values, zall - 1, 0))
        return right[b - 1] + weight * near(v, q, b, width) + lines[...] * (before + after) - diag[f + b - 1] * values

    def beside(t):
        inrow = lane % n2
        return jnp.where(inrow == 0, 0.0, pltpu.roll(t, 1, 1)) + jnp.where(inrow == n2 - 1, 0.0, pltpu.roll(t, 127, 1))

    def pair2(left, own, right, right_own, right_rim):
        upper = lane >= n2
        rim = jnp.where(upper, left, right)
        far = jnp.where(upper, right, left)
        new = solve(1, right_own + h[2] * (beside(own) + pltpu.roll(own + rim, n2, 1)))
        return new, solve(7, right_rim + h[2] * (beside(rim) + pltpu.roll(own + far, n2, 1)))

    def lines2(cycle):
        right = gx.at[cycle]
        begin, end = blocks(right, 8)
        begin()
        v2[1] = solve(1, right[1])
        end()
        for b in (0, 2):
            v2[b] = solve(b, right[b])
        right_rim = jnp.where(lane >= n2, right[0], right[2])
        v2[3], v2[4] = pair2(v2[0], v2[1], v2[2], right[1], right_rim)
        own = v2[3]
        before = jnp.where(rows == 0, 0.0, pltpu.roll(own, 1, 0))
        after = jnp.where(rows == zall - 1, 0.0, pltpu.roll(own, zall - 1, 0))
        around = beside(own) + pltpu.roll(own + v2[4], n2, 1)
        res = right[1] + h[2] * around + lines[...] * (before + after) - diag[1] * own
        win3[cycle, 3 + par] = pack(dot_parts(res, down3[...]), n3)
        e3 = lines3(cycle)
        cx[cycle, 1] = v2[3] + dot_parts(e3, up3[par])
        begin, end = blocks(cx.at[cycle], 9)
        begin()
        end()
        v2[0], v2[1] = pair2(cx[cycle, 0], cx[cycle, 1], cx[cycle, 2], right[1], jnp.where(lane >= n2, right[0], right[2]))
        return solve(1, right[1] + h[2] * (beside(v2[0]) + pltpu.roll(v2[0] + v2[1], n2, 1)))

    def lines3(cycle):
        begin, end = window3(cycle)
        begin()
        end()
        unpack3(cycle, g3)
        loop(1, 3, lambda b: v3.__setitem__((0, b), solve(3 + b - 1, g3[b - 1])))
        lines_sweep(v3, 0, 1, 1, 3, g3, 3, h[3], n3)
        both = None
        for t in range(2):
            part = dot_parts(line_residual(v3, 1, t + 1, g3, 3, h[3], n3), down4[t])
            both = part if both is None else both + part
        win4[cycle, 4] = pack(both, n4)
        e4 = lines4(cycle)
        for t in range(2):
            v3[0, t + 1] = v3[1, t + 1] + dot_parts(e4, up4[t])
        lines_sweep(v3, 0, 1, 1, 3, g3, 3, h[3], n3)
        return solve(3 + par, g3[par] + h[3] * near(v3, 1, 1 + par, n3))

    def lines4(cycle):
        begin, end = window4(cycle)
        begin()
        end()
        unpack4(cycle, g4)
        loop(1, 3, lambda b: v4.__setitem__((0, b), solve(5 + b - 1, g4[b - 1])))
        q = 0
        for k in range(1, COARSE - 1):
            v4[1 - q, 1] = solve(5, g4[0] + h[4] * near(v4, q, 1, n4))
            q = 1 - q
        return solve(5, g4[0] + h[4] * near(v4, q, 1, n4))

    def correct0(m, q, lo, hi, fn):
        def body(i):
            i = fn(i)
            for r in range(0, zall, CROWS):
                e = dot_parts(v1[0, i + 2, PAD + r : PAD + r + CROWS, :], upy[...])
                for x in (2 * i + 2, 2 * i + 3):
                    v0[q, x, PAD + r : PAD + r + CROWS, :] = v0[m, x, PAD + r : PAD + r + CROWS, :] + e
        loop(lo, hi, body)

    def put(x, z, t, value):
        turn[t, pl.ds(z * r0 + x, 8, stride=r0), :] = value

    def fold(j):
        at = pl.ds(pl.multiple_of(PAD * r0 * j, PAD * r0), PAD * r0)
        for t in range(nt0):
            staged[at, 128 * t : 128 * (t + 1)] = turn[t, at, :]

    pair0(0, 1, hook=(halo_factors, halo_level0), restrict=True)
    coarse(0)
    correct0(1, 2, 0, 2, lambda i: i * (r1 - 1))
    pair0(2, 0, before=lambda: correct0(1, 2, 1, r1 - 1, same))
    pair0(0, 2, record=0)
    begin, end = planes0(2, 1)
    begin()
    restrict0(2, 1, r1 - 1, same)
    row1(3, 1)[0]()
    end()
    restrict0(2, 0, 2, lambda i: i * (r1 - 1))
    coarse(1)
    correct0(2, 0, 0, 2, lambda i: i * (r1 - 1))
    pair0(0, 2, put=put, before=lambda: correct0(2, 0, 1, r1 - 1, same))
    loop(0, zall // PAD, fold)
    begin, end = planes0(2, 1)
    begin()
    start_o(1, nd * 5 // 8)
    keep = pltpu.make_async_copy(zrows(stage, me), piece(out, p), load.at[2])
    keep.start()

    def last_norm(x):
        for r in range(0, zall, CROWS):
            for res in residual(level0, 2, x, r):
                acc[CYCLES - 1] += (res * res).reshape(CROWS // 8, 8, 128).sum(axis=0)

    loop(1, r0 - 1, last_norm)
    end()
    loop(0, 2, lambda i: last_norm(i * (r0 - 1)))
    ridx = lax.broadcasted_iota(jnp.int32, (8, 128), 0)
    part = jnp.zeros((8, 128), f32)
    for k in range(CYCLES):
        part = jnp.where(ridx == k, jnp.sum(acc[k]), part)
    nsend[...] = part
    start_n()
    start_o(nd * 5 // 8, nd)
    total = part
    done_v()
    done_r()
    done_s()

    def finish(s):
        @pl.when(s != me)
        def _():
            landed_o(s)
    loop(0, nd, finish)
    landed_n(None)
    nrecv[me] = part
    total = jnp.sum(nrecv[...], axis=0)
    for k in range(CYCLES):
        norms[k] = total[k, 0] * (1.0 / (zall * n0 * n0))
    keep.wait()
    done_o()
    done_n()


def chain_shards(gz, gy, source, vertical, reaction):
    depth, n0 = source.shape[0], source.shape[1]
    nd = gz * gy
    zall = nd * depth
    n1, n2, n3, n4 = n0 // 2, n0 // 4, n0 // 8, n0 // 16
    r0, r1 = n0 // nd, n1 // nd
    f32 = jnp.float32
    bf16 = jnp.bfloat16

    sm = pl.BlockSpec(memory_space=pltpu.SMEM)
    ns = (zall - 1).bit_length()
    dma = pltpu.SemaphoreType.DMA
    solution, norms = pl.pallas_call(
        functools.partial(chain_kernel, (gz, gy, depth)),
        out_shape=(
            pltpu.VMEM(source.shape, f32),
            jax.ShapeDtypeStruct((CYCLES,), f32),
        ),
        in_specs=[pl.BlockSpec(memory_space=pltpu.HBM)] * 2 + [sm],
        out_specs=(pl.BlockSpec(memory_space=pltpu.VMEM), sm),
        scratch_shapes=[
            pltpu.VMEM(source.shape, f32),
            pltpu.VMEM(source.shape, f32),
            pltpu.VMEM((n0, n1), bf16),
            pltpu.VMEM((n1, n0), bf16),
            pltpu.VMEM((r1 // 2, 128, n1), bf16),
            pltpu.VMEM((128, 128), bf16),
            pltpu.VMEM((2, 128, 128), bf16),
            pltpu.VMEM((2, 128, 128), bf16),
            pltpu.VMEM((2, 128, 128), bf16),
            pltpu.SemaphoreType.DMA((3,)),
            pltpu.VMEM((3, r0 + 4, zall + 2 * PAD, n0), f32),
            pltpu.VMEM((r0 + 2, zall, n0), f32),
            pltpu.VMEM((r0 + 2, zall, n0), f32),
            pltpu.VMEM((r0 + 2, zall, n0), f32),
            pltpu.VMEM((3, r1 + 4, zall + 2 * PAD, n1), f32),
            pltpu.VMEM((r1 + 4, zall, n1), f32),
            pltpu.VMEM((r1 + 4, zall, n1), f32),
            pltpu.VMEM((r1 + 4, zall, n1), f32),
            pltpu.VMEM((zall, r0, n0), f32),
            pltpu.VMEM((zall, r0, n0), f32),
            pltpu.VMEM((zall, r0, n0), f32),
            pltpu.VMEM((n0 // 128, zall * r0, 128), f32),
            pltpu.VMEM((zall, 128), f32),
            pltpu.VMEM((depth, 128), f32),
            pltpu.VMEM((nd, depth, 128), f32),
            pltpu.VMEM((CYCLES, 3, zall, 128), f32),
            pltpu.VMEM((CYCLES, 3, zall, 128), f32),
            pltpu.VMEM((3, zall, 128), f32),
            pltpu.VMEM((CYCLES + 1, 8, n3 * zall // 128, 128), f32),
            pltpu.VMEM((CYCLES + 1, 9, n4 * zall // 128, 128), f32),
            pltpu.VMEM((5, zall, 128), f32),
            pltpu.VMEM((2, 4, zall, 128), f32),
            pltpu.VMEM((2, 4, zall, 128), f32),
            pltpu.VMEM((2, zall, 128), f32),
            pltpu.VMEM((2, zall, 128), f32),
            pltpu.VMEM((7, zall, 128), f32),
            pltpu.VMEM((8, 2 * ns + 1, zall, 128), f32),
            pltpu.VMEM((7, zall, 128), f32),
            pltpu.VMEM((CYCLES, 8, 128), f32),
            pltpu.VMEM((8, 128), f32),
            pltpu.VMEM((nd, 8, 128), f32),
            dma((5,)),
            dma((5,)),
            dma((nd,)),
            dma((11, 2)),
            dma((11, 2)),
            dma((10,)),
            dma((2, 8)),
            dma((9,)),
            dma((2, 9)),
        ],
        compiler_params=pltpu.CompilerParams(
            has_side_effects=True, vmem_limit_bytes=VMEM_LIMIT
        ),
    )(source, reaction, vertical)
    return solution, norms


def shards_of(gz, gy, source, vertical, reaction):
    depth, n0 = source.shape[0], source.shape[1]
    nd = gz * gy
    fits = (
        gz % 2 == 0 and n0 % (8 * nd) == 0 and n0 // nd == 8 and n0 % 256 == 0 and n0 // 4 * 2 == 128
        and PAD % depth == 0 and nd * depth % 128 == 0 and (LEVELS, SWITCH, SWEEPS, COARSE, CYCLES) == (5, 2, 2, 4, 2)
    )
    return (chain_shards if fits else shards)(gz, gy, source, vertical, reaction)


def solution(mesh):
    return jax.shard_map(
        functools.partial(shards_of, mesh.shape["gz"], mesh.shape["gy"]),
        mesh=mesh,
        in_specs=(P(("gz", "gy"), None, None), P(("gz", "gy")), P(("gz", "gy"), None, None)),
        out_specs=(P(("gz", "gy"), None, None), P()),
        check_vma=False,
    )
```

```python
import functools

import jax
import jax.numpy as jnp
import numpy as np
from jax import lax
from jax.experimental import pallas as pl
from jax.experimental.pallas import tpu as pltpu
from jax.sharding import PartitionSpec as P

LEVELS = 5
SWITCH = 2
CYCLES = 2
SWEEPS = 2
COARSE = 4
DAMPING = 0.8
COUPLING = 1.0
CHUNK = 32
MESH = pl.DeviceIdType.MESH


def dot(a, b):
    return lax.dot_general(
        a,
        b,
        (((1,), (0,)), ((), ())),
        precision=lax.Precision.HIGHEST,
        preferred_element_type=jnp.float32,
    )


def parts_of(x):
    first = x.astype(jnp.bfloat16)
    rest = x - first.astype(jnp.float32)
    second = rest.astype(jnp.bfloat16)
    third = (rest - second.astype(jnp.float32)).astype(jnp.bfloat16)
    return (third, second, first)


def dot_right(x, m):
    m = m.astype(jnp.bfloat16)
    total = None
    for x in parts_of(x):
        term = jnp.dot(x, m, preferred_element_type=jnp.float32)
        total = term if total is None else total + term
    return total


def dot_left(m, x):
    m = m.astype(jnp.bfloat16)
    total = None
    for x in parts_of(x):
        term = jnp.dot(m, x, preferred_element_type=jnp.float32)
        total = term if total is None else total + term
    return total


def kernel(
    dims,
    source, reaction, vert_s, vert_b, down0, downt0, down1, cols, mask, group, ups, groupt, colst,
    out, norms,
    v0, v1, w0, d1, w1, g1, r1, tmp0, res1, corr1, send_a, recv_a, send_v, recv_v, recv_b,
    send_n, recv_n, lines, diag, factor, target, around, halo, rowbuf, acc,
    plane_send, plane_recv, line_send, line_recv, a2a_send, a2a_recv,
):
    gz, gy, depth, cp = dims
    nd = gz * gy
    zall = nd * depth
    n0 = source.shape[1]
    n1 = n0 // 2
    a_me = lax.axis_index("gz")
    b_me = lax.axis_index("gy")
    me = a_me * gy + b_me
    h = [COUPLING / 4.0**k for k in range(LEVELS)]

    @pl.when(me == 0)
    def _():
        for p in range(2):
            v0[p, 0] = jnp.zeros((n0, n0), jnp.float32)
            v1[p, 0] = jnp.zeros((n1, n1), jnp.float32)

    @pl.when(me == nd - 1)
    def _():
        for p in range(2):
            v0[p, depth + 1] = jnp.zeros((n0, n0), jnp.float32)
            v1[p, depth + 1] = jnp.zeros((n1, n1), jnp.float32)

    edges = [a_me == 0, a_me == gz - 1, b_me == 0, b_me == gy - 1]
    for k in range(4):
        @pl.when(edges[k])
        def _(k=k):
            for p in range(2):
                halo[p, k] = jnp.zeros((zall, cp), jnp.float32)

    def flat(d):
        return (d // gy, d % gy)

    def plane_copy(v, p, level, up):
        if up:
            src, dst, to = v.at[p, depth], v.at[p, 0], flat(me + 1)
        else:
            src, dst, to = v.at[p, 1], v.at[p, depth + 1], flat(me + nd - 1 - nd * ((me + nd - 1) // nd))
        if up:
            to = flat((me + 1) % nd)
        k = 0 if up else 1
        return pltpu.make_async_remote_copy(
            src_ref=src, dst_ref=dst,
            send_sem=plane_send.at[level, p, k], recv_sem=plane_recv.at[level, p, k],
            device_id=to, device_id_type=MESH,
        )

    def plane_start(v, p, level):
        @pl.when(me < nd - 1)
        def _():
            plane_copy(v, p, level, True).start()

        @pl.when(me > 0)
        def _():
            plane_copy(v, p, level, False).start()

    def plane_wait(v, p, level):
        @pl.when(me < nd - 1)
        def _():
            plane_copy(v, p, level, True).wait_send()
            plane_copy(v, p, level, False).wait_recv()

        @pl.when(me > 0)
        def _():
            plane_copy(v, p, level, False).wait_send()
            plane_copy(v, p, level, True).wait_recv()

    def residual_chunk(v, p, z, r, n, target_ref, diag_of, weight):
        centre = v[p, z, pl.ds(r, CHUNK), :]
        rows = lax.broadcasted_iota(jnp.int32, (CHUNK, n), 0)
        lanes = lax.broadcasted_iota(jnp.int32, (CHUNK, n), 1)
        if r == 0:
            above = jnp.where(rows == 0, 0.0, pltpu.roll(centre, 1, 0))
        else:
            above = v[p, z, pl.ds(r - 1, CHUNK), :]
        if r + CHUNK == n:
            below = jnp.where(rows == CHUNK - 1, 0.0, pltpu.roll(centre, CHUNK - 1, 0))
        else:
            below = v[p, z, pl.ds(r + 1, CHUNK), :]
        left = jnp.where(lanes == 0, 0.0, pltpu.roll(centre, 1, 1))
        right = jnp.where(lanes == n - 1, 0.0, pltpu.roll(centre, n - 1, 1))
        vert = vert_s[z - 1]
        applied = (
            diag_of(z - 1, r, vert) * centre
            - vert * (v[p, z - 1, pl.ds(r, CHUNK), :] + v[p, z + 1, pl.ds(r, CHUNK), :])
            - weight * (above + below + left + right)
        )
        return centre, target_ref[z - 1, pl.ds(r, CHUNK), :] - applied

    def diag0(z, r, vert):
        return 2.0 * vert + 4.0 * h[0] + reaction[z, pl.ds(r, CHUNK), :]

    def diag1(z, r, vert):
        return d1[z, pl.ds(r, CHUNK), :]

    def over_planes(v, p, level, body):
        plane_start(v, p, level)

        def inner(z, c):
            body(z)
            return c

        lax.fori_loop(2, depth, inner, 0)
        plane_wait(v, p, level)

        def outer(i, c):
            body(1 + i * (depth - 1))
            return c

        lax.fori_loop(0, 2, outer, 0)

    def level_parts(level):
        if level == 0:
            return v0, source, diag0, w0, n0
        return v1, g1, diag1, w1, n1

    def sweep(level, p, record=None):
        v, tgt, dg, w, n = level_parts(level)

        def body(z):
            for r in range(0, n, CHUNK):
                centre, res = residual_chunk(v, p, z, r, n, tgt, dg, h[level])
                v[1 - p, z, pl.ds(r, CHUNK), :] = centre + w[z - 1, pl.ds(r, CHUNK), :] * res
                if record is not None:
                    sq = (res * res).reshape(CHUNK // 8, 8, n).sum(axis=0)
                    acc[record, :, :] += sq

        over_planes(v, p, level, body)
        return 1 - p

    def first_sweep(level):
        v, tgt, dg, w, n = level_parts(level)

        def body(z, c):
            v[0, z + 1] = w[z] * tgt[z]
            return c

        lax.fori_loop(0, depth, body, 0)
        return 0

    def restrict0(read_chunk, store):
        def body(z):
            for r in range(0, n0, CHUNK):
                tmp0[pl.ds(r, CHUNK), :] = dot_right(read_chunk(z, r), downt0[...])
            store(z, dot_left(down0[...], tmp0[...]))
        return body

    def restrict1(z, plane):
        half = dot(down1[...], plane)
        for b in range(gy):
            spread = dot(half, cols[b]) * mask[...]
            packed = dot(group[...], spread)
            for a in range(gz):
                send_a[b, a, z : z + 1, :] = packed[a : a + 1, :]

    def exchange_all(kind, src_of, recv):
        def copy(k):
            dst = (me + k) % nd
            a, b = dst // gy, dst % gy
            return pltpu.make_async_remote_copy(
                src_ref=src_of(a, b), dst_ref=recv.at[b_me, a_me],
                send_sem=a2a_send.at[kind, k], recv_sem=a2a_recv.at[kind, me],
                device_id=(a, b), device_id_type=MESH,
            )

        def start(k, c):
            copy(k).start()
            return c

        def finish(k, c):
            copy(k).wait_send()
            src = (me + k) % nd
            a, b = src // gy, src % gy
            pltpu.make_async_remote_copy(
                src_ref=recv.at[b, a], dst_ref=recv.at[b, a],
                send_sem=a2a_send.at[kind, k], recv_sem=a2a_recv.at[kind, src],
                device_id=(a, b), device_id_type=MESH,
            ).wait_recv()
            return c

        def begin():
            lax.fori_loop(1, nd, start, 0)

        def end():
            lax.fori_loop(1, nd, finish, 0)

        return begin, end

    def to_lines(recv, dest):
        for a in range(gz):
            for b in range(gy):
                s = (a * gy + b) * depth
                dest[s : s + depth, :] = recv[b, a]

    bx2, by2 = (n1 // 2 // gz, n1 // 2 // gy)
    steps = []
    s = 1
    while s < zall:
        steps.append(s)
        s *= 2
    ns = len(steps)

    def setup_lines(offset):
        rows = lax.broadcasted_iota(jnp.int32, (zall, cp), 0)
        vert = lines[...]
        a = jnp.where(rows == 0, 0.0, -vert)
        c = jnp.where(rows == zall - 1, 0.0, -vert)
        b = diag[offset]
        for k, s in enumerate(steps):
            alpha = -a / pltpu.roll(b, s, 0)
            gamma = -c / pltpu.roll(b, zall - s, 0)
            b = b + alpha * pltpu.roll(c, s, 0) + gamma * pltpu.roll(a, zall - s, 0)
            a = alpha * pltpu.roll(a, s, 0)
            c = gamma * pltpu.roll(c, zall - s, 0)
            factor[offset, 2 * k] = alpha
            factor[offset, 2 * k + 1] = gamma
        factor[offset, 2 * ns] = 1.0 / b

    def solve(offset, right):
        for k, s in enumerate(steps):
            right = (
                right
                + factor[offset, 2 * k] * pltpu.roll(right, s, 0)
                + factor[offset, 2 * k + 1] * pltpu.roll(right, zall - s, 0)
            )
        return right * factor[offset, 2 * ns]

    count = [0]
    def line_copy(p, k):
        if k == 0:
            to, slot = ((a_me + gz - 1) % gz, b_me), 1
        elif k == 1:
            to, slot = ((a_me + 1) % gz, b_me), 0
        elif k == 2:
            to, slot = (a_me, (b_me + gy - 1) % gy), 3
        else:
            to, slot = (a_me, (b_me + 1) % gy), 2
        return pltpu.make_async_remote_copy(
            src_ref=around.at[p], dst_ref=halo.at[p, slot],
            send_sem=line_send.at[p, k], recv_sem=line_recv.at[p, slot],
            device_id=to, device_id_type=MESH,
        )

    def line_landed(p, k):
        return pltpu.make_async_remote_copy(
            src_ref=around.at[p], dst_ref=halo.at[p, k],
            send_sem=line_send.at[p, k], recv_sem=line_recv.at[p, k],
            device_id=(a_me, b_me), device_id_type=MESH,
        )

    def neighbours(offset, values):
        bx, by = bx2 >> offset, by2 >> offset
        cells = bx * by
        p = count[0] % 2
        count[0] += 1
        around[p] = values
        for k in range(4):
            @pl.when(jnp.logical_not(edges[k]))
            def _(k=k):
                line_copy(p, k).start()
        for k in range(4):
            @pl.when(jnp.logical_not(edges[k]))
            def _(k=k):
                line_copy(p, k).wait_send()
                line_landed(p, k).wait_recv()
        lane = lax.broadcasted_iota(jnp.int32, (zall, cp), 1)

        def roll(x, amount):
            amount = amount % cp
            return x if amount == 0 else pltpu.roll(x, amount, 1)

        total = jnp.where(lane < by, roll(halo[p, 0], by - cells), roll(values, by))
        total += jnp.where(lane >= cells - by, roll(halo[p, 1], cells - by), roll(values, -by))
        inrow = lane & (by - 1)
        total += jnp.where(inrow == 0, roll(halo[p, 2], 1 - by), roll(values, 1))
        total += jnp.where(inrow == by - 1, roll(halo[p, 3], by - 1), roll(values, -1))
        return total

    def line_descend(offset):
        weight = h[SWITCH + offset]
        values = solve(offset, target[offset])
        repeats = COARSE if offset == LEVELS - 1 - SWITCH else SWEEPS
        for _ in range(1, repeats):
            values = solve(offset, target[offset] + weight * neighbours(offset, values))
        if offset == LEVELS - 1 - SWITCH:
            return values
        near = neighbours(offset, values)
        rows = lax.broadcasted_iota(jnp.int32, (zall, cp), 0)
        before = jnp.where(rows == 0, 0.0, pltpu.roll(values, 1, 0))
        after = jnp.where(rows == zall - 1, 0.0, pltpu.roll(values, zall - 1, 0))
        res = target[offset] - (
            diag[offset] * values - lines[...] * (before + after) - weight * near
        )
        target[offset + 1] = dot(res, ups[2 * offset])
        tmp = values
        lower = line_descend(offset + 1)
        values = tmp + dot(lower, ups[2 * offset + 1])
        for _ in range(SWEEPS):
            values = solve(offset, target[offset] + weight * neighbours(offset, values))
        return values

    def fill0(z, c):
        w0[z] = DAMPING / (2.0 * vert_s[z] + 4.0 * h[0] + reaction[z])
        return c

    lax.fori_loop(0, depth, fill0, 0)

    def keep_r1(z, value):
        r1[z] = value
        dv = 2.0 * vert_s[z] + 4.0 * h[1] + value
        d1[z] = dv
        w1[z] = DAMPING / dv

    body = restrict0(lambda z, r: reaction[z, pl.ds(r, CHUNK), :], keep_r1)
    lax.fori_loop(0, depth, lambda z, c: (body(z), c)[1], 0)
    for z in range(depth):
        restrict1(z, r1[z])
    send_v[...] = send_a[...]
    begin_v, end_v = exchange_all(0, lambda a, b: vert_b, recv_v)
    begin_r, end_r = exchange_all(1, lambda a, b: send_v.at[b, a], recv_a)
    begin_v()
    begin_r()
    recv_v[b_me, a_me] = vert_b[...]
    recv_a[b_me, a_me] = send_v[b_me, a_me]
    acc[...] = jnp.zeros_like(acc)

    begin_a, end_a = exchange_all(2, lambda a, b: send_a.at[b, a], recv_b.at[0])
    begin_b, end_b = exchange_all(3, lambda a, b: send_n.at[b, a], recv_b.at[1])

    p0 = first_sweep(0)
    for cycle in range(CYCLES):
        for k in range(SWEEPS):
            if cycle == 0 and k == 0:
                continue
            p0 = sweep(0, p0, record=cycle - 1 if cycle > 0 and k == 0 else None)

        def read0(z, r, p0=p0):
            return residual_chunk(v0, p0, z, r, n0, source, diag0, h[0])[1]

        def keep_g1(z, value):
            g1[z - 1] = value

        over_planes(v0, p0, 0, restrict0(read0, keep_g1))
        p1 = first_sweep(1)
        for k in range(1, SWEEPS):
            p1 = sweep(1, p1)

        def keep_res(z, p1=p1):
            for r in range(0, n1, CHUNK):
                res1[z - 1, pl.ds(r, CHUNK), :] = residual_chunk(
                    v1, p1, z, r, n1, g1, diag1, h[1]
                )[1]

        over_planes(v1, p1, 1, keep_res)
        for z in range(depth):
            restrict1(z, res1[z])
        begin_a()
        recv_b[0, b_me, a_me] = send_a[b_me, a_me]
        if cycle == 0:
            end_v()
            end_r()
            to_lines(recv_v, lines)
            to_lines(recv_a, target.at[0])
            coarse = target[0]
            for offset in range(LEVELS - SWITCH):
                if offset > 0:
                    coarse = dot(coarse, ups[2 * offset - 2])
                diag[offset] = 2.0 * lines[...] + 4.0 * h[SWITCH + offset] + coarse
            for offset in range(LEVELS - SWITCH):
                setup_lines(offset)
        end_a()
        to_lines(recv_b.at[0], target.at[0])
        rowbuf[...] = line_descend(0)
        for a in range(gz):
            for b in range(gy):
                s = (a * gy + b) * depth
                send_n[b, a] = rowbuf[s : s + depth, :]
        begin_b()
        recv_b[1, b_me, a_me] = send_n[b_me, a_me]
        end_b()
        for z in range(depth):
            wide = None
            for b in range(gy):
                for a in range(gz):
                    corr1[a : a + 1, :] = recv_b[1, b, a, z : z + 1, :]
                part = dot(dot(groupt[...], corr1[...]) * mask[...], colst[b])
                wide = part if wide is None else wide + part
            v1[1 - p1, z + 1] = v1[p1, z + 1] + dot(down1[...].T * 2.0, wide)
        p1 = 1 - p1
        for _ in range(SWEEPS):
            p1 = sweep(1, p1)

        def correct0(z, c, p0=p0, p1=p1):
            tmp0[...] = dot_left(downt0[...] * 2.0, v1[p1, z])
            for r in range(0, n0, CHUNK):
                v0[1 - p0, z, pl.ds(r, CHUNK), :] = v0[p0, z, pl.ds(r, CHUNK), :] + dot_right(
                    tmp0[pl.ds(r, CHUNK), :], down0[...] * 2.0
                )
            return c

        lax.fori_loop(1, depth + 1, correct0, 0)
        p0 = 1 - p0
        for _ in range(SWEEPS):
            p0 = sweep(0, p0)

    def last(z, p0=p0):
        for r in range(0, n0, CHUNK):
            centre, res = residual_chunk(v0, p0, z, r, n0, source, diag0, h[0])
            out[z - 1, pl.ds(r, CHUNK), :] = centre
            acc[CYCLES - 1, :, :] += (res * res).reshape(CHUNK // 8, 8, n0).sum(axis=0)

    over_planes(v0, p0, 0, last)
    ridx = lax.broadcasted_iota(jnp.int32, (8, 128), 0)
    part = jnp.zeros((8, 128), jnp.float32)
    for k in range(CYCLES):
        part = jnp.where(ridx == k, jnp.sum(acc[k]), part)
    rowbuf_n = tmp_n = send_n
    target_n = recv_n
    w_n = acc
    acc[0, :, 0:128] = part
    begin_n, end_n = exchange_all(4, lambda a, b: acc.at[0, :, pl.ds(0, 128)], recv_n)
    begin_n()
    recv_n[b_me, a_me] = part
    end_n()
    total = jnp.zeros((8, 128), jnp.float32)
    for a in range(gz):
        for b in range(gy):
            total = total + recv_n[b, a]
    norms[...] = total * (1.0 / (zall * n0 * n0))


def pair_matrix(n, value):
    return (np.arange(n)[None, :] // 2 == np.arange(n // 2)[:, None]).astype(np.float32) * value


def shards(gz, gy, source, vertical, reaction):
    depth, n0 = source.shape[0], source.shape[1]
    nd = gz * gy
    zall = nd * depth
    n1, n2 = n0 // 2, n0 // 4
    bx, by = n2 // gz, n2 // gy
    cells = bx * by
    cp = -(-cells // 128) * 128
    down0 = pair_matrix(n0, 0.5)
    down1 = pair_matrix(n1, 0.5)
    lane = np.arange(cp)
    cols = np.zeros((gy, n1, cp), np.float32)
    colst = np.zeros((gy, cp, n1), np.float32)
    for b in range(gy):
        hit = (np.arange(n1)[:, None] // 2 == b * by + lane[None, :] % by) & (lane[None, :] < cells)
        cols[b] = hit * 0.5
        colst[b] = hit.T
    mask = ((lane[None, :] // by == np.arange(n2)[:, None] % bx) & (lane[None, :] < cells)).astype(np.float32)
    group = (np.arange(n2)[None, :] // bx == np.arange(gz)[:, None]).astype(np.float32)
    ups = []
    for offset in range(LEVELS - SWITCH - 1):
        fx, fy = bx >> offset, by >> offset
        cy = fy // 2
        matrix = np.zeros((cp, cp), np.float32)
        for i in range(fx):
            for j in range(fy):
                matrix[i * fy + j, (i // 2) * cy + j // 2] = 1.0
        ups += [matrix * 0.25, matrix.T]
    ups = np.stack(ups)
    steps = (zall - 1).bit_length()
    f32 = jnp.float32
    nl = LEVELS - SWITCH
    vm = pl.BlockSpec(memory_space=pltpu.VMEM)
    consts = [down0, down0.T.copy(), down1, cols, mask, group, ups, group.T.copy(), colst]
    solution, norms = pl.pallas_call(
        functools.partial(kernel, (gz, gy, depth, cp)),
        out_shape=(
            jax.ShapeDtypeStruct(source.shape, f32),
            jax.ShapeDtypeStruct((8, 128), f32),
        ),
        in_specs=[vm, vm, pl.BlockSpec(memory_space=pltpu.SMEM), vm] + [vm] * len(consts),
        out_specs=(vm, vm),
        scratch_shapes=[
            pltpu.VMEM((2, depth + 2, n0, n0), f32),
            pltpu.VMEM((2, depth + 2, n1, n1), f32),
            pltpu.VMEM((depth, n0, n0), f32),
            pltpu.VMEM((depth, n1, n1), f32),
            pltpu.VMEM((depth, n1, n1), f32),
            pltpu.VMEM((depth, n1, n1), f32),
            pltpu.VMEM((depth, n1, n1), f32),
            pltpu.VMEM((n0, n1), f32),
            pltpu.VMEM((depth, n1, n1), f32),
            pltpu.VMEM((gz, cp), f32),
            pltpu.VMEM((gy, gz, depth, cp), f32),
            pltpu.VMEM((gy, gz, depth, cp), f32),
            pltpu.VMEM((gy, gz, depth, cp), f32),
            pltpu.VMEM((gy, gz, depth, cp), f32),
            pltpu.VMEM((2, gy, gz, depth, cp), f32),
            pltpu.VMEM((gy, gz, depth, cp), f32),
            pltpu.VMEM((gy, gz, 8, 128), f32),
            pltpu.VMEM((zall, cp), f32),
            pltpu.VMEM((nl, zall, cp), f32),
            pltpu.VMEM((nl, 2 * steps + 1, zall, cp), f32),
            pltpu.VMEM((nl, zall, cp), f32),
            pltpu.VMEM((2, zall, cp), f32),
            pltpu.VMEM((2, 4, zall, cp), f32),
            pltpu.VMEM((zall, cp), f32),
            pltpu.VMEM((CYCLES, 8, n0), f32),
            pltpu.SemaphoreType.DMA((2, 2, 2)),
            pltpu.SemaphoreType.DMA((2, 2, 2)),
            pltpu.SemaphoreType.DMA((2, 4)),
            pltpu.SemaphoreType.DMA((2, 4)),
            pltpu.SemaphoreType.DMA((5, nd)),
            pltpu.SemaphoreType.DMA((5, nd)),
        ],
        compiler_params=pltpu.CompilerParams(
            has_side_effects=True, vmem_limit_bytes=64000 * 1024
        ),
    )(
        source,
        reaction,
        vertical,
        jnp.broadcast_to(vertical[:, None], (depth, cp)),
        *[jnp.asarray(c) for c in consts],
    )
    return solution, norms[:CYCLES, 0]


CROWS = 32
GROUP = 2
VMEM_LIMIT = 64000 * 1024
PAD = 8


def dot_parts(x, m, parts=2):
    total = None
    rest = x
    for k in range(parts):
        piece = rest.astype(jnp.bfloat16)
        if k + 1 < parts:
            rest = rest - piece.astype(jnp.float32)
        term = jnp.dot(piece, m, preferred_element_type=jnp.float32)
        total = term if total is None else total + term
    return total


def chain_kernel(
    dims,
    source_in, reaction_in, vertical,
    out, norms,
    source, reaction, downy, upy, up2, down3, down4, up3, up4, load,
    v0, g0, w0, d0, v1, g1, w1, d1, raw_r, raw_s, stage, turn, lines, vsend, vrecv,
    gx, cx, ex, dx, win3, win4, v2, v3, v4, g3, g4, diag, fac, mask, acc, nsend, nrecv,
    a2a_send, a2a_recv, from_sem, x_send, x_recv, w3_send, w3_recv, w4_send, w4_recv,
):
    gz, gy, depth = dims
    nd = gz * gy
    zall = nd * depth
    n0 = source.shape[1]
    n1, n2, n3, n4 = n0 // 2, n0 // 4, n0 // 8, n0 // 16
    r0, r1 = n0 // nd, n0 // 2 // nd
    nt0 = n0 // 128
    h = [COUPLING / 4.0**k for k in range(LEVELS)]
    f32 = jnp.float32
    a_me, b_me = lax.axis_index("gz"), lax.axis_index("gy")
    me = a_me * gy + b_me
    nchip = gz // 2

    def div(x, n):
        return lax.div(x, jnp.int32(n))

    def rem(x, n):
        return lax.rem(x, jnp.int32(n))

    def bend(c):
        return c + div(c, 2) - 2 * div(c, 3) if nchip == 4 else c

    def place(i):
        k, core = div(i, 2), rem(i, 2)
        b, q = div(k, nchip), rem(k, nchip)
        q = q + rem(b, 2) * (nchip - 1 - 2 * q)
        return (bend(q) * 2 + core, b)

    q_me = bend(a_me // 2)
    q_me = q_me + (b_me % 2) * (nchip - 1 - 2 * q_me)
    p = (b_me * nchip + q_me) * 2 + a_me % 2
    chip, par = p // 2, p % 2

    def loop(lo, hi, body):
        def step(i, c):
            body(i)
            return c
        lax.fori_loop(lo, hi, step, 0)

    def remote(src, dst, ss, rs, to):
        return pltpu.make_async_remote_copy(
            src_ref=src, dst_ref=dst, send_sem=ss, recv_sem=rs, device_id=to, device_id_type=MESH
        )

    def target(k):
        return rem(p + nd + (div(k, 2) + rem(k, 2)) * (1 - 2 * rem(k, 2)), nd)

    def flat(i):
        a, b = place(i)
        return a * gy + b

    def spread(kind, src_of, dst_mine, whole, each=None):
        def start(k):
            t = target(k)
            sem = a2a_recv.at[kind] if each is None else from_sem.at[me]
            remote(src_of(t), dst_mine, a2a_send.at[kind], sem, place(t)).start()

        def wait_all(recv):
            copy = remote(whole, whole, a2a_send.at[kind], a2a_recv.at[kind], place(p))
            copy.wait_recv() if recv else copy.wait_send()

        def landed(s):
            if each is None:
                wait_all(True)
            else:
                r = each(s)
                remote(r, r, a2a_send.at[kind], from_sem.at[s], place(p)).wait_recv()

        return lambda lo=1, hi=nd: loop(lo, hi, start), lambda: wait_all(False), landed

    def piece(ref, t):
        return ref.at[:, pl.ds(r0 * t, r0), :]

    def zrows(ref, s):
        return ref.at[pl.ds(depth * s, depth)]

    zrest = pl.ds(0, depth * (nd - 1))
    rest = pl.ds(0, nd - 1)
    start_v, done_v, landed_v = spread(0, lambda t: vsend, vrecv.at[me], vrecv.at[rest])
    start_r, done_r, landed_r = spread(1, lambda t: piece(reaction, t), zrows(raw_r, me), raw_r.at[zrest])
    start_s, done_s, landed_s = spread(
        2, lambda t: piece(source, t), zrows(raw_s, me), raw_s.at[zrest], lambda s: zrows(raw_s, s))
    start_o, done_o, landed_o = spread(
        3, lambda t: zrows(stage, flat(t)), piece(out, p), stage.at[zrest], lambda s: zrows(stage, s))
    start_n, done_n, landed_n = spread(4, lambda t: nsend, nrecv.at[me], nrecv.at[rest])

    load_r = pltpu.make_async_copy(reaction_in, reaction, load.at[0])
    load_s = pltpu.make_async_copy(source_in, source, load.at[1])
    load_r.start()
    load_s.start()
    for i in range(depth):
        vsend[i : i + 1, :] = jnp.full((1, 128), vertical[i], f32)
    load_r.wait()
    start_r()
    start_v()
    load_s.wait()
    start_s()

    def fill(ref, at, value):
        shape = ref.shape[-2:]
        row = lax.broadcasted_iota(jnp.int32, shape, 0)
        col = lax.broadcasted_iota(jnp.int32, shape, 1)
        hit, scale = value(row, col)
        ref[at] = jnp.where(hit, scale, 0.0).astype(jnp.bfloat16)

    fill(downy, ..., lambda r, c: (r // 2 == c, 0.25))
    fill(upy, ..., lambda r, c: (r == c // 2, 1.0))
    for i in range(r1 // 2):
        fill(up2, i, lambda r, c: (r == n2 * i + c // 2, 1.0))
    fill(down3, ..., lambda r, c: (r % n2 // 2 == c % n3, 0.25))
    fill(down4, 0, lambda r, c: ((r >= 3 * n3) & ((r - 3 * n3) // 2 == c % n4), 0.25))
    fill(down4, 1, lambda r, c: ((r < n3) & (r // 2 == c % n4), 0.25))
    fill(up3, 0, lambda r, c: (r == 3 * n3 + c % n2 // 2, 1.0))
    fill(up3, 1, lambda r, c: (r == c % n2 // 2, 1.0))
    for t in range(2):
        fill(up4, t, lambda r, c: (r == n4 * (4 + (4 * t + c // n3 + 5) // 2 - 4) + c % n3 // 2, 1.0))

    first, last = p == 0, p == nd - 1

    def xchg(kind, lo_src, lo_dst, hi_src, hi_dst):
        def down():
            return remote(lo_src, hi_dst, x_send.at[kind, 0], x_recv.at[kind, 0], place((p + nd - 1) % nd))

        def up():
            return remote(hi_src, lo_dst, x_send.at[kind, 1], x_recv.at[kind, 1], place((p + 1) % nd))

        def begin(sides=(0, 1)):
            if 0 in sides:
                @pl.when(jnp.logical_not(first))
                def _():
                    down().start()

            if 1 in sides:
                @pl.when(jnp.logical_not(last))
                def _():
                    up().start()

        def end():
            @pl.when(jnp.logical_not(first))
            def _():
                down().wait_send()
                up().wait_recv()

            @pl.when(jnp.logical_not(last))
            def _():
                up().wait_send()
                down().wait_recv()

        return begin, end

    def planes0(m, dep):
        def at(lo):
            return v0.at[m, pl.ds(lo, dep), pl.ds(PAD, zall), :]
        return xchg(m, at(2), at(2 - dep), at(2 + r0 - dep), at(2 + r0))

    def row1(kind, far):
        return xchg(kind, g1.at[2 + far], g1.at[1 - far], g1.at[r1 + 1 - far], g1.at[r1 + 2 + far])

    def planes1(ref, kind):
        return xchg(kind, ref.at[pl.ds(2, 2)], ref.at[pl.ds(0, 2)],
                    ref.at[pl.ds(r1, 2)], ref.at[pl.ds(r1 + 2, 2)])

    def far0(m):
        def at(x):
            return v0.at[m, x, pl.ds(PAD, zall), :]
        return xchg(11, at(3), at(0), at(r0), at(r0 + 3))

    def norm0():
        def at(m, x):
            return v0.at[m, x, pl.ds(PAD, zall), :]
        return xchg(1, at(2, 2), at(1, 0), at(2, r0 + 1), at(1, r0 + 3))

    def rows1():
        def at(x):
            return v1.at[0, x, pl.ds(PAD, zall), :]
        return xchg(12, at(2), at(1), at(r1 + 1), at(r1 + 2))

    def far1():
        def at(x):
            return v1.at[1, x, pl.ds(PAD, zall), :]
        return xchg(13, at(3), at(0), at(r1), at(r1 + 3))

    def blocks(ref, kind):
        return xchg(kind, ref.at[1], ref.at[0], ref.at[1], ref.at[2])

    def halo_d0():
        return xchg(5, d0.at[1], d0.at[0], d0.at[r0], d0.at[r0 + 1])

    offs3 = [(o, c) for o in (0, -1, 1, -2, 2) for c in range(2)]

    def window3(kind):
        buf = win3.at[kind]

        def out_of(o, c):
            slot = par + 3 - 2 * o
            return remote(buf.at[3 + par], buf.at[slot], w3_send.at[4 + 2 * o + c], w3_recv.at[kind // CYCLES, slot],
                          place((2 * (chip + o) + c + nd) % nd))

        def goes(o, c):
            there = jnp.logical_and(chip + o >= 0, chip + o < nd // 2)
            if o == 0:
                return par != c
            if o == -2:
                return jnp.logical_and(there, par == 0)
            if o == 2:
                return jnp.logical_and(there, par == 1)
            return there

        def begin():
            for o, c in offs3:
                @pl.when(goes(o, c))
                def _(o=o, c=c):
                    out_of(o, c).start()

        def end():
            for o, c in offs3:
                @pl.when(goes(o, c))
                def _(o=o, c=c):
                    out_of(o, c).wait_send()
            for q in range(8):
                row = 2 * chip - 3 + q
                inside = jnp.logical_and(row >= 0, row < nd)
                if q in (3, 4):
                    inside = par != q - 3

                @pl.when(inside)
                def _(q=q):
                    remote(buf.at[q], buf.at[q], w3_send.at[0], w3_recv.at[kind // CYCLES, q], place(p)).wait_recv()

        return begin, end

    offs4 = [-1, 1, -2, 2, -3, 3, -4, 4]

    def window4(kind):
        buf = win4.at[kind]

        def each(fn):
            for o in offs4:
                @pl.when(jnp.logical_and(chip + o >= 0, chip + o < nd // 2))
                def _(o=o):
                    fn(o)

        def out_of(o):
            return remote(buf.at[4], buf.at[4 - o], w4_send.at[4 + o], w4_recv.at[kind // CYCLES, 4 - o],
                          place((p + 2 * o + nd) % nd))

        def begin():
            each(lambda o: out_of(o).start())

        def end():
            def fn(o):
                out_of(o).wait_send()
                remote(buf.at[4 + o], buf.at[4 + o], w4_send.at[4 + o], w4_recv.at[kind // CYCLES, 4 + o],
                       place(p)).wait_recv()
            each(fn)

        return begin, end

    zpad = jnp.zeros((PAD, n0), f32)
    for m in range(3):
        def zero0(x, m=m):
            v0[m, x, 0:PAD, :] = zpad
            v0[m, x, PAD + zall : 2 * PAD + zall, :] = zpad
        loop(0, r0 + 4, zero0)

        def zero1(x, m=m):
            v1[m, x, 0:PAD, :] = zpad[:, :n1]
            v1[m, x, PAD + zall : 2 * PAD + zall, :] = zpad[:, :n1]
        loop(0, r1 + 4, zero1)

    tile0 = jnp.zeros((zall, 128), f32)
    plane0 = jnp.zeros((zall, n0), f32)

    def blank(lo0, x0, lo1, b):
        for q in range(2):
            for m in range(3):
                v0[m, lo0 + q, PAD : PAD + zall, :] = plane0
            v1[1, lo1 + q, PAD : PAD + zall, :] = tile0
            g1[lo1 + q] = tile0
            d1[lo1 + q] = tile0
            w1[lo1 + q] = tile0
        d0[x0] = plane0
        w0[x0] = plane0
        for k in range(CYCLES):
            gx[k, b] = tile0
            cx[k, b] = tile0
            ex[k, b] = tile0
        dx[b] = tile0

    @pl.when(first)
    def _():
        blank(0, 0, 0, 0)

    @pl.when(last)
    def _():
        blank(r0 + 2, r0 + 1, r1 + 2, 2)

    for k in range(CYCLES + 1):
        for q in range(8):
            @pl.when(jnp.logical_or(2 * chip - 3 + q < 0, 2 * chip - 3 + q >= nd))
            def _(q=q, k=k):
                win3[k, q] = jnp.zeros((n3 * zall // 128, 128), f32)
        for o in offs4:
            @pl.when(jnp.logical_or(chip + o < 0, chip + o >= nd // 2))
            def _(o=o, k=k):
                win4[k, 4 + o] = jnp.zeros((n4 * zall // 128, 128), f32)
    for q in range(2):
        v3[q, 0] = tile0
        v3[q, 3] = tile0
        v4[q, 0] = tile0
        v4[q, 3] = tile0
    v4[1, 2] = tile0
    acc[...] = jnp.zeros_like(acc)

    lane = lax.broadcasted_iota(jnp.int32, (zall, 128), 1)
    rows = lax.broadcasted_iota(jnp.int32, (zall, 128), 0)

    for t in range(3):
        good = [p > 0, None, p < nd - 1][t]
        one = jnp.ones((zall, 128), f32)
        mask[t] = one if good is None else one * good.astype(f32)
    for t in range(2):
        row = 2 * chip - 3 + 4 * t + lane // n3
        mask[3 + t] = jnp.where((row >= 0) & (row < nd), 1.0, 0.0)
        row = chip - 4 + 8 * t + lane // n4
        mask[5 + t] = jnp.where((row >= 0) & (row < nd // 2) & (row < chip + 5), 1.0, 0.0)

    def pack(rep, width):
        k = 128 // width
        zb = zall // k
        part = lane[:zb]
        got = rep[0:zb]
        for j in range(1, k):
            got = jnp.where(part // width == j, rep[zb * j : zb * (j + 1)], got)
        return got

    def unpack(slots, width):
        k = 128 // width
        zb = zall // k
        part = lane[:zb] // width
        parts = []
        for j in range(k):
            got = jnp.zeros((zb, 128), f32)
            for s, x in enumerate(slots):
                turn = (width * (s - j)) % 128
                x = x if turn == 0 else pltpu.roll(x, turn, 1)
                got = jnp.where(part == s, x, got)
            parts.append(got)
        return parts

    def unpack3(kind, dest, add=None):
        for t in range(2):
            slots = [win3[kind, 4 * t + k] for k in range(4)]
            zb = zall // 4
            for j, x in enumerate(unpack(slots, n3)):
                if add is not None:
                    x = x + add(j * zb, zb)
                dest[t, j * zb : (j + 1) * zb] = x

    def unpack4(kind, dest, add=None):
        for t in range(2):
            slots = [win4[kind, r] for r in range(8 * t, min(8 * t + 8, 9))]
            zb = zall // 8
            for j, x in enumerate(unpack(slots, n4)):
                if add is not None:
                    x = x + add(j * zb, zb)
                dest[t, j * zb : (j + 1) * zb] = x

    rawr = raw_r.reshape(zall * r0, n0)
    raws = raw_s.reshape(zall * r0, n0)
    staged = stage.reshape(zall * r0, n0)

    def unfold(raw, j):
        at = pl.ds(pl.multiple_of(PAD * r0 * j, PAD * r0), PAD * r0)
        for t in range(nt0):
            turn[t, at, :] = raw[at, 128 * t : 128 * (t + 1)]
    raw_r[pl.ds(depth * me, depth)] = reaction[:, pl.ds(r0 * p, r0), :]
    raw_s[pl.ds(depth * me, depth)] = source[:, pl.ds(r0 * p, r0), :]
    vrecv[me] = vsend[...]
    group = PAD // depth

    def each_rows(landed, body):
        def step(i):
            j = (me // group + i) % (zall // PAD)
            for k in range(group if landed is not None else 0):
                s = group * j + k

                @pl.when(s != me)
                def _():
                    landed(s)
            body(j)
        loop(0, zall // PAD, step)

    landed_v(None)
    for s in range(nd):
        lines[depth * s : depth * (s + 1), :] = vrecv[s]

    def take_r(j):
        z = pl.multiple_of(PAD * j, PAD)
        unfold(rawr, j)
        for x in range(r0):
            for t in range(nt0):
                d0[x + 1, pl.ds(z, PAD), 128 * t : 128 * (t + 1)] = turn[
                    t, pl.ds(PAD * r0 * j + x, PAD, stride=r0), :]

    landed_r(None)
    each_rows(None, take_r)

    def shrink_r(i):
        for r in range(0, zall, CROWS):
            at = pl.ds(r, CROWS)
            a, b = d0[2 * i + 1, at, :], d0[2 * i + 2, at, :]
            got = dot_parts(a + b, downy[...], 3)
            vert = lines[at, :]
            base = 2.0 * vert + 4.0 * h[1]
            w1[i + 2, at, :] = got
            d = base + got
            d1[i + 2, at, :] = d
            base = jnp.concatenate([2.0 * vert + 4.0 * h[0]] * nt0, axis=1)
            for k, x in ((1, a), (2, b)):
                x = base + x
                d0[2 * i + k, at, :] = x
                w0[2 * i + k, at, :] = DAMPING / x

    loop(0, r1, shrink_r)
    begin_d0, end_d0 = halo_d0()
    begin_d0()
    begin_d1, end_d1 = planes1(d1, 6)
    begin_d1()
    rx2 = dot_parts(jnp.concatenate([w1[2] + w1[3], w1[4] + w1[5]], axis=1), downy[...], 3)
    dx[1] = rx2
    begin_dx, end_dx = blocks(dx, 7)
    begin_dx()
    rx3 = dot_parts(rx2, down3[...], 3)
    win3[CYCLES, 3 + par] = pack(rx3, n3)
    begin_w3, end_w3 = window3(CYCLES)
    begin_w3()
    begin_w4, end_w4 = window4(CYCLES)
    loop(2, r1 + 2, lambda x: w1.__setitem__(x, DAMPING / d1[x]))

    def take_s(j):
        z = pl.multiple_of(PAD * j, PAD)
        unfold(raws, j)
        for x in range(r0):
            for t in range(nt0):
                cut = slice(128 * t, 128 * (t + 1))
                got = turn[t, pl.ds(PAD * r0 * j + x, PAD, stride=r0), :]
                g0[x + 1, pl.ds(z, PAD), cut] = got
                v0[0, x + 2, pl.ds(z + PAD, PAD), cut] = w0[x + 1, pl.ds(z, PAD), cut] * got

    each_rows(landed_s, take_s)

    ns = (zall - 1).bit_length()

    def factors(f):
        vert = lines[...]
        a = jnp.where(rows == 0, 0.0, -vert)
        c = jnp.where(rows == zall - 1, 0.0, -vert)
        b = diag[f]
        for k in range(ns):
            s = 1 << k
            inv = 1.0 / b
            alpha = -a * pltpu.roll(inv, s, 0)
            gamma = -c * pltpu.roll(inv, zall - s, 0)
            b = b + alpha * pltpu.roll(c, s, 0) + gamma * pltpu.roll(a, zall - s, 0)
            a = alpha * pltpu.roll(a, s, 0)
            c = gamma * pltpu.roll(c, zall - s, 0)
            fac[f, 2 * k] = alpha
            fac[f, 2 * k + 1] = gamma
        fac[f, 2 * ns] = mask[f] / b

    def solve(f, right):
        for k in range(ns):
            s = 1 << k
            right = (
                right
                + fac[f, 2 * k] * pltpu.roll(right, s, 0)
                + fac[f, 2 * k + 1] * pltpu.roll(right, zall - s, 0)
            )
        return right * fac[f, 2 * ns]

    def near(v, q, b, width):
        t = v[q, b]
        below = pltpu.roll(jnp.where(lane >= 128 - width, v[q, b - 1], t), width, 1)
        above = pltpu.roll(jnp.where(lane < width, v[q, b + 1], t), 128 - width, 1)
        inrow = lane % width
        left = jnp.where(inrow == 0, 0.0, pltpu.roll(t, 1, 1))
        right = jnp.where(inrow == width - 1, 0.0, pltpu.roll(t, 127, 1))
        return (below + above) + (left + right)

    edge = lax.broadcasted_iota(jnp.int32, (CROWS, 128), 1)
    level0 = (v0, g0, w0, d0, nt0, h[0], 1)
    level1 = (v1, g1, w1, d1, 1, h[1], 2)

    def stencil(level, m, x, r):
        v, g, w, d, nt, weight, go = level
        centre, turn_r, turn_l = [], [], []
        for t in range(nt):
            cut = slice(128 * t, 128 * (t + 1))
            c = v[m, x + 2, PAD + r : PAD + r + CROWS, cut]
            centre.append(c)
            turn_r.append(pltpu.roll(c, 1, 1))
            turn_l.append(pltpu.roll(c, 127, 1))
        vert = lines[r : r + CROWS, :]
        got = []
        for t in range(nt):
            cut = slice(128 * t, 128 * (t + 1))
            left = jnp.where(edge == 0, turn_r[t - 1] if t else 0.0, turn_r[t])
            right = jnp.where(edge == 127, turn_l[t + 1] if t + 1 < nt else 0.0, turn_l[t])
            side = (v[m, x + 1, PAD + r : PAD + r + CROWS, cut] + v[m, x + 3, PAD + r : PAD + r + CROWS, cut]) + (left + right)
            if weight != 1.0:
                side = weight * side
            ends = v[m, x + 2, PAD + r - 1 : PAD + r - 1 + CROWS, cut] + v[m, x + 2, PAD + r + 1 : PAD + r + 1 + CROWS, cut]
            got.append(g[x + go, r : r + CROWS, cut] + side + vert * ends)
        return centre, got

    def sweep_plane(level, m, q, x, record=None, put=None):
        v, g, w, d, nt, weight, go = level
        for lo in range(0, zall, GROUP * CROWS):
            new = []
            for r in range(lo, lo + GROUP * CROWS, CROWS):
                centre, got = stencil(level, m, x, r)
                for t in range(nt):
                    cut = slice(128 * t, 128 * (t + 1))
                    wt = w[x + go, r : r + CROWS, cut]
                    if record is None:
                        value = (1.0 - DAMPING) * centre[t] + wt * got[t]
                    else:
                        res = got[t] - d[x + go, r : r + CROWS, cut] * centre[t]
                        value = centre[t] + wt * res
                        acc[record] += (res * res).reshape(CROWS // 8, 8, 128).sum(axis=0)
                    new.append((r, t, value))
            for r, t, value in new:
                v[q, x + 2, PAD + r : PAD + r + CROWS, 128 * t : 128 * (t + 1)] = value
                if put is not None:
                    for e in range(0, CROWS, 8):
                        put(x, r + e, t, value[e : e + 8])

    def residual(level, m, x, r):
        v, g, w, d, nt, weight, go = level
        centre, got = stencil(level, m, x, r)
        res = [
            got[t] - d[x + go, r : r + CROWS, 128 * t : 128 * (t + 1)] * centre[t] for t in range(nt)]
        return res

    def sweeps(level, m, q, xs, record=None, put=None):
        lo, hi, fn = xs
        loop(lo, hi, lambda i: sweep_plane(level, m, q, fn(i), record, put))

    def restrict0(m, lo, hi, fn):
        def body(i):
            i = fn(i)
            for r in range(0, zall, CROWS):
                a = residual(level0, m, 2 * i, r)
                b = residual(level0, m, 2 * i + 1, r)
                both = jnp.concatenate([s + t for s, t in zip(a, b)], axis=1)
                g1[i + 2, r : r + CROWS, :] = dot_parts(both, downy[...])
        loop(lo, hi, body)

    def same(i):
        return i

    def pair0(m, q, then, record=None, hook=None, put=None, restrict=False, fix=None):
        if fix is None:
            end = planes0(m, 2)[1]
        else:
            end = rows1()[1]
            far0(fix)[1]()
            correct0(fix, m, 0, r1, same)
        if hook is not None:
            hook[0]()
        sweeps(level0, m, 1, (1, r0 - 1, same), record)
        if restrict:
            restrict0(1, 1, r1 - 1, same)
            row1(3, 1)[0]()
        else:
            sweeps(level0, 1, q, (2, r0 - 2, same), None, put)
        end()
        if hook is not None:
            hook[1]()
        for side in range(2):
            if fix is not None:
                correct0(fix, m, 0, 1, lambda i: r1 if side else -1)
            sweep_plane(level0, m, 1, r0 if side else -1)
            sweep_plane(level0, m, 1, r0 - 1 if side else 0, record)
            if restrict:
                restrict0(1, 0, 1, lambda i: r1 - 1 if side else 0)
            else:
                for k in range(2):
                    sweep_plane(level0, 1, q, r0 - 2 + k if side else k, None, put)
            then((side,))

    def halo_factors():
        end_dx()
        for t in range(3):
            diag[t] = 2.0 * lines[...] + 4.0 * h[2] + dx[t]
        loop(0, 3, factors)
        for k in range(2 * ns + 1):
            fac[7, k] = jnp.where(lane >= n2, fac[0, k], fac[2, k])
        end_w3()
        unpack3(CYCLES, g3)
        win4[CYCLES, 4] = pack(
            dot_parts(g3[0], down4[0], 3) + dot_parts(g3[1], down4[1], 3), n4)
        begin_w4()

    def window_factors():
        def add(level):
            return lambda r, n: 2.0 * lines[r : r + n, :] + 4.0 * h[level]
        for t in range(2):
            diag[3 + t] = 2.0 * lines[...] + 4.0 * h[3] + g3[t]
        loop(3, 5, factors)
        end_w4()
        unpack4(CYCLES, diag.at[pl.ds(5, 2)], add(4))
        loop(5, 7, factors)

    def halo_level0():
        end_d0()
        for x, inside in ((0, jnp.logical_not(first)), (r0 + 1, jnp.logical_not(last))):
            @pl.when(inside)
            def _(x=x):
                w0[x] = DAMPING / d0[x]
            g0[x] = v0[0, x + 1, PAD : PAD + zall, :] * d0[x] * (1.0 / DAMPING)

    def halo_level1():
        end_d1()
        for x, inside in ((0, jnp.logical_not(first)), (r1 + 2, jnp.logical_not(last))):
            @pl.when(inside)
            def _(x=x):
                for q in range(2):
                    w1[x + q] = DAMPING / d1[x + q]

    def coarse(cycle, m):
        end = row1(10, 0)[1]
        far0(m)[0]()
        if cycle == 0:
            window_factors()
        loop(2, r1 + 2, lambda x: v1.__setitem__((0, x, pl.ds(PAD, zall)), w1[x] * g1[x]))
        row1(3, 1)[1]()
        end()
        if cycle == 0:
            halo_level1()
        for x in (0, 1, r1 + 2, r1 + 3):
            v1[0, x, PAD : PAD + zall] = w1[x] * g1[x]
        sweeps(level1, 0, 1, (-1, r1 + 1, same))

        pairs = []
        for i in range(r1 // 2):
            cuts = []
            for r in range(0, zall, CROWS):
                a = residual(level1, 1, 2 * i, r)[0]
                b = residual(level1, 1, 2 * i + 1, r)[0]
                cuts.append(a + b)
            pairs.append(jnp.concatenate(cuts, axis=0))
        gx[cycle, 1] = dot_parts(jnp.concatenate(pairs, axis=1), downy[...])
        e2 = lines2(cycle, far1()[0])
        ex[cycle, 1] = e2
        begin, end = blocks(ex.at[cycle], 4)
        begin()

        for i in range(r1 // 2):
            e = dot_parts(e2, up2[i])
            for x in (2 * i, 2 * i + 1):
                v1[2, x + 2, PAD : PAD + zall] = v1[1, x + 2, PAD : PAD + zall] + e
        far1()[1]()
        sweeps(level1, 2, 1, (1, r1 - 1, same))
        end()
        for side in range(2):
            e = dot_parts(ex[cycle, 2], up2[0]) if side else dot_parts(ex[cycle, 0], up2[r1 // 2 - 1])
            for x in (r1 + 2, r1 + 3) if side else (0, 1):
                v1[2, x, PAD : PAD + zall] = v1[1, x, PAD : PAD + zall] + e
        for x in (-1, 0, r1 - 1, r1):
            sweep_plane(level1, 2, 1, x)
        for x in (0, r1 - 1):
            sweep_plane(level1, 1, 0, x)
        rows1()[0]()
        sweeps(level1, 1, 0, (1, r1 - 1, same))

    def lines_sweep(v, q, s, lo, hi, right, f, weight, width):
        for b in range(lo, hi):
            v[s, b] = solve(f + b - 1, right[b - 1] + weight * near(v, q, b, width))

    def line_residual(v, q, b, right, f, weight, width):
        values = v[q, b]
        before = jnp.where(rows == 0, 0.0, pltpu.roll(values, 1, 0))
        after = jnp.where(rows == zall - 1, 0.0, pltpu.roll(values, zall - 1, 0))
        return right[b - 1] + weight * near(v, q, b, width) + lines[...] * (before + after) - diag[f + b - 1] * values

    def beside(t):
        inrow = lane % n2
        return jnp.where(inrow == 0, 0.0, pltpu.roll(t, 1, 1)) + jnp.where(inrow == n2 - 1, 0.0, pltpu.roll(t, 127, 1))

    def pair2(left, own, right, right_own, right_rim):
        upper = lane >= n2
        rim = jnp.where(upper, left, right)
        far = jnp.where(upper, right, left)
        new = solve(1, right_own + h[2] * (beside(own) + pltpu.roll(own + rim, n2, 1)))
        return new, solve(7, right_rim + h[2] * (beside(rim) + pltpu.roll(own + far, n2, 1)))

    def lines2(cycle, after):
        right = gx.at[cycle]
        begin, end = blocks(right, 8)
        begin()
        after()
        v2[1] = solve(1, right[1])
        end()
        for b in (0, 2):
            v2[b] = solve(b, right[b])
        right_rim = jnp.where(lane >= n2, right[0], right[2])
        v2[3], v2[4] = pair2(v2[0], v2[1], v2[2], right[1], right_rim)
        own = v2[3]
        before = jnp.where(rows == 0, 0.0, pltpu.roll(own, 1, 0))
        after = jnp.where(rows == zall - 1, 0.0, pltpu.roll(own, zall - 1, 0))
        around = beside(own) + pltpu.roll(own + v2[4], n2, 1)
        res = right[1] + h[2] * around + lines[...] * (before + after) - diag[1] * own
        win3[cycle, 3 + par] = pack(dot_parts(res, down3[...]), n3)
        e3 = lines3(cycle)
        cx[cycle, 1] = v2[3] + dot_parts(e3, up3[par])
        begin, end = blocks(cx.at[cycle], 9)
        begin()
        end()
        v2[0], v2[1] = pair2(cx[cycle, 0], cx[cycle, 1], cx[cycle, 2], right[1], jnp.where(lane >= n2, right[0], right[2]))
        return solve(1, right[1] + h[2] * (beside(v2[0]) + pltpu.roll(v2[0] + v2[1], n2, 1)))

    def lines3(cycle):
        begin, end = window3(cycle)
        begin()
        end()
        unpack3(cycle, g3)
        loop(1, 3, lambda b: v3.__setitem__((0, b), solve(3 + b - 1, g3[b - 1])))
        lines_sweep(v3, 0, 1, 1, 3, g3, 3, h[3], n3)
        both = None
        for t in range(2):
            part = dot_parts(line_residual(v3, 1, t + 1, g3, 3, h[3], n3), down4[t])
            both = part if both is None else both + part
        win4[cycle, 4] = pack(both, n4)
        e4 = lines4(cycle)
        for t in range(2):
            v3[0, t + 1] = v3[1, t + 1] + dot_parts(e4, up4[t])
        lines_sweep(v3, 0, 1, 1, 3, g3, 3, h[3], n3)
        return solve(3 + par, g3[par] + h[3] * near(v3, 1, 1 + par, n3))

    def lines4(cycle):
        begin, end = window4(cycle)
        begin()
        end()
        unpack4(cycle, g4)
        loop(1, 3, lambda b: v4.__setitem__((0, b), solve(5 + b - 1, g4[b - 1])))
        q = 0
        for k in range(1, COARSE - 1):
            v4[1 - q, 1] = solve(5, g4[0] + h[4] * near(v4, q, 1, n4))
            q = 1 - q
        return solve(5, g4[0] + h[4] * near(v4, q, 1, n4))

    def correct0(m, q, lo, hi, fn):
        def body(i):
            i = fn(i)
            for r in range(0, zall, CROWS):
                e = dot_parts(v1[0, i + 2, PAD + r : PAD + r + CROWS, :], upy[...])
                for x in (2 * i + 2, 2 * i + 3):
                    v0[q, x, PAD + r : PAD + r + CROWS, :] = v0[m, x, PAD + r : PAD + r + CROWS, :] + e
        loop(lo, hi, body)

    def put(x, z, t, value):
        turn[t, pl.ds(z * r0 + x, 8, stride=r0), :] = value

    def fold(j):
        at = pl.ds(pl.multiple_of(PAD * r0 * j, PAD * r0), PAD * r0)
        for t in range(nt0):
            staged[at, 128 * t : 128 * (t + 1)] = turn[t, at, :]

    planes0(0, 2)[0]()
    pair0(0, 1, row1(10, 0)[0], hook=(halo_factors, halo_level0), restrict=True)
    coarse(0, 1)
    pair0(2, 0, planes0(0, 2)[0], fix=1)
    pair0(0, 2, planes0(2, 1)[0], record=0)
    end = planes0(2, 1)[1]
    restrict0(2, 1, r1 - 1, same)
    row1(3, 1)[0]()
    end()
    for side in range(2):
        restrict0(2, 0, 1, lambda i: r1 - 1 if side else 0)
        row1(10, 0)[0]((side,))
    coarse(1, 2)
    pair0(0, 2, norm0()[0], put=put, fix=2)
    loop(0, zall // PAD, fold)
    end = norm0()[1]
    start_o(1, nd * 5 // 8)
    keep = pltpu.make_async_copy(zrows(stage, me), piece(out, p), load.at[2])
    keep.start()

    def last_norm(x):
        for r in range(0, zall, CROWS):
            for res in residual(level0, 2, x, r):
                acc[CYCLES - 1] += (res * res).reshape(CROWS // 8, 8, 128).sum(axis=0)

    loop(1, r0 - 1, last_norm)
    end()
    for x, y in ((1, 0), (r0 + 2, r0 + 3)):
        v0[2, x, PAD : PAD + zall, :] = v0[1, y, PAD : PAD + zall, :]
    loop(0, 2, lambda i: last_norm(i * (r0 - 1)))
    ridx = lax.broadcasted_iota(jnp.int32, (8, 128), 0)
    part = jnp.zeros((8, 128), f32)
    for k in range(CYCLES):
        part = jnp.where(ridx == k, jnp.sum(acc[k]), part)
    nsend[...] = part
    start_n()
    start_o(nd * 5 // 8, nd)
    total = part
    done_v()
    done_r()
    done_s()

    def finish(s):
        @pl.when(s != me)
        def _():
            landed_o(s)
    loop(0, nd, finish)
    landed_n(None)
    nrecv[me] = part
    total = jnp.sum(nrecv[...], axis=0)
    for k in range(CYCLES):
        norms[k] = total[k, 0] * (1.0 / (zall * n0 * n0))
    keep.wait()
    done_o()
    done_n()


def chain_shards(gz, gy, source, vertical, reaction):
    depth, n0 = source.shape[0], source.shape[1]
    nd = gz * gy
    zall = nd * depth
    n1, n2, n3, n4 = n0 // 2, n0 // 4, n0 // 8, n0 // 16
    r0, r1 = n0 // nd, n1 // nd
    f32 = jnp.float32
    bf16 = jnp.bfloat16

    sm = pl.BlockSpec(memory_space=pltpu.SMEM)
    ns = (zall - 1).bit_length()
    dma = pltpu.SemaphoreType.DMA
    solution, norms = pl.pallas_call(
        functools.partial(chain_kernel, (gz, gy, depth)),
        out_shape=(
            pltpu.VMEM(source.shape, f32),
            jax.ShapeDtypeStruct((CYCLES,), f32),
        ),
        in_specs=[pl.BlockSpec(memory_space=pltpu.HBM)] * 2 + [sm],
        out_specs=(pl.BlockSpec(memory_space=pltpu.VMEM), sm),
        scratch_shapes=[
            pltpu.VMEM(source.shape, f32),
            pltpu.VMEM(source.shape, f32),
            pltpu.VMEM((n0, n1), bf16),
            pltpu.VMEM((n1, n0), bf16),
            pltpu.VMEM((r1 // 2, 128, n1), bf16),
            pltpu.VMEM((128, 128), bf16),
            pltpu.VMEM((2, 128, 128), bf16),
            pltpu.VMEM((2, 128, 128), bf16),
            pltpu.VMEM((2, 128, 128), bf16),
            pltpu.SemaphoreType.DMA((3,)),
            pltpu.VMEM((3, r0 + 4, zall + 2 * PAD, n0), f32),
            pltpu.VMEM((r0 + 2, zall, n0), f32),
            pltpu.VMEM((r0 + 2, zall, n0), f32),
            pltpu.VMEM((r0 + 2, zall, n0), f32),
            pltpu.VMEM((3, r1 + 4, zall + 2 * PAD, n1), f32),
            pltpu.VMEM((r1 + 4, zall, n1), f32),
            pltpu.VMEM((r1 + 4, zall, n1), f32),
            pltpu.VMEM((r1 + 4, zall, n1), f32),
            pltpu.VMEM((zall, r0, n0), f32),
            pltpu.VMEM((zall, r0, n0), f32),
            pltpu.VMEM((zall, r0, n0), f32),
            pltpu.VMEM((n0 // 128, zall * r0, 128), f32),
            pltpu.VMEM((zall, 128), f32),
            pltpu.VMEM((depth, 128), f32),
            pltpu.VMEM((nd, depth, 128), f32),
            pltpu.VMEM((CYCLES, 3, zall, 128), f32),
            pltpu.VMEM((CYCLES, 3, zall, 128), f32),
            pltpu.VMEM((CYCLES, 3, zall, 128), f32),
            pltpu.VMEM((3, zall, 128), f32),
            pltpu.VMEM((CYCLES + 1, 8, n3 * zall // 128, 128), f32),
            pltpu.VMEM((CYCLES + 1, 9, n4 * zall // 128, 128), f32),
            pltpu.VMEM((5, zall, 128), f32),
            pltpu.VMEM((2, 4, zall, 128), f32),
            pltpu.VMEM((2, 4, zall, 128), f32),
            pltpu.VMEM((2, zall, 128), f32),
            pltpu.VMEM((2, zall, 128), f32),
            pltpu.VMEM((7, zall, 128), f32),
            pltpu.VMEM((8, 2 * ns + 1, zall, 128), f32),
            pltpu.VMEM((7, zall, 128), f32),
            pltpu.VMEM((CYCLES, 8, 128), f32),
            pltpu.VMEM((8, 128), f32),
            pltpu.VMEM((nd, 8, 128), f32),
            dma((5,)),
            dma((5,)),
            dma((nd,)),
            dma((14, 2)),
            dma((14, 2)),
            dma((10,)),
            dma((2, 8)),
            dma((9,)),
            dma((2, 9)),
        ],
        compiler_params=pltpu.CompilerParams(
            has_side_effects=True, vmem_limit_bytes=VMEM_LIMIT
        ),
    )(source, reaction, vertical)
    return solution, norms


def shards_of(gz, gy, source, vertical, reaction):
    depth, n0 = source.shape[0], source.shape[1]
    nd = gz * gy
    fits = (
        gz % 2 == 0 and n0 % (8 * nd) == 0 and n0 // nd == 8 and n0 % 256 == 0 and n0 // 4 * 2 == 128
        and PAD % depth == 0 and nd * depth % 128 == 0 and (LEVELS, SWITCH, SWEEPS, COARSE, CYCLES) == (5, 2, 2, 4, 2)
    )
    return (chain_shards if fits else shards)(gz, gy, source, vertical, reaction)


def solution(mesh):
    return jax.shard_map(
        functools.partial(shards_of, mesh.shape["gz"], mesh.shape["gy"]),
        mesh=mesh,
        in_specs=(P(("gz", "gy"), None, None), P(("gz", "gy")), P(("gz", "gy"), None, None)),
        out_specs=(P(("gz", "gy"), None, None), P()),
        check_vma=False,
    )
```

```python
import functools

import jax
import jax.numpy as jnp
import numpy as np
from jax import lax
from jax.experimental import pallas as pl
from jax.experimental.pallas import tpu as pltpu
from jax.sharding import PartitionSpec as P

LEVELS = 5
SWITCH = 2
CYCLES = 2
SWEEPS = 2
COARSE = 4
DAMPING = 0.8
COUPLING = 1.0
CHUNK = 32
MESH = pl.DeviceIdType.MESH


def dot(a, b):
    return lax.dot_general(
        a,
        b,
        (((1,), (0,)), ((), ())),
        precision=lax.Precision.HIGHEST,
        preferred_element_type=jnp.float32,
    )


def parts_of(x):
    first = x.astype(jnp.bfloat16)
    rest = x - first.astype(jnp.float32)
    second = rest.astype(jnp.bfloat16)
    third = (rest - second.astype(jnp.float32)).astype(jnp.bfloat16)
    return (third, second, first)


def dot_right(x, m):
    m = m.astype(jnp.bfloat16)
    total = None
    for x in parts_of(x):
        term = jnp.dot(x, m, preferred_element_type=jnp.float32)
        total = term if total is None else total + term
    return total


def dot_left(m, x):
    m = m.astype(jnp.bfloat16)
    total = None
    for x in parts_of(x):
        term = jnp.dot(m, x, preferred_element_type=jnp.float32)
        total = term if total is None else total + term
    return total


def kernel(
    dims,
    source, reaction, vert_s, vert_b, down0, downt0, down1, cols, mask, group, ups, groupt, colst,
    out, norms,
    v0, v1, w0, d1, w1, g1, r1, tmp0, res1, corr1, send_a, recv_a, send_v, recv_v, recv_b,
    send_n, recv_n, lines, diag, factor, target, around, halo, rowbuf, acc,
    plane_send, plane_recv, line_send, line_recv, a2a_send, a2a_recv,
):
    gz, gy, depth, cp = dims
    nd = gz * gy
    zall = nd * depth
    n0 = source.shape[1]
    n1 = n0 // 2
    a_me = lax.axis_index("gz")
    b_me = lax.axis_index("gy")
    me = a_me * gy + b_me
    h = [COUPLING / 4.0**k for k in range(LEVELS)]

    @pl.when(me == 0)
    def _():
        for p in range(2):
            v0[p, 0] = jnp.zeros((n0, n0), jnp.float32)
            v1[p, 0] = jnp.zeros((n1, n1), jnp.float32)

    @pl.when(me == nd - 1)
    def _():
        for p in range(2):
            v0[p, depth + 1] = jnp.zeros((n0, n0), jnp.float32)
            v1[p, depth + 1] = jnp.zeros((n1, n1), jnp.float32)

    edges = [a_me == 0, a_me == gz - 1, b_me == 0, b_me == gy - 1]
    for k in range(4):
        @pl.when(edges[k])
        def _(k=k):
            for p in range(2):
                halo[p, k] = jnp.zeros((zall, cp), jnp.float32)

    def flat(d):
        return (d // gy, d % gy)

    def plane_copy(v, p, level, up):
        if up:
            src, dst, to = v.at[p, depth], v.at[p, 0], flat(me + 1)
        else:
            src, dst, to = v.at[p, 1], v.at[p, depth + 1], flat(me + nd - 1 - nd * ((me + nd - 1) // nd))
        if up:
            to = flat((me + 1) % nd)
        k = 0 if up else 1
        return pltpu.make_async_remote_copy(
            src_ref=src, dst_ref=dst,
            send_sem=plane_send.at[level, p, k], recv_sem=plane_recv.at[level, p, k],
            device_id=to, device_id_type=MESH,
        )

    def plane_start(v, p, level):
        @pl.when(me < nd - 1)
        def _():
            plane_copy(v, p, level, True).start()

        @pl.when(me > 0)
        def _():
            plane_copy(v, p, level, False).start()

    def plane_wait(v, p, level):
        @pl.when(me < nd - 1)
        def _():
            plane_copy(v, p, level, True).wait_send()
            plane_copy(v, p, level, False).wait_recv()

        @pl.when(me > 0)
        def _():
            plane_copy(v, p, level, False).wait_send()
            plane_copy(v, p, level, True).wait_recv()

    def residual_chunk(v, p, z, r, n, target_ref, diag_of, weight):
        centre = v[p, z, pl.ds(r, CHUNK), :]
        rows = lax.broadcasted_iota(jnp.int32, (CHUNK, n), 0)
        lanes = lax.broadcasted_iota(jnp.int32, (CHUNK, n), 1)
        if r == 0:
            above = jnp.where(rows == 0, 0.0, pltpu.roll(centre, 1, 0))
        else:
            above = v[p, z, pl.ds(r - 1, CHUNK), :]
        if r + CHUNK == n:
            below = jnp.where(rows == CHUNK - 1, 0.0, pltpu.roll(centre, CHUNK - 1, 0))
        else:
            below = v[p, z, pl.ds(r + 1, CHUNK), :]
        left = jnp.where(lanes == 0, 0.0, pltpu.roll(centre, 1, 1))
        right = jnp.where(lanes == n - 1, 0.0, pltpu.roll(centre, n - 1, 1))
        vert = vert_s[z - 1]
        applied = (
            diag_of(z - 1, r, vert) * centre
            - vert * (v[p, z - 1, pl.ds(r, CHUNK), :] + v[p, z + 1, pl.ds(r, CHUNK), :])
            - weight * (above + below + left + right)
        )
        return centre, target_ref[z - 1, pl.ds(r, CHUNK), :] - applied

    def diag0(z, r, vert):
        return 2.0 * vert + 4.0 * h[0] + reaction[z, pl.ds(r, CHUNK), :]

    def diag1(z, r, vert):
        return d1[z, pl.ds(r, CHUNK), :]

    def over_planes(v, p, level, body):
        plane_start(v, p, level)

        def inner(z, c):
            body(z)
            return c

        lax.fori_loop(2, depth, inner, 0)
        plane_wait(v, p, level)

        def outer(i, c):
            body(1 + i * (depth - 1))
            return c

        lax.fori_loop(0, 2, outer, 0)

    def level_parts(level):
        if level == 0:
            return v0, source, diag0, w0, n0
        return v1, g1, diag1, w1, n1

    def sweep(level, p, record=None):
        v, tgt, dg, w, n = level_parts(level)

        def body(z):
            for r in range(0, n, CHUNK):
                centre, res = residual_chunk(v, p, z, r, n, tgt, dg, h[level])
                v[1 - p, z, pl.ds(r, CHUNK), :] = centre + w[z - 1, pl.ds(r, CHUNK), :] * res
                if record is not None:
                    sq = (res * res).reshape(CHUNK // 8, 8, n).sum(axis=0)
                    acc[record, :, :] += sq

        over_planes(v, p, level, body)
        return 1 - p

    def first_sweep(level):
        v, tgt, dg, w, n = level_parts(level)

        def body(z, c):
            v[0, z + 1] = w[z] * tgt[z]
            return c

        lax.fori_loop(0, depth, body, 0)
        return 0

    def restrict0(read_chunk, store):
        def body(z):
            for r in range(0, n0, CHUNK):
                tmp0[pl.ds(r, CHUNK), :] = dot_right(read_chunk(z, r), downt0[...])
            store(z, dot_left(down0[...], tmp0[...]))
        return body

    def restrict1(z, plane):
        half = dot(down1[...], plane)
        for b in range(gy):
            spread = dot(half, cols[b]) * mask[...]
            packed = dot(group[...], spread)
            for a in range(gz):
                send_a[b, a, z : z + 1, :] = packed[a : a + 1, :]

    def exchange_all(kind, src_of, recv):
        def copy(k):
            dst = (me + k) % nd
            a, b = dst // gy, dst % gy
            return pltpu.make_async_remote_copy(
                src_ref=src_of(a, b), dst_ref=recv.at[b_me, a_me],
                send_sem=a2a_send.at[kind, k], recv_sem=a2a_recv.at[kind, me],
                device_id=(a, b), device_id_type=MESH,
            )

        def start(k, c):
            copy(k).start()
            return c

        def finish(k, c):
            copy(k).wait_send()
            src = (me + k) % nd
            a, b = src // gy, src % gy
            pltpu.make_async_remote_copy(
                src_ref=recv.at[b, a], dst_ref=recv.at[b, a],
                send_sem=a2a_send.at[kind, k], recv_sem=a2a_recv.at[kind, src],
                device_id=(a, b), device_id_type=MESH,
            ).wait_recv()
            return c

        def begin():
            lax.fori_loop(1, nd, start, 0)

        def end():
            lax.fori_loop(1, nd, finish, 0)

        return begin, end

    def to_lines(recv, dest):
        for a in range(gz):
            for b in range(gy):
                s = (a * gy + b) * depth
                dest[s : s + depth, :] = recv[b, a]

    bx2, by2 = (n1 // 2 // gz, n1 // 2 // gy)
    steps = []
    s = 1
    while s < zall:
        steps.append(s)
        s *= 2
    ns = len(steps)

    def setup_lines(offset):
        rows = lax.broadcasted_iota(jnp.int32, (zall, cp), 0)
        vert = lines[...]
        a = jnp.where(rows == 0, 0.0, -vert)
        c = jnp.where(rows == zall - 1, 0.0, -vert)
        b = diag[offset]
        for k, s in enumerate(steps):
            alpha = -a / pltpu.roll(b, s, 0)
            gamma = -c / pltpu.roll(b, zall - s, 0)
            b = b + alpha * pltpu.roll(c, s, 0) + gamma * pltpu.roll(a, zall - s, 0)
            a = alpha * pltpu.roll(a, s, 0)
            c = gamma * pltpu.roll(c, zall - s, 0)
            factor[offset, 2 * k] = alpha
            factor[offset, 2 * k + 1] = gamma
        factor[offset, 2 * ns] = 1.0 / b

    def solve(offset, right):
        for k, s in enumerate(steps):
            right = (
                right
                + factor[offset, 2 * k] * pltpu.roll(right, s, 0)
                + factor[offset, 2 * k + 1] * pltpu.roll(right, zall - s, 0)
            )
        return right * factor[offset, 2 * ns]

    count = [0]
    def line_copy(p, k):
        if k == 0:
            to, slot = ((a_me + gz - 1) % gz, b_me), 1
        elif k == 1:
            to, slot = ((a_me + 1) % gz, b_me), 0
        elif k == 2:
            to, slot = (a_me, (b_me + gy - 1) % gy), 3
        else:
            to, slot = (a_me, (b_me + 1) % gy), 2
        return pltpu.make_async_remote_copy(
            src_ref=around.at[p], dst_ref=halo.at[p, slot],
            send_sem=line_send.at[p, k], recv_sem=line_recv.at[p, slot],
            device_id=to, device_id_type=MESH,
        )

    def line_landed(p, k):
        return pltpu.make_async_remote_copy(
            src_ref=around.at[p], dst_ref=halo.at[p, k],
            send_sem=line_send.at[p, k], recv_sem=line_recv.at[p, k],
            device_id=(a_me, b_me), device_id_type=MESH,
        )

    def neighbours(offset, values):
        bx, by = bx2 >> offset, by2 >> offset
        cells = bx * by
        p = count[0] % 2
        count[0] += 1
        around[p] = values
        for k in range(4):
            @pl.when(jnp.logical_not(edges[k]))
            def _(k=k):
                line_copy(p, k).start()
        for k in range(4):
            @pl.when(jnp.logical_not(edges[k]))
            def _(k=k):
                line_copy(p, k).wait_send()
                line_landed(p, k).wait_recv()
        lane = lax.broadcasted_iota(jnp.int32, (zall, cp), 1)

        def roll(x, amount):
            amount = amount % cp
            return x if amount == 0 else pltpu.roll(x, amount, 1)

        total = jnp.where(lane < by, roll(halo[p, 0], by - cells), roll(values, by))
        total += jnp.where(lane >= cells - by, roll(halo[p, 1], cells - by), roll(values, -by))
        inrow = lane & (by - 1)
        total += jnp.where(inrow == 0, roll(halo[p, 2], 1 - by), roll(values, 1))
        total += jnp.where(inrow == by - 1, roll(halo[p, 3], by - 1), roll(values, -1))
        return total

    def line_descend(offset):
        weight = h[SWITCH + offset]
        values = solve(offset, target[offset])
        repeats = COARSE if offset == LEVELS - 1 - SWITCH else SWEEPS
        for _ in range(1, repeats):
            values = solve(offset, target[offset] + weight * neighbours(offset, values))
        if offset == LEVELS - 1 - SWITCH:
            return values
        near = neighbours(offset, values)
        rows = lax.broadcasted_iota(jnp.int32, (zall, cp), 0)
        before = jnp.where(rows == 0, 0.0, pltpu.roll(values, 1, 0))
        after = jnp.where(rows == zall - 1, 0.0, pltpu.roll(values, zall - 1, 0))
        res = target[offset] - (
            diag[offset] * values - lines[...] * (before + after) - weight * near
        )
        target[offset + 1] = dot(res, ups[2 * offset])
        tmp = values
        lower = line_descend(offset + 1)
        values = tmp + dot(lower, ups[2 * offset + 1])
        for _ in range(SWEEPS):
            values = solve(offset, target[offset] + weight * neighbours(offset, values))
        return values

    def fill0(z, c):
        w0[z] = DAMPING / (2.0 * vert_s[z] + 4.0 * h[0] + reaction[z])
        return c

    lax.fori_loop(0, depth, fill0, 0)

    def keep_r1(z, value):
        r1[z] = value
        dv = 2.0 * vert_s[z] + 4.0 * h[1] + value
        d1[z] = dv
        w1[z] = DAMPING / dv

    body = restrict0(lambda z, r: reaction[z, pl.ds(r, CHUNK), :], keep_r1)
    lax.fori_loop(0, depth, lambda z, c: (body(z), c)[1], 0)
    for z in range(depth):
        restrict1(z, r1[z])
    send_v[...] = send_a[...]
    begin_v, end_v = exchange_all(0, lambda a, b: vert_b, recv_v)
    begin_r, end_r = exchange_all(1, lambda a, b: send_v.at[b, a], recv_a)
    begin_v()
    begin_r()
    recv_v[b_me, a_me] = vert_b[...]
    recv_a[b_me, a_me] = send_v[b_me, a_me]
    acc[...] = jnp.zeros_like(acc)

    begin_a, end_a = exchange_all(2, lambda a, b: send_a.at[b, a], recv_b.at[0])
    begin_b, end_b = exchange_all(3, lambda a, b: send_n.at[b, a], recv_b.at[1])

    p0 = first_sweep(0)
    for cycle in range(CYCLES):
        for k in range(SWEEPS):
            if cycle == 0 and k == 0:
                continue
            p0 = sweep(0, p0, record=cycle - 1 if cycle > 0 and k == 0 else None)

        def read0(z, r, p0=p0):
            return residual_chunk(v0, p0, z, r, n0, source, diag0, h[0])[1]

        def keep_g1(z, value):
            g1[z - 1] = value

        over_planes(v0, p0, 0, restrict0(read0, keep_g1))
        p1 = first_sweep(1)
        for k in range(1, SWEEPS):
            p1 = sweep(1, p1)

        def keep_res(z, p1=p1):
            for r in range(0, n1, CHUNK):
                res1[z - 1, pl.ds(r, CHUNK), :] = residual_chunk(
                    v1, p1, z, r, n1, g1, diag1, h[1]
                )[1]

        over_planes(v1, p1, 1, keep_res)
        for z in range(depth):
            restrict1(z, res1[z])
        begin_a()
        recv_b[0, b_me, a_me] = send_a[b_me, a_me]
        if cycle == 0:
            end_v()
            end_r()
            to_lines(recv_v, lines)
            to_lines(recv_a, target.at[0])
            coarse = target[0]
            for offset in range(LEVELS - SWITCH):
                if offset > 0:
                    coarse = dot(coarse, ups[2 * offset - 2])
                diag[offset] = 2.0 * lines[...] + 4.0 * h[SWITCH + offset] + coarse
            for offset in range(LEVELS - SWITCH):
                setup_lines(offset)
        end_a()
        to_lines(recv_b.at[0], target.at[0])
        rowbuf[...] = line_descend(0)
        for a in range(gz):
            for b in range(gy):
                s = (a * gy + b) * depth
                send_n[b, a] = rowbuf[s : s + depth, :]
        begin_b()
        recv_b[1, b_me, a_me] = send_n[b_me, a_me]
        end_b()
        for z in range(depth):
            wide = None
            for b in range(gy):
                for a in range(gz):
                    corr1[a : a + 1, :] = recv_b[1, b, a, z : z + 1, :]
                part = dot(dot(groupt[...], corr1[...]) * mask[...], colst[b])
                wide = part if wide is None else wide + part
            v1[1 - p1, z + 1] = v1[p1, z + 1] + dot(down1[...].T * 2.0, wide)
        p1 = 1 - p1
        for _ in range(SWEEPS):
            p1 = sweep(1, p1)

        def correct0(z, c, p0=p0, p1=p1):
            tmp0[...] = dot_left(downt0[...] * 2.0, v1[p1, z])
            for r in range(0, n0, CHUNK):
                v0[1 - p0, z, pl.ds(r, CHUNK), :] = v0[p0, z, pl.ds(r, CHUNK), :] + dot_right(
                    tmp0[pl.ds(r, CHUNK), :], down0[...] * 2.0
                )
            return c

        lax.fori_loop(1, depth + 1, correct0, 0)
        p0 = 1 - p0
        for _ in range(SWEEPS):
            p0 = sweep(0, p0)

    def last(z, p0=p0):
        for r in range(0, n0, CHUNK):
            centre, res = residual_chunk(v0, p0, z, r, n0, source, diag0, h[0])
            out[z - 1, pl.ds(r, CHUNK), :] = centre
            acc[CYCLES - 1, :, :] += (res * res).reshape(CHUNK // 8, 8, n0).sum(axis=0)

    over_planes(v0, p0, 0, last)
    ridx = lax.broadcasted_iota(jnp.int32, (8, 128), 0)
    part = jnp.zeros((8, 128), jnp.float32)
    for k in range(CYCLES):
        part = jnp.where(ridx == k, jnp.sum(acc[k]), part)
    rowbuf_n = tmp_n = send_n
    target_n = recv_n
    w_n = acc
    acc[0, :, 0:128] = part
    begin_n, end_n = exchange_all(4, lambda a, b: acc.at[0, :, pl.ds(0, 128)], recv_n)
    begin_n()
    recv_n[b_me, a_me] = part
    end_n()
    total = jnp.zeros((8, 128), jnp.float32)
    for a in range(gz):
        for b in range(gy):
            total = total + recv_n[b, a]
    norms[...] = total * (1.0 / (zall * n0 * n0))


def pair_matrix(n, value):
    return (np.arange(n)[None, :] // 2 == np.arange(n // 2)[:, None]).astype(np.float32) * value


def shards(gz, gy, source, vertical, reaction):
    depth, n0 = source.shape[0], source.shape[1]
    nd = gz * gy
    zall = nd * depth
    n1, n2 = n0 // 2, n0 // 4
    bx, by = n2 // gz, n2 // gy
    cells = bx * by
    cp = -(-cells // 128) * 128
    down0 = pair_matrix(n0, 0.5)
    down1 = pair_matrix(n1, 0.5)
    lane = np.arange(cp)
    cols = np.zeros((gy, n1, cp), np.float32)
    colst = np.zeros((gy, cp, n1), np.float32)
    for b in range(gy):
        hit = (np.arange(n1)[:, None] // 2 == b * by + lane[None, :] % by) & (lane[None, :] < cells)
        cols[b] = hit * 0.5
        colst[b] = hit.T
    mask = ((lane[None, :] // by == np.arange(n2)[:, None] % bx) & (lane[None, :] < cells)).astype(np.float32)
    group = (np.arange(n2)[None, :] // bx == np.arange(gz)[:, None]).astype(np.float32)
    ups = []
    for offset in range(LEVELS - SWITCH - 1):
        fx, fy = bx >> offset, by >> offset
        cy = fy // 2
        matrix = np.zeros((cp, cp), np.float32)
        for i in range(fx):
            for j in range(fy):
                matrix[i * fy + j, (i // 2) * cy + j // 2] = 1.0
        ups += [matrix * 0.25, matrix.T]
    ups = np.stack(ups)
    steps = (zall - 1).bit_length()
    f32 = jnp.float32
    nl = LEVELS - SWITCH
    vm = pl.BlockSpec(memory_space=pltpu.VMEM)
    consts = [down0, down0.T.copy(), down1, cols, mask, group, ups, group.T.copy(), colst]
    solution, norms = pl.pallas_call(
        functools.partial(kernel, (gz, gy, depth, cp)),
        out_shape=(
            jax.ShapeDtypeStruct(source.shape, f32),
            jax.ShapeDtypeStruct((8, 128), f32),
        ),
        in_specs=[vm, vm, pl.BlockSpec(memory_space=pltpu.SMEM), vm] + [vm] * len(consts),
        out_specs=(vm, vm),
        scratch_shapes=[
            pltpu.VMEM((2, depth + 2, n0, n0), f32),
            pltpu.VMEM((2, depth + 2, n1, n1), f32),
            pltpu.VMEM((depth, n0, n0), f32),
            pltpu.VMEM((depth, n1, n1), f32),
            pltpu.VMEM((depth, n1, n1), f32),
            pltpu.VMEM((depth, n1, n1), f32),
            pltpu.VMEM((depth, n1, n1), f32),
            pltpu.VMEM((n0, n1), f32),
            pltpu.VMEM((depth, n1, n1), f32),
            pltpu.VMEM((gz, cp), f32),
            pltpu.VMEM((gy, gz, depth, cp), f32),
            pltpu.VMEM((gy, gz, depth, cp), f32),
            pltpu.VMEM((gy, gz, depth, cp), f32),
            pltpu.VMEM((gy, gz, depth, cp), f32),
            pltpu.VMEM((2, gy, gz, depth, cp), f32),
            pltpu.VMEM((gy, gz, depth, cp), f32),
            pltpu.VMEM((gy, gz, 8, 128), f32),
            pltpu.VMEM((zall, cp), f32),
            pltpu.VMEM((nl, zall, cp), f32),
            pltpu.VMEM((nl, 2 * steps + 1, zall, cp), f32),
            pltpu.VMEM((nl, zall, cp), f32),
            pltpu.VMEM((2, zall, cp), f32),
            pltpu.VMEM((2, 4, zall, cp), f32),
            pltpu.VMEM((zall, cp), f32),
            pltpu.VMEM((CYCLES, 8, n0), f32),
            pltpu.SemaphoreType.DMA((2, 2, 2)),
            pltpu.SemaphoreType.DMA((2, 2, 2)),
            pltpu.SemaphoreType.DMA((2, 4)),
            pltpu.SemaphoreType.DMA((2, 4)),
            pltpu.SemaphoreType.DMA((5, nd)),
            pltpu.SemaphoreType.DMA((5, nd)),
        ],
        compiler_params=pltpu.CompilerParams(
            has_side_effects=True, vmem_limit_bytes=64000 * 1024
        ),
    )(
        source,
        reaction,
        vertical,
        jnp.broadcast_to(vertical[:, None], (depth, cp)),
        *[jnp.asarray(c) for c in consts],
    )
    return solution, norms[:CYCLES, 0]


CROWS = 32
GROUP = 2
VMEM_LIMIT = 64000 * 1024
PAD = 8


def dot_parts(x, m, parts=2):
    total = None
    rest = x
    for k in range(parts):
        piece = rest.astype(jnp.bfloat16)
        if k + 1 < parts:
            rest = rest - piece.astype(jnp.float32)
        term = jnp.dot(piece, m, preferred_element_type=jnp.float32)
        total = term if total is None else total + term
    return total


def chain_kernel(
    dims,
    source_in, reaction_in, vertical,
    out, norms,
    source, reaction, downy, upy, up2, down3, down4, up3, up4, load,
    v0, g0, w0, d0, v1, g1, w1, d1, raw_r, raw_s, stage, turn, lines, vsend, vrecv,
    gx, cx, ex, dx, win3, win4, v2, v3, v4, g3, g4, diag, fac, mask, acc, nsend, nrecv,
    a2a_send, a2a_recv, from_sem, x_send, x_recv, w3_send, w3_recv, w4_send, w4_recv,
):
    gz, gy, depth = dims
    nd = gz * gy
    zall = nd * depth
    n0 = source.shape[1]
    n1, n2, n3, n4 = n0 // 2, n0 // 4, n0 // 8, n0 // 16
    r0, r1 = n0 // nd, n0 // 2 // nd
    nt0 = n0 // 128
    h = [COUPLING / 4.0**k for k in range(LEVELS)]
    f32 = jnp.float32
    a_me, b_me = lax.axis_index("gz"), lax.axis_index("gy")
    me = a_me * gy + b_me
    nchip = gz // 2

    def div(x, n):
        return lax.div(x, jnp.int32(n))

    def rem(x, n):
        return lax.rem(x, jnp.int32(n))

    def bend(c):
        return c + div(c, 2) - 2 * div(c, 3) if nchip == 4 else c

    def place(i):
        k, core = div(i, 2), rem(i, 2)
        b, q = div(k, nchip), rem(k, nchip)
        q = q + rem(b, 2) * (nchip - 1 - 2 * q)
        return (bend(q) * 2 + core, b)

    q_me = bend(a_me // 2)
    q_me = q_me + (b_me % 2) * (nchip - 1 - 2 * q_me)
    p = (b_me * nchip + q_me) * 2 + a_me % 2
    chip, par = p // 2, p % 2

    def loop(lo, hi, body):
        def step(i, c):
            body(i)
            return c
        lax.fori_loop(lo, hi, step, 0)

    def remote(src, dst, ss, rs, to):
        return pltpu.make_async_remote_copy(
            src_ref=src, dst_ref=dst, send_sem=ss, recv_sem=rs, device_id=to, device_id_type=MESH
        )

    def target(k):
        return rem(p + nd + (div(k, 2) + rem(k, 2)) * (1 - 2 * rem(k, 2)), nd)

    def flat(i):
        a, b = place(i)
        return a * gy + b

    def spread(kind, src_of, dst_mine, whole, each=None):
        def start(k):
            t = target(k)
            sem = a2a_recv.at[kind] if each is None else from_sem.at[me]
            remote(src_of(t), dst_mine, a2a_send.at[kind], sem, place(t)).start()

        def wait_all(recv):
            copy = remote(whole, whole, a2a_send.at[kind], a2a_recv.at[kind], place(p))
            copy.wait_recv() if recv else copy.wait_send()

        def landed(s):
            if each is None:
                wait_all(True)
            else:
                r = each(s)
                remote(r, r, a2a_send.at[kind], from_sem.at[s], place(p)).wait_recv()

        return lambda lo=1, hi=nd: loop(lo, hi, start), lambda: wait_all(False), landed

    def piece(ref, t):
        return ref.at[:, pl.ds(r0 * t, r0), :]

    def zrows(ref, s):
        return ref.at[pl.ds(depth * s, depth)]

    zrest = pl.ds(0, depth * (nd - 1))
    rest = pl.ds(0, nd - 1)
    start_v, done_v, landed_v = spread(0, lambda t: vsend, vrecv.at[me], vrecv.at[rest])
    start_r, done_r, landed_r = spread(1, lambda t: piece(reaction, t), zrows(raw_r, me), raw_r.at[zrest])
    start_s, done_s, landed_s = spread(
        2, lambda t: piece(source, t), zrows(raw_s, me), raw_s.at[zrest], lambda s: zrows(raw_s, s))
    start_o, done_o, landed_o = spread(
        3, lambda t: zrows(stage, flat(t)), piece(out, p), stage.at[zrest], lambda s: zrows(stage, s))
    start_n, done_n, landed_n = spread(4, lambda t: nsend, nrecv.at[me], nrecv.at[rest])

    load_r = pltpu.make_async_copy(reaction_in, reaction, load.at[0])
    load_s = pltpu.make_async_copy(source_in, source, load.at[1])
    load_r.start()
    load_s.start()
    barrier = pltpu.get_barrier_semaphore()

    def greet(k):
        pl.semaphore_signal(barrier, inc=1, device_id=place(target(nd - k)), device_id_type=MESH)

    loop(1, nd, greet)
    for i in range(depth):
        vsend[i : i + 1, :] = jnp.full((1, 128), vertical[i], f32)
    pl.semaphore_wait(barrier, nd - 1)
    load_r.wait()
    start_r()
    start_v()
    load_s.wait()
    start_s()

    def fill(ref, at, value):
        shape = ref.shape[-2:]
        row = lax.broadcasted_iota(jnp.int32, shape, 0)
        col = lax.broadcasted_iota(jnp.int32, shape, 1)
        hit, scale = value(row, col)
        ref[at] = jnp.where(hit, scale, 0.0).astype(jnp.bfloat16)

    fill(downy, ..., lambda r, c: (r // 2 == c, 0.25))
    fill(upy, ..., lambda r, c: (r == c // 2, 1.0))
    for i in range(r1 // 2):
        fill(up2, i, lambda r, c: (r == n2 * i + c // 2, 1.0))
    fill(down3, ..., lambda r, c: (r % n2 // 2 == c % n3, 0.25))
    fill(down4, 0, lambda r, c: ((r >= 3 * n3) & ((r - 3 * n3) // 2 == c % n4), 0.25))
    fill(down4, 1, lambda r, c: ((r < n3) & (r // 2 == c % n4), 0.25))
    fill(up3, 0, lambda r, c: (r == 3 * n3 + c % n2 // 2, 1.0))
    fill(up3, 1, lambda r, c: (r == c % n2 // 2, 1.0))
    for t in range(2):
        fill(up4, t, lambda r, c: (r == n4 * (4 + (4 * t + c // n3 + 5) // 2 - 4) + c % n3 // 2, 1.0))

    first, last = p == 0, p == nd - 1

    def xchg(kind, lo_src, lo_dst, hi_src, hi_dst):
        def down():
            return remote(lo_src, hi_dst, x_send.at[kind, 0], x_recv.at[kind, 0], place((p + nd - 1) % nd))

        def up():
            return remote(hi_src, lo_dst, x_send.at[kind, 1], x_recv.at[kind, 1], place((p + 1) % nd))

        def begin(sides=(0, 1)):
            if 0 in sides:
                @pl.when(jnp.logical_not(first))
                def _():
                    down().start()

            if 1 in sides:
                @pl.when(jnp.logical_not(last))
                def _():
                    up().start()

        def end():
            @pl.when(jnp.logical_not(first))
            def _():
                down().wait_send()
                up().wait_recv()

            @pl.when(jnp.logical_not(last))
            def _():
                up().wait_send()
                down().wait_recv()

        return begin, end

    def planes0(m, dep):
        def at(lo):
            return v0.at[m, pl.ds(lo, dep), pl.ds(PAD, zall), :]
        return xchg(m, at(2), at(2 - dep), at(2 + r0 - dep), at(2 + r0))

    def row1(kind, far):
        return xchg(kind, g1.at[2 + far], g1.at[1 - far], g1.at[r1 + 1 - far], g1.at[r1 + 2 + far])

    def planes1(ref, kind):
        return xchg(kind, ref.at[pl.ds(2, 2)], ref.at[pl.ds(0, 2)],
                    ref.at[pl.ds(r1, 2)], ref.at[pl.ds(r1 + 2, 2)])

    def far0(m):
        def at(x):
            return v0.at[m, x, pl.ds(PAD, zall), :]
        return xchg(11, at(3), at(0), at(r0), at(r0 + 3))

    def norm0():
        def at(m, x):
            return v0.at[m, x, pl.ds(PAD, zall), :]
        return xchg(1, at(2, 2), at(1, 0), at(2, r0 + 1), at(1, r0 + 3))

    def rows1():
        def at(x):
            return v1.at[0, x, pl.ds(PAD, zall), :]
        return xchg(12, at(2), at(1), at(r1 + 1), at(r1 + 2))

    def far1():
        def at(x):
            return v1.at[1, x, pl.ds(PAD, zall), :]
        return xchg(13, at(3), at(0), at(r1), at(r1 + 3))

    def blocks(ref, kind):
        return xchg(kind, ref.at[1], ref.at[0], ref.at[1], ref.at[2])

    def halo_d0():
        return xchg(5, d0.at[1], d0.at[0], d0.at[r0], d0.at[r0 + 1])

    offs3 = [(o, c) for o in (0, -1, 1, -2, 2) for c in range(2)]

    def window3(kind):
        buf = win3.at[kind]

        def out_of(o, c):
            slot = par + 3 - 2 * o
            return remote(buf.at[3 + par], buf.at[slot], w3_send.at[4 + 2 * o + c], w3_recv.at[kind // CYCLES, slot],
                          place((2 * (chip + o) + c + nd) % nd))

        def goes(o, c):
            there = jnp.logical_and(chip + o >= 0, chip + o < nd // 2)
            if o == 0:
                return par != c
            if o == -2:
                return jnp.logical_and(there, par == 0)
            if o == 2:
                return jnp.logical_and(there, par == 1)
            return there

        def begin():
            for o, c in offs3:
                @pl.when(goes(o, c))
                def _(o=o, c=c):
                    out_of(o, c).start()

        def end():
            for o, c in offs3:
                @pl.when(goes(o, c))
                def _(o=o, c=c):
                    out_of(o, c).wait_send()
            for q in range(8):
                row = 2 * chip - 3 + q
                inside = jnp.logical_and(row >= 0, row < nd)
                if q in (3, 4):
                    inside = par != q - 3

                @pl.when(inside)
                def _(q=q):
                    remote(buf.at[q], buf.at[q], w3_send.at[0], w3_recv.at[kind // CYCLES, q], place(p)).wait_recv()

        return begin, end

    offs4 = [-1, 1, -2, 2, -3, 3, -4, 4]

    def window4(kind):
        buf = win4.at[kind]

        def each(fn):
            for o in offs4:
                @pl.when(jnp.logical_and(chip + o >= 0, chip + o < nd // 2))
                def _(o=o):
                    fn(o)

        def out_of(o):
            return remote(buf.at[4], buf.at[4 - o], w4_send.at[4 + o], w4_recv.at[kind // CYCLES, 4 - o],
                          place((p + 2 * o + nd) % nd))

        def begin():
            each(lambda o: out_of(o).start())

        def end():
            def fn(o):
                out_of(o).wait_send()
                remote(buf.at[4 + o], buf.at[4 + o], w4_send.at[4 + o], w4_recv.at[kind // CYCLES, 4 + o],
                       place(p)).wait_recv()
            each(fn)

        return begin, end

    zpad = jnp.zeros((PAD, n0), f32)
    for m in range(3):
        def zero0(x, m=m):
            v0[m, x, 0:PAD, :] = zpad
            v0[m, x, PAD + zall : 2 * PAD + zall, :] = zpad
        loop(0, r0 + 4, zero0)

        def zero1(x, m=m):
            v1[m, x, 0:PAD, :] = zpad[:, :n1]
            v1[m, x, PAD + zall : 2 * PAD + zall, :] = zpad[:, :n1]
        loop(0, r1 + 4, zero1)

    tile0 = jnp.zeros((zall, 128), f32)
    plane0 = jnp.zeros((zall, n0), f32)

    def blank(lo0, x0, lo1, b):
        for q in range(2):
            for m in range(3):
                v0[m, lo0 + q, PAD : PAD + zall, :] = plane0
            v1[1, lo1 + q, PAD : PAD + zall, :] = tile0
            g1[lo1 + q] = tile0
            d1[lo1 + q] = tile0
            w1[lo1 + q] = tile0
        d0[x0] = plane0
        w0[x0] = plane0
        for k in range(CYCLES):
            gx[k, b] = tile0
            cx[k, b] = tile0
            ex[k, b] = tile0
        dx[b] = tile0

    @pl.when(first)
    def _():
        blank(0, 0, 0, 0)

    @pl.when(last)
    def _():
        blank(r0 + 2, r0 + 1, r1 + 2, 2)

    for k in range(CYCLES + 1):
        for q in range(8):
            @pl.when(jnp.logical_or(2 * chip - 3 + q < 0, 2 * chip - 3 + q >= nd))
            def _(q=q, k=k):
                win3[k, q] = jnp.zeros((n3 * zall // 128, 128), f32)
        for o in offs4:
            @pl.when(jnp.logical_or(chip + o < 0, chip + o >= nd // 2))
            def _(o=o, k=k):
                win4[k, 4 + o] = jnp.zeros((n4 * zall // 128, 128), f32)
    for q in range(2):
        v3[q, 0] = tile0
        v3[q, 3] = tile0
        v4[q, 0] = tile0
        v4[q, 3] = tile0
    v4[1, 2] = tile0
    acc[...] = jnp.zeros_like(acc)

    lane = lax.broadcasted_iota(jnp.int32, (zall, 128), 1)
    rows = lax.broadcasted_iota(jnp.int32, (zall, 128), 0)

    for t in range(3):
        good = [p > 0, None, p < nd - 1][t]
        one = jnp.ones((zall, 128), f32)
        mask[t] = one if good is None else one * good.astype(f32)
    for t in range(2):
        row = 2 * chip - 3 + 4 * t + lane // n3
        mask[3 + t] = jnp.where((row >= 0) & (row < nd), 1.0, 0.0)
        row = chip - 4 + 8 * t + lane // n4
        mask[5 + t] = jnp.where((row >= 0) & (row < nd // 2) & (row < chip + 5), 1.0, 0.0)

    def pack(rep, width):
        k = 128 // width
        zb = zall // k
        part = lane[:zb]
        got = rep[0:zb]
        for j in range(1, k):
            got = jnp.where(part // width == j, rep[zb * j : zb * (j + 1)], got)
        return got

    def unpack(slots, width):
        k = 128 // width
        zb = zall // k
        part = lane[:zb] // width
        parts = []
        for j in range(k):
            got = jnp.zeros((zb, 128), f32)
            for s, x in enumerate(slots):
                turn = (width * (s - j)) % 128
                x = x if turn == 0 else pltpu.roll(x, turn, 1)
                got = jnp.where(part == s, x, got)
            parts.append(got)
        return parts

    def unpack3(kind, dest, add=None):
        for t in range(2):
            slots = [win3[kind, 4 * t + k] for k in range(4)]
            zb = zall // 4
            for j, x in enumerate(unpack(slots, n3)):
                if add is not None:
                    x = x + add(j * zb, zb)
                dest[t, j * zb : (j + 1) * zb] = x

    def unpack4(kind, dest, add=None):
        for t in range(2):
            slots = [win4[kind, r] for r in range(8 * t, min(8 * t + 8, 9))]
            zb = zall // 8
            for j, x in enumerate(unpack(slots, n4)):
                if add is not None:
                    x = x + add(j * zb, zb)
                dest[t, j * zb : (j + 1) * zb] = x

    rawr = raw_r.reshape(zall * r0, n0)
    raws = raw_s.reshape(zall * r0, n0)
    staged = stage.reshape(zall * r0, n0)

    def unfold(raw, j):
        at = pl.ds(pl.multiple_of(PAD * r0 * j, PAD * r0), PAD * r0)
        for t in range(nt0):
            turn[t, at, :] = raw[at, 128 * t : 128 * (t + 1)]
    raw_r[pl.ds(depth * me, depth)] = reaction[:, pl.ds(r0 * p, r0), :]
    raw_s[pl.ds(depth * me, depth)] = source[:, pl.ds(r0 * p, r0), :]
    vrecv[me] = vsend[...]
    group = PAD // depth

    def each_rows(landed, body):
        def step(i):
            j = (me // group + i) % (zall // PAD)
            for k in range(group if landed is not None else 0):
                s = group * j + k

                @pl.when(s != me)
                def _():
                    landed(s)
            body(j)
        loop(0, zall // PAD, step)

    landed_v(None)
    for s in range(nd):
        lines[depth * s : depth * (s + 1), :] = vrecv[s]

    def take_r(j):
        z = pl.multiple_of(PAD * j, PAD)
        unfold(rawr, j)
        for x in range(r0):
            for t in range(nt0):
                d0[x + 1, pl.ds(z, PAD), 128 * t : 128 * (t + 1)] = turn[
                    t, pl.ds(PAD * r0 * j + x, PAD, stride=r0), :]

    landed_r(None)
    each_rows(None, take_r)

    def shrink_r(i):
        for r in range(0, zall, CROWS):
            at = pl.ds(r, CROWS)
            a, b = d0[2 * i + 1, at, :], d0[2 * i + 2, at, :]
            got = dot_parts(a + b, downy[...], 3)
            vert = lines[at, :]
            base = 2.0 * vert + 4.0 * h[1]
            w1[i + 2, at, :] = got
            d = base + got
            d1[i + 2, at, :] = d
            base = jnp.concatenate([2.0 * vert + 4.0 * h[0]] * nt0, axis=1)
            for k, x in ((1, a), (2, b)):
                x = base + x
                d0[2 * i + k, at, :] = x
                w0[2 * i + k, at, :] = DAMPING / x

    loop(0, r1, shrink_r)
    begin_d0, end_d0 = halo_d0()
    begin_d0()
    begin_d1, end_d1 = planes1(d1, 6)
    begin_d1()
    rx2 = dot_parts(jnp.concatenate([w1[2] + w1[3], w1[4] + w1[5]], axis=1), downy[...], 3)
    dx[1] = rx2
    begin_dx, end_dx = blocks(dx, 7)
    begin_dx()
    rx3 = dot_parts(rx2, down3[...], 3)
    win3[CYCLES, 3 + par] = pack(rx3, n3)
    begin_w3, end_w3 = window3(CYCLES)
    begin_w3()
    begin_w4, end_w4 = window4(CYCLES)
    loop(2, r1 + 2, lambda x: w1.__setitem__(x, DAMPING / d1[x]))

    def take_s(j):
        z = pl.multiple_of(PAD * j, PAD)
        unfold(raws, j)
        for x in range(r0):
            for t in range(nt0):
                cut = slice(128 * t, 128 * (t + 1))
                got = turn[t, pl.ds(PAD * r0 * j + x, PAD, stride=r0), :]
                g0[x + 1, pl.ds(z, PAD), cut] = got
                v0[0, x + 2, pl.ds(z + PAD, PAD), cut] = w0[x + 1, pl.ds(z, PAD), cut] * got

    each_rows(landed_s, take_s)

    ns = (zall - 1).bit_length()

    def factors(f):
        vert = lines[...]
        a = jnp.where(rows == 0, 0.0, -vert)
        c = jnp.where(rows == zall - 1, 0.0, -vert)
        b = diag[f]
        for k in range(ns):
            s = 1 << k
            inv = 1.0 / b
            alpha = -a * pltpu.roll(inv, s, 0)
            gamma = -c * pltpu.roll(inv, zall - s, 0)
            b = b + alpha * pltpu.roll(c, s, 0) + gamma * pltpu.roll(a, zall - s, 0)
            a = alpha * pltpu.roll(a, s, 0)
            c = gamma * pltpu.roll(c, zall - s, 0)
            fac[f, 2 * k] = alpha
            fac[f, 2 * k + 1] = gamma
        fac[f, 2 * ns] = mask[f] / b

    def solve(f, right):
        for k in range(ns):
            s = 1 << k
            right = (
                right
                + fac[f, 2 * k] * pltpu.roll(right, s, 0)
                + fac[f, 2 * k + 1] * pltpu.roll(right, zall - s, 0)
            )
        return right * fac[f, 2 * ns]

    def near(v, q, b, width):
        t = v[q, b]
        below = pltpu.roll(jnp.where(lane >= 128 - width, v[q, b - 1], t), width, 1)
        above = pltpu.roll(jnp.where(lane < width, v[q, b + 1], t), 128 - width, 1)
        inrow = lane % width
        left = jnp.where(inrow == 0, 0.0, pltpu.roll(t, 1, 1))
        right = jnp.where(inrow == width - 1, 0.0, pltpu.roll(t, 127, 1))
        return (below + above) + (left + right)

    edge = lax.broadcasted_iota(jnp.int32, (CROWS, 128), 1)
    level0 = (v0, g0, w0, d0, nt0, h[0], 1)
    level1 = (v1, g1, w1, d1, 1, h[1], 2)

    def stencil(level, m, x, r):
        v, g, w, d, nt, weight, go = level
        centre, turn_r, turn_l = [], [], []
        for t in range(nt):
            cut = slice(128 * t, 128 * (t + 1))
            c = v[m, x + 2, PAD + r : PAD + r + CROWS, cut]
            centre.append(c)
            turn_r.append(pltpu.roll(c, 1, 1))
            turn_l.append(pltpu.roll(c, 127, 1))
        vert = lines[r : r + CROWS, :]
        got = []
        for t in range(nt):
            cut = slice(128 * t, 128 * (t + 1))
            left = jnp.where(edge == 0, turn_r[t - 1] if t else 0.0, turn_r[t])
            right = jnp.where(edge == 127, turn_l[t + 1] if t + 1 < nt else 0.0, turn_l[t])
            side = (v[m, x + 1, PAD + r : PAD + r + CROWS, cut] + v[m, x + 3, PAD + r : PAD + r + CROWS, cut]) + (left + right)
            if weight != 1.0:
                side = weight * side
            ends = v[m, x + 2, PAD + r - 1 : PAD + r - 1 + CROWS, cut] + v[m, x + 2, PAD + r + 1 : PAD + r + 1 + CROWS, cut]
            got.append(g[x + go, r : r + CROWS, cut] + side + vert * ends)
        return centre, got

    def sweep_plane(level, m, q, x, record=None, put=None):
        v, g, w, d, nt, weight, go = level
        for lo in range(0, zall, GROUP * CROWS):
            new = []
            for r in range(lo, lo + GROUP * CROWS, CROWS):
                centre, got = stencil(level, m, x, r)
                for t in range(nt):
                    cut = slice(128 * t, 128 * (t + 1))
                    wt = w[x + go, r : r + CROWS, cut]
                    if record is None:
                        value = (1.0 - DAMPING) * centre[t] + wt * got[t]
                    else:
                        res = got[t] - d[x + go, r : r + CROWS, cut] * centre[t]
                        value = centre[t] + wt * res
                        acc[record] += (res * res).reshape(CROWS // 8, 8, 128).sum(axis=0)
                    new.append((r, t, value))
            for r, t, value in new:
                v[q, x + 2, PAD + r : PAD + r + CROWS, 128 * t : 128 * (t + 1)] = value
                if put is not None:
                    for e in range(0, CROWS, 8):
                        put(x, r + e, t, value[e : e + 8])

    def residual(level, m, x, r):
        v, g, w, d, nt, weight, go = level
        centre, got = stencil(level, m, x, r)
        res = [
            got[t] - d[x + go, r : r + CROWS, 128 * t : 128 * (t + 1)] * centre[t] for t in range(nt)]
        return res

    def sweeps(level, m, q, xs, record=None, put=None):
        lo, hi, fn = xs
        loop(lo, hi, lambda i: sweep_plane(level, m, q, fn(i), record, put))

    def restrict0(m, lo, hi, fn):
        def body(i):
            i = fn(i)
            for r in range(0, zall, CROWS):
                a = residual(level0, m, 2 * i, r)
                b = residual(level0, m, 2 * i + 1, r)
                both = jnp.concatenate([s + t for s, t in zip(a, b)], axis=1)
                g1[i + 2, r : r + CROWS, :] = dot_parts(both, downy[...])
        loop(lo, hi, body)

    def same(i):
        return i

    def pair0(m, q, then, record=None, hook=None, put=None, restrict=False, fix=None):
        if fix is None:
            end = planes0(m, 2)[1]
        else:
            end = rows1()[1]
            far0(fix)[1]()
            correct0(fix, m, 0, r1, same)
        if hook is not None:
            hook[0]()
        sweeps(level0, m, 1, (1, r0 - 1, same), record)
        if restrict:
            restrict0(1, 1, r1 - 1, same)
            row1(3, 1)[0]()
        else:
            sweeps(level0, 1, q, (2, r0 - 2, same), None, put)
        end()
        if hook is not None:
            hook[1]()
        for side in range(2):
            if fix is not None:
                correct0(fix, m, 0, 1, lambda i: r1 if side else -1)
            sweep_plane(level0, m, 1, r0 if side else -1)
            sweep_plane(level0, m, 1, r0 - 1 if side else 0, record)
            if restrict:
                restrict0(1, 0, 1, lambda i: r1 - 1 if side else 0)
            else:
                for k in range(2):
                    sweep_plane(level0, 1, q, r0 - 2 + k if side else k, None, put)
            then((side,))

    def halo_factors():
        end_dx()
        for t in range(3):
            diag[t] = 2.0 * lines[...] + 4.0 * h[2] + dx[t]
        loop(0, 3, factors)
        for k in range(2 * ns + 1):
            fac[7, k] = jnp.where(lane >= n2, fac[0, k], fac[2, k])
        end_w3()
        unpack3(CYCLES, g3)
        win4[CYCLES, 4] = pack(
            dot_parts(g3[0], down4[0], 3) + dot_parts(g3[1], down4[1], 3), n4)
        begin_w4()

    def window_factors():
        def add(level):
            return lambda r, n: 2.0 * lines[r : r + n, :] + 4.0 * h[level]
        for t in range(2):
            diag[3 + t] = 2.0 * lines[...] + 4.0 * h[3] + g3[t]
        loop(3, 5, factors)
        end_w4()
        unpack4(CYCLES, diag.at[pl.ds(5, 2)], add(4))
        loop(5, 7, factors)

    def halo_level0():
        end_d0()
        for x, inside in ((0, jnp.logical_not(first)), (r0 + 1, jnp.logical_not(last))):
            @pl.when(inside)
            def _(x=x):
                w0[x] = DAMPING / d0[x]
            g0[x] = v0[0, x + 1, PAD : PAD + zall, :] * d0[x] * (1.0 / DAMPING)

    def halo_level1():
        end_d1()
        for x, inside in ((0, jnp.logical_not(first)), (r1 + 2, jnp.logical_not(last))):
            @pl.when(inside)
            def _(x=x):
                for q in range(2):
                    w1[x + q] = DAMPING / d1[x + q]

    def coarse(cycle, m):
        end = row1(10, 0)[1]
        far0(m)[0]()
        if cycle == 0:
            window_factors()
        loop(2, r1 + 2, lambda x: v1.__setitem__((0, x, pl.ds(PAD, zall)), w1[x] * g1[x]))
        row1(3, 1)[1]()
        end()
        if cycle == 0:
            halo_level1()
        for x in (0, 1, r1 + 2, r1 + 3):
            v1[0, x, PAD : PAD + zall] = w1[x] * g1[x]
        for x in range(-1, r1 + 1):
            sweep_plane(level1, 0, 1, x)

        pairs = []
        for i in range(r1 // 2):
            cuts = []
            for r in range(0, zall, CROWS):
                a = residual(level1, 1, 2 * i, r)[0]
                b = residual(level1, 1, 2 * i + 1, r)[0]
                cuts.append(a + b)
            pairs.append(jnp.concatenate(cuts, axis=0))
        gx[cycle, 1] = dot_parts(jnp.concatenate(pairs, axis=1), downy[...])
        e2 = lines2(cycle, far1()[0])
        ex[cycle, 1] = e2
        begin, end = blocks(ex.at[cycle], 4)
        begin()

        for i in range(r1 // 2):
            e = dot_parts(e2, up2[i])
            for x in (2 * i, 2 * i + 1):
                v1[2, x + 2, PAD : PAD + zall] = v1[1, x + 2, PAD : PAD + zall] + e
        far1()[1]()
        for x in range(1, r1 - 1):
            sweep_plane(level1, 2, 1, x)
        end()
        for side in range(2):
            e = dot_parts(ex[cycle, 2], up2[0]) if side else dot_parts(ex[cycle, 0], up2[r1 // 2 - 1])
            for x in (r1 + 2, r1 + 3) if side else (0, 1):
                v1[2, x, PAD : PAD + zall] = v1[1, x, PAD : PAD + zall] + e
            for x in (r1 - 1, r1) if side else (-1, 0):
                sweep_plane(level1, 2, 1, x)
            sweep_plane(level1, 1, 0, r1 - 1 if side else 0)
            rows1()[0]((side,))
        for x in range(1, r1 - 1):
            sweep_plane(level1, 1, 0, x)

    def lines_sweep(v, q, s, lo, hi, right, f, weight, width):
        for b in range(lo, hi):
            v[s, b] = solve(f + b - 1, right[b - 1] + weight * near(v, q, b, width))

    def line_residual(v, q, b, right, f, weight, width):
        values = v[q, b]
        before = jnp.where(rows == 0, 0.0, pltpu.roll(values, 1, 0))
        after = jnp.where(rows == zall - 1, 0.0, pltpu.roll(values, zall - 1, 0))
        return right[b - 1] + weight * near(v, q, b, width) + lines[...] * (before + after) - diag[f + b - 1] * values

    def beside(t):
        inrow = lane % n2
        return jnp.where(inrow == 0, 0.0, pltpu.roll(t, 1, 1)) + jnp.where(inrow == n2 - 1, 0.0, pltpu.roll(t, 127, 1))

    def pair2(left, own, right, right_own, right_rim):
        upper = lane >= n2
        rim = jnp.where(upper, left, right)
        far = jnp.where(upper, right, left)
        new = solve(1, right_own + h[2] * (beside(own) + pltpu.roll(own + rim, n2, 1)))
        return new, solve(7, right_rim + h[2] * (beside(rim) + pltpu.roll(own + far, n2, 1)))

    def lines2(cycle, after):
        right = gx.at[cycle]
        begin, end = blocks(right, 8)
        begin()
        after()
        v2[1] = solve(1, right[1])
        end()
        for b in (0, 2):
            v2[b] = solve(b, right[b])
        right_rim = jnp.where(lane >= n2, right[0], right[2])
        v2[3], v2[4] = pair2(v2[0], v2[1], v2[2], right[1], right_rim)
        own = v2[3]
        before = jnp.where(rows == 0, 0.0, pltpu.roll(own, 1, 0))
        after = jnp.where(rows == zall - 1, 0.0, pltpu.roll(own, zall - 1, 0))
        around = beside(own) + pltpu.roll(own + v2[4], n2, 1)
        res = right[1] + h[2] * around + lines[...] * (before + after) - diag[1] * own
        win3[cycle, 3 + par] = pack(dot_parts(res, down3[...]), n3)
        e3 = lines3(cycle)
        cx[cycle, 1] = v2[3] + dot_parts(e3, up3[par])
        begin, end = blocks(cx.at[cycle], 9)
        begin()
        end()
        v2[0], v2[1] = pair2(cx[cycle, 0], cx[cycle, 1], cx[cycle, 2], right[1], jnp.where(lane >= n2, right[0], right[2]))
        return solve(1, right[1] + h[2] * (beside(v2[0]) + pltpu.roll(v2[0] + v2[1], n2, 1)))

    def lines3(cycle):
        begin, end = window3(cycle)
        begin()
        end()
        unpack3(cycle, g3)
        loop(1, 3, lambda b: v3.__setitem__((0, b), solve(3 + b - 1, g3[b - 1])))
        lines_sweep(v3, 0, 1, 1, 3, g3, 3, h[3], n3)
        both = None
        for t in range(2):
            part = dot_parts(line_residual(v3, 1, t + 1, g3, 3, h[3], n3), down4[t])
            both = part if both is None else both + part
        win4[cycle, 4] = pack(both, n4)
        e4 = lines4(cycle)
        for t in range(2):
            v3[0, t + 1] = v3[1, t + 1] + dot_parts(e4, up4[t])
        lines_sweep(v3, 0, 1, 1, 3, g3, 3, h[3], n3)
        return solve(3 + par, g3[par] + h[3] * near(v3, 1, 1 + par, n3))

    def lines4(cycle):
        begin, end = window4(cycle)
        begin()
        end()
        unpack4(cycle, g4)
        loop(1, 3, lambda b: v4.__setitem__((0, b), solve(5 + b - 1, g4[b - 1])))
        q = 0
        for k in range(1, COARSE - 1):
            v4[1 - q, 1] = solve(5, g4[0] + h[4] * near(v4, q, 1, n4))
            q = 1 - q
        return solve(5, g4[0] + h[4] * near(v4, q, 1, n4))

    def correct0(m, q, lo, hi, fn):
        def body(i):
            i = fn(i)
            for r in range(0, zall, 2 * CROWS):
                cut = slice(PAD + r, PAD + r + 2 * CROWS)
                e = dot_parts(v1[0, i + 2, cut, :], upy[...])
                for x in (2 * i + 2, 2 * i + 3):
                    v0[q, x, cut, :] = v0[m, x, cut, :] + e
        loop(lo, hi, body)

    def put(x, z, t, value):
        turn[t, pl.ds(z * r0 + x, 8, stride=r0), :] = value

    def fold(j):
        at = pl.ds(pl.multiple_of(PAD * r0 * j, PAD * r0), PAD * r0)
        for t in range(nt0):
            staged[at, 128 * t : 128 * (t + 1)] = turn[t, at, :]

    planes0(0, 2)[0]()
    pair0(0, 1, row1(10, 0)[0], hook=(halo_factors, halo_level0), restrict=True)
    coarse(0, 1)
    pair0(2, 0, planes0(0, 2)[0], fix=1)
    pair0(0, 2, planes0(2, 1)[0], record=0)
    end = planes0(2, 1)[1]
    restrict0(2, 1, r1 - 1, same)
    row1(3, 1)[0]()
    end()
    for side in range(2):
        restrict0(2, 0, 1, lambda i: r1 - 1 if side else 0)
        row1(10, 0)[0]((side,))
    coarse(1, 2)
    pair0(0, 2, norm0()[0], put=put, fix=2)
    loop(0, zall // PAD, fold)
    end = norm0()[1]
    start_o(1, nd * 5 // 8)
    keep = pltpu.make_async_copy(zrows(stage, me), piece(out, p), load.at[2])
    keep.start()

    def last_norm(x):
        for r in range(0, zall, CROWS):
            for res in residual(level0, 2, x, r):
                acc[CYCLES - 1] += (res * res).reshape(CROWS // 8, 8, 128).sum(axis=0)

    loop(1, r0 - 1, last_norm)
    end()
    for x, y in ((1, 0), (r0 + 2, r0 + 3)):
        v0[2, x, PAD : PAD + zall, :] = v0[1, y, PAD : PAD + zall, :]
    loop(0, 2, lambda i: last_norm(i * (r0 - 1)))
    ridx = lax.broadcasted_iota(jnp.int32, (8, 128), 0)
    part = jnp.zeros((8, 128), f32)
    for k in range(CYCLES):
        part = jnp.where(ridx == k, jnp.sum(acc[k]), part)
    nsend[...] = part
    start_n()
    start_o(nd * 5 // 8, nd)
    total = part
    done_v()
    done_r()
    done_s()

    def finish(s):
        @pl.when(s != me)
        def _():
            landed_o(s)
    loop(0, nd, finish)
    landed_n(None)
    nrecv[me] = part
    total = jnp.sum(nrecv[...], axis=0)
    for k in range(CYCLES):
        norms[k] = total[k, 0] * (1.0 / (zall * n0 * n0))
    keep.wait()
    done_o()
    done_n()


def chain_shards(gz, gy, source, vertical, reaction):
    depth, n0 = source.shape[0], source.shape[1]
    nd = gz * gy
    zall = nd * depth
    n1, n2, n3, n4 = n0 // 2, n0 // 4, n0 // 8, n0 // 16
    r0, r1 = n0 // nd, n1 // nd
    f32 = jnp.float32
    bf16 = jnp.bfloat16

    sm = pl.BlockSpec(memory_space=pltpu.SMEM)
    ns = (zall - 1).bit_length()
    dma = pltpu.SemaphoreType.DMA
    solution, norms = pl.pallas_call(
        functools.partial(chain_kernel, (gz, gy, depth)),
        out_shape=(
            pltpu.VMEM(source.shape, f32),
            jax.ShapeDtypeStruct((CYCLES,), f32),
        ),
        in_specs=[pl.BlockSpec(memory_space=pltpu.HBM)] * 2 + [sm],
        out_specs=(pl.BlockSpec(memory_space=pltpu.VMEM), sm),
        scratch_shapes=[
            pltpu.VMEM(source.shape, f32),
            pltpu.VMEM(source.shape, f32),
            pltpu.VMEM((n0, n1), bf16),
            pltpu.VMEM((n1, n0), bf16),
            pltpu.VMEM((r1 // 2, 128, n1), bf16),
            pltpu.VMEM((128, 128), bf16),
            pltpu.VMEM((2, 128, 128), bf16),
            pltpu.VMEM((2, 128, 128), bf16),
            pltpu.VMEM((2, 128, 128), bf16),
            pltpu.SemaphoreType.DMA((3,)),
            pltpu.VMEM((3, r0 + 4, zall + 2 * PAD, n0), f32),
            pltpu.VMEM((r0 + 2, zall, n0), f32),
            pltpu.VMEM((r0 + 2, zall, n0), f32),
            pltpu.VMEM((r0 + 2, zall, n0), f32),
            pltpu.VMEM((3, r1 + 4, zall + 2 * PAD, n1), f32),
            pltpu.VMEM((r1 + 4, zall, n1), f32),
            pltpu.VMEM((r1 + 4, zall, n1), f32),
            pltpu.VMEM((r1 + 4, zall, n1), f32),
            pltpu.VMEM((zall, r0, n0), f32),
            pltpu.VMEM((zall, r0, n0), f32),
            pltpu.VMEM((zall, r0, n0), f32),
            pltpu.VMEM((n0 // 128, zall * r0, 128), f32),
            pltpu.VMEM((zall, 128), f32),
            pltpu.VMEM((depth, 128), f32),
            pltpu.VMEM((nd, depth, 128), f32),
            pltpu.VMEM((CYCLES, 3, zall, 128), f32),
            pltpu.VMEM((CYCLES, 3, zall, 128), f32),
            pltpu.VMEM((CYCLES, 3, zall, 128), f32),
            pltpu.VMEM((3, zall, 128), f32),
            pltpu.VMEM((CYCLES + 1, 8, n3 * zall // 128, 128), f32),
            pltpu.VMEM((CYCLES + 1, 9, n4 * zall // 128, 128), f32),
            pltpu.VMEM((5, zall, 128), f32),
            pltpu.VMEM((2, 4, zall, 128), f32),
            pltpu.VMEM((2, 4, zall, 128), f32),
            pltpu.VMEM((2, zall, 128), f32),
            pltpu.VMEM((2, zall, 128), f32),
            pltpu.VMEM((7, zall, 128), f32),
            pltpu.VMEM((8, 2 * ns + 1, zall, 128), f32),
            pltpu.VMEM((7, zall, 128), f32),
            pltpu.VMEM((CYCLES, 8, 128), f32),
            pltpu.VMEM((8, 128), f32),
            pltpu.VMEM((nd, 8, 128), f32),
            dma((5,)),
            dma((5,)),
            dma((nd,)),
            dma((14, 2)),
            dma((14, 2)),
            dma((10,)),
            dma((2, 8)),
            dma((9,)),
            dma((2, 9)),
        ],
        compiler_params=pltpu.CompilerParams(
            has_side_effects=True, vmem_limit_bytes=VMEM_LIMIT, collective_id=0
        ),
    )(source, reaction, vertical)
    return solution, norms


def shards_of(gz, gy, source, vertical, reaction):
    depth, n0 = source.shape[0], source.shape[1]
    nd = gz * gy
    fits = (
        gz % 2 == 0 and n0 % (8 * nd) == 0 and n0 // nd == 8 and n0 % 256 == 0 and n0 // 4 * 2 == 128
        and PAD % depth == 0 and nd * depth % 128 == 0 and (LEVELS, SWITCH, SWEEPS, COARSE, CYCLES) == (5, 2, 2, 4, 2)
    )
    return (chain_shards if fits else shards)(gz, gy, source, vertical, reaction)


def solution(mesh):
    return jax.shard_map(
        functools.partial(shards_of, mesh.shape["gz"], mesh.shape["gy"]),
        mesh=mesh,
        in_specs=(P(("gz", "gy"), None, None), P(("gz", "gy")), P(("gz", "gy"), None, None)),
        out_specs=(P(("gz", "gy"), None, None), P()),
        check_vma=False,
    )
```

```python
import functools

import jax
import jax.numpy as jnp
import numpy as np
from jax import lax
from jax.experimental import pallas as pl
from jax.experimental.pallas import tpu as pltpu
from jax.sharding import PartitionSpec as P

LEVELS = 5
SWITCH = 2
CYCLES = 2
SWEEPS = 2
COARSE = 4
DAMPING = 0.8
COUPLING = 1.0
CHUNK = 32
MESH = pl.DeviceIdType.MESH


def dot(a, b):
    return lax.dot_general(
        a,
        b,
        (((1,), (0,)), ((), ())),
        precision=lax.Precision.HIGHEST,
        preferred_element_type=jnp.float32,
    )


def parts_of(x):
    first = x.astype(jnp.bfloat16)
    rest = x - first.astype(jnp.float32)
    second = rest.astype(jnp.bfloat16)
    third = (rest - second.astype(jnp.float32)).astype(jnp.bfloat16)
    return (third, second, first)


def dot_right(x, m):
    m = m.astype(jnp.bfloat16)
    total = None
    for x in parts_of(x):
        term = jnp.dot(x, m, preferred_element_type=jnp.float32)
        total = term if total is None else total + term
    return total


def dot_left(m, x):
    m = m.astype(jnp.bfloat16)
    total = None
    for x in parts_of(x):
        term = jnp.dot(m, x, preferred_element_type=jnp.float32)
        total = term if total is None else total + term
    return total


def kernel(
    dims,
    source, reaction, vert_s, vert_b, down0, downt0, down1, cols, mask, group, ups, groupt, colst,
    out, norms,
    v0, v1, w0, d1, w1, g1, r1, tmp0, res1, corr1, send_a, recv_a, send_v, recv_v, recv_b,
    send_n, recv_n, lines, diag, factor, target, around, halo, rowbuf, acc,
    plane_send, plane_recv, line_send, line_recv, a2a_send, a2a_recv,
):
    gz, gy, depth, cp = dims
    nd = gz * gy
    zall = nd * depth
    n0 = source.shape[1]
    n1 = n0 // 2
    a_me = lax.axis_index("gz")
    b_me = lax.axis_index("gy")
    me = a_me * gy + b_me
    h = [COUPLING / 4.0**k for k in range(LEVELS)]

    @pl.when(me == 0)
    def _():
        for p in range(2):
            v0[p, 0] = jnp.zeros((n0, n0), jnp.float32)
            v1[p, 0] = jnp.zeros((n1, n1), jnp.float32)

    @pl.when(me == nd - 1)
    def _():
        for p in range(2):
            v0[p, depth + 1] = jnp.zeros((n0, n0), jnp.float32)
            v1[p, depth + 1] = jnp.zeros((n1, n1), jnp.float32)

    edges = [a_me == 0, a_me == gz - 1, b_me == 0, b_me == gy - 1]
    for k in range(4):
        @pl.when(edges[k])
        def _(k=k):
            for p in range(2):
                halo[p, k] = jnp.zeros((zall, cp), jnp.float32)

    def flat(d):
        return (d // gy, d % gy)

    def plane_copy(v, p, level, up):
        if up:
            src, dst, to = v.at[p, depth], v.at[p, 0], flat(me + 1)
        else:
            src, dst, to = v.at[p, 1], v.at[p, depth + 1], flat(me + nd - 1 - nd * ((me + nd - 1) // nd))
        if up:
            to = flat((me + 1) % nd)
        k = 0 if up else 1
        return pltpu.make_async_remote_copy(
            src_ref=src, dst_ref=dst,
            send_sem=plane_send.at[level, p, k], recv_sem=plane_recv.at[level, p, k],
            device_id=to, device_id_type=MESH,
        )

    def plane_start(v, p, level):
        @pl.when(me < nd - 1)
        def _():
            plane_copy(v, p, level, True).start()

        @pl.when(me > 0)
        def _():
            plane_copy(v, p, level, False).start()

    def plane_wait(v, p, level):
        @pl.when(me < nd - 1)
        def _():
            plane_copy(v, p, level, True).wait_send()
            plane_copy(v, p, level, False).wait_recv()

        @pl.when(me > 0)
        def _():
            plane_copy(v, p, level, False).wait_send()
            plane_copy(v, p, level, True).wait_recv()

    def residual_chunk(v, p, z, r, n, target_ref, diag_of, weight):
        centre = v[p, z, pl.ds(r, CHUNK), :]
        rows = lax.broadcasted_iota(jnp.int32, (CHUNK, n), 0)
        lanes = lax.broadcasted_iota(jnp.int32, (CHUNK, n), 1)
        if r == 0:
            above = jnp.where(rows == 0, 0.0, pltpu.roll(centre, 1, 0))
        else:
            above = v[p, z, pl.ds(r - 1, CHUNK), :]
        if r + CHUNK == n:
            below = jnp.where(rows == CHUNK - 1, 0.0, pltpu.roll(centre, CHUNK - 1, 0))
        else:
            below = v[p, z, pl.ds(r + 1, CHUNK), :]
        left = jnp.where(lanes == 0, 0.0, pltpu.roll(centre, 1, 1))
        right = jnp.where(lanes == n - 1, 0.0, pltpu.roll(centre, n - 1, 1))
        vert = vert_s[z - 1]
        applied = (
            diag_of(z - 1, r, vert) * centre
            - vert * (v[p, z - 1, pl.ds(r, CHUNK), :] + v[p, z + 1, pl.ds(r, CHUNK), :])
            - weight * (above + below + left + right)
        )
        return centre, target_ref[z - 1, pl.ds(r, CHUNK), :] - applied

    def diag0(z, r, vert):
        return 2.0 * vert + 4.0 * h[0] + reaction[z, pl.ds(r, CHUNK), :]

    def diag1(z, r, vert):
        return d1[z, pl.ds(r, CHUNK), :]

    def over_planes(v, p, level, body):
        plane_start(v, p, level)

        def inner(z, c):
            body(z)
            return c

        lax.fori_loop(2, depth, inner, 0)
        plane_wait(v, p, level)

        def outer(i, c):
            body(1 + i * (depth - 1))
            return c

        lax.fori_loop(0, 2, outer, 0)

    def level_parts(level):
        if level == 0:
            return v0, source, diag0, w0, n0
        return v1, g1, diag1, w1, n1

    def sweep(level, p, record=None):
        v, tgt, dg, w, n = level_parts(level)

        def body(z):
            for r in range(0, n, CHUNK):
                centre, res = residual_chunk(v, p, z, r, n, tgt, dg, h[level])
                v[1 - p, z, pl.ds(r, CHUNK), :] = centre + w[z - 1, pl.ds(r, CHUNK), :] * res
                if record is not None:
                    sq = (res * res).reshape(CHUNK // 8, 8, n).sum(axis=0)
                    acc[record, :, :] += sq

        over_planes(v, p, level, body)
        return 1 - p

    def first_sweep(level):
        v, tgt, dg, w, n = level_parts(level)

        def body(z, c):
            v[0, z + 1] = w[z] * tgt[z]
            return c

        lax.fori_loop(0, depth, body, 0)
        return 0

    def restrict0(read_chunk, store):
        def body(z):
            for r in range(0, n0, CHUNK):
                tmp0[pl.ds(r, CHUNK), :] = dot_right(read_chunk(z, r), downt0[...])
            store(z, dot_left(down0[...], tmp0[...]))
        return body

    def restrict1(z, plane):
        half = dot(down1[...], plane)
        for b in range(gy):
            spread = dot(half, cols[b]) * mask[...]
            packed = dot(group[...], spread)
            for a in range(gz):
                send_a[b, a, z : z + 1, :] = packed[a : a + 1, :]

    def exchange_all(kind, src_of, recv):
        def copy(k):
            dst = (me + k) % nd
            a, b = dst // gy, dst % gy
            return pltpu.make_async_remote_copy(
                src_ref=src_of(a, b), dst_ref=recv.at[b_me, a_me],
                send_sem=a2a_send.at[kind, k], recv_sem=a2a_recv.at[kind, me],
                device_id=(a, b), device_id_type=MESH,
            )

        def start(k, c):
            copy(k).start()
            return c

        def finish(k, c):
            copy(k).wait_send()
            src = (me + k) % nd
            a, b = src // gy, src % gy
            pltpu.make_async_remote_copy(
                src_ref=recv.at[b, a], dst_ref=recv.at[b, a],
                send_sem=a2a_send.at[kind, k], recv_sem=a2a_recv.at[kind, src],
                device_id=(a, b), device_id_type=MESH,
            ).wait_recv()
            return c

        def begin():
            lax.fori_loop(1, nd, start, 0)

        def end():
            lax.fori_loop(1, nd, finish, 0)

        return begin, end

    def to_lines(recv, dest):
        for a in range(gz):
            for b in range(gy):
                s = (a * gy + b) * depth
                dest[s : s + depth, :] = recv[b, a]

    bx2, by2 = (n1 // 2 // gz, n1 // 2 // gy)
    steps = []
    s = 1
    while s < zall:
        steps.append(s)
        s *= 2
    ns = len(steps)

    def setup_lines(offset):
        rows = lax.broadcasted_iota(jnp.int32, (zall, cp), 0)
        vert = lines[...]
        a = jnp.where(rows == 0, 0.0, -vert)
        c = jnp.where(rows == zall - 1, 0.0, -vert)
        b = diag[offset]
        for k, s in enumerate(steps):
            alpha = -a / pltpu.roll(b, s, 0)
            gamma = -c / pltpu.roll(b, zall - s, 0)
            b = b + alpha * pltpu.roll(c, s, 0) + gamma * pltpu.roll(a, zall - s, 0)
            a = alpha * pltpu.roll(a, s, 0)
            c = gamma * pltpu.roll(c, zall - s, 0)
            factor[offset, 2 * k] = alpha
            factor[offset, 2 * k + 1] = gamma
        factor[offset, 2 * ns] = 1.0 / b

    def solve(offset, right):
        for k, s in enumerate(steps):
            right = (
                right
                + factor[offset, 2 * k] * pltpu.roll(right, s, 0)
                + factor[offset, 2 * k + 1] * pltpu.roll(right, zall - s, 0)
            )
        return right * factor[offset, 2 * ns]

    count = [0]
    def line_copy(p, k):
        if k == 0:
            to, slot = ((a_me + gz - 1) % gz, b_me), 1
        elif k == 1:
            to, slot = ((a_me + 1) % gz, b_me), 0
        elif k == 2:
            to, slot = (a_me, (b_me + gy - 1) % gy), 3
        else:
            to, slot = (a_me, (b_me + 1) % gy), 2
        return pltpu.make_async_remote_copy(
            src_ref=around.at[p], dst_ref=halo.at[p, slot],
            send_sem=line_send.at[p, k], recv_sem=line_recv.at[p, slot],
            device_id=to, device_id_type=MESH,
        )

    def line_landed(p, k):
        return pltpu.make_async_remote_copy(
            src_ref=around.at[p], dst_ref=halo.at[p, k],
            send_sem=line_send.at[p, k], recv_sem=line_recv.at[p, k],
            device_id=(a_me, b_me), device_id_type=MESH,
        )

    def neighbours(offset, values):
        bx, by = bx2 >> offset, by2 >> offset
        cells = bx * by
        p = count[0] % 2
        count[0] += 1
        around[p] = values
        for k in range(4):
            @pl.when(jnp.logical_not(edges[k]))
            def _(k=k):
                line_copy(p, k).start()
        for k in range(4):
            @pl.when(jnp.logical_not(edges[k]))
            def _(k=k):
                line_copy(p, k).wait_send()
                line_landed(p, k).wait_recv()
        lane = lax.broadcasted_iota(jnp.int32, (zall, cp), 1)

        def roll(x, amount):
            amount = amount % cp
            return x if amount == 0 else pltpu.roll(x, amount, 1)

        total = jnp.where(lane < by, roll(halo[p, 0], by - cells), roll(values, by))
        total += jnp.where(lane >= cells - by, roll(halo[p, 1], cells - by), roll(values, -by))
        inrow = lane & (by - 1)
        total += jnp.where(inrow == 0, roll(halo[p, 2], 1 - by), roll(values, 1))
        total += jnp.where(inrow == by - 1, roll(halo[p, 3], by - 1), roll(values, -1))
        return total

    def line_descend(offset):
        weight = h[SWITCH + offset]
        values = solve(offset, target[offset])
        repeats = COARSE if offset == LEVELS - 1 - SWITCH else SWEEPS
        for _ in range(1, repeats):
            values = solve(offset, target[offset] + weight * neighbours(offset, values))
        if offset == LEVELS - 1 - SWITCH:
            return values
        near = neighbours(offset, values)
        rows = lax.broadcasted_iota(jnp.int32, (zall, cp), 0)
        before = jnp.where(rows == 0, 0.0, pltpu.roll(values, 1, 0))
        after = jnp.where(rows == zall - 1, 0.0, pltpu.roll(values, zall - 1, 0))
        res = target[offset] - (
            diag[offset] * values - lines[...] * (before + after) - weight * near
        )
        target[offset + 1] = dot(res, ups[2 * offset])
        tmp = values
        lower = line_descend(offset + 1)
        values = tmp + dot(lower, ups[2 * offset + 1])
        for _ in range(SWEEPS):
            values = solve(offset, target[offset] + weight * neighbours(offset, values))
        return values

    def fill0(z, c):
        w0[z] = DAMPING / (2.0 * vert_s[z] + 4.0 * h[0] + reaction[z])
        return c

    lax.fori_loop(0, depth, fill0, 0)

    def keep_r1(z, value):
        r1[z] = value
        dv = 2.0 * vert_s[z] + 4.0 * h[1] + value
        d1[z] = dv
        w1[z] = DAMPING / dv

    body = restrict0(lambda z, r: reaction[z, pl.ds(r, CHUNK), :], keep_r1)
    lax.fori_loop(0, depth, lambda z, c: (body(z), c)[1], 0)
    for z in range(depth):
        restrict1(z, r1[z])
    send_v[...] = send_a[...]
    begin_v, end_v = exchange_all(0, lambda a, b: vert_b, recv_v)
    begin_r, end_r = exchange_all(1, lambda a, b: send_v.at[b, a], recv_a)
    begin_v()
    begin_r()
    recv_v[b_me, a_me] = vert_b[...]
    recv_a[b_me, a_me] = send_v[b_me, a_me]
    acc[...] = jnp.zeros_like(acc)

    begin_a, end_a = exchange_all(2, lambda a, b: send_a.at[b, a], recv_b.at[0])
    begin_b, end_b = exchange_all(3, lambda a, b: send_n.at[b, a], recv_b.at[1])

    p0 = first_sweep(0)
    for cycle in range(CYCLES):
        for k in range(SWEEPS):
            if cycle == 0 and k == 0:
                continue
            p0 = sweep(0, p0, record=cycle - 1 if cycle > 0 and k == 0 else None)

        def read0(z, r, p0=p0):
            return residual_chunk(v0, p0, z, r, n0, source, diag0, h[0])[1]

        def keep_g1(z, value):
            g1[z - 1] = value

        over_planes(v0, p0, 0, restrict0(read0, keep_g1))
        p1 = first_sweep(1)
        for k in range(1, SWEEPS):
            p1 = sweep(1, p1)

        def keep_res(z, p1=p1):
            for r in range(0, n1, CHUNK):
                res1[z - 1, pl.ds(r, CHUNK), :] = residual_chunk(
                    v1, p1, z, r, n1, g1, diag1, h[1]
                )[1]

        over_planes(v1, p1, 1, keep_res)
        for z in range(depth):
            restrict1(z, res1[z])
        begin_a()
        recv_b[0, b_me, a_me] = send_a[b_me, a_me]
        if cycle == 0:
            end_v()
            end_r()
            to_lines(recv_v, lines)
            to_lines(recv_a, target.at[0])
            coarse = target[0]
            for offset in range(LEVELS - SWITCH):
                if offset > 0:
                    coarse = dot(coarse, ups[2 * offset - 2])
                diag[offset] = 2.0 * lines[...] + 4.0 * h[SWITCH + offset] + coarse
            for offset in range(LEVELS - SWITCH):
                setup_lines(offset)
        end_a()
        to_lines(recv_b.at[0], target.at[0])
        rowbuf[...] = line_descend(0)
        for a in range(gz):
            for b in range(gy):
                s = (a * gy + b) * depth
                send_n[b, a] = rowbuf[s : s + depth, :]
        begin_b()
        recv_b[1, b_me, a_me] = send_n[b_me, a_me]
        end_b()
        for z in range(depth):
            wide = None
            for b in range(gy):
                for a in range(gz):
                    corr1[a : a + 1, :] = recv_b[1, b, a, z : z + 1, :]
                part = dot(dot(groupt[...], corr1[...]) * mask[...], colst[b])
                wide = part if wide is None else wide + part
            v1[1 - p1, z + 1] = v1[p1, z + 1] + dot(down1[...].T * 2.0, wide)
        p1 = 1 - p1
        for _ in range(SWEEPS):
            p1 = sweep(1, p1)

        def correct0(z, c, p0=p0, p1=p1):
            tmp0[...] = dot_left(downt0[...] * 2.0, v1[p1, z])
            for r in range(0, n0, CHUNK):
                v0[1 - p0, z, pl.ds(r, CHUNK), :] = v0[p0, z, pl.ds(r, CHUNK), :] + dot_right(
                    tmp0[pl.ds(r, CHUNK), :], down0[...] * 2.0
                )
            return c

        lax.fori_loop(1, depth + 1, correct0, 0)
        p0 = 1 - p0
        for _ in range(SWEEPS):
            p0 = sweep(0, p0)

    def last(z, p0=p0):
        for r in range(0, n0, CHUNK):
            centre, res = residual_chunk(v0, p0, z, r, n0, source, diag0, h[0])
            out[z - 1, pl.ds(r, CHUNK), :] = centre
            acc[CYCLES - 1, :, :] += (res * res).reshape(CHUNK // 8, 8, n0).sum(axis=0)

    over_planes(v0, p0, 0, last)
    ridx = lax.broadcasted_iota(jnp.int32, (8, 128), 0)
    part = jnp.zeros((8, 128), jnp.float32)
    for k in range(CYCLES):
        part = jnp.where(ridx == k, jnp.sum(acc[k]), part)
    rowbuf_n = tmp_n = send_n
    target_n = recv_n
    w_n = acc
    acc[0, :, 0:128] = part
    begin_n, end_n = exchange_all(4, lambda a, b: acc.at[0, :, pl.ds(0, 128)], recv_n)
    begin_n()
    recv_n[b_me, a_me] = part
    end_n()
    total = jnp.zeros((8, 128), jnp.float32)
    for a in range(gz):
        for b in range(gy):
            total = total + recv_n[b, a]
    norms[...] = total * (1.0 / (zall * n0 * n0))


def pair_matrix(n, value):
    return (np.arange(n)[None, :] // 2 == np.arange(n // 2)[:, None]).astype(np.float32) * value


def shards(gz, gy, source, vertical, reaction):
    depth, n0 = source.shape[0], source.shape[1]
    nd = gz * gy
    zall = nd * depth
    n1, n2 = n0 // 2, n0 // 4
    bx, by = n2 // gz, n2 // gy
    cells = bx * by
    cp = -(-cells // 128) * 128
    down0 = pair_matrix(n0, 0.5)
    down1 = pair_matrix(n1, 0.5)
    lane = np.arange(cp)
    cols = np.zeros((gy, n1, cp), np.float32)
    colst = np.zeros((gy, cp, n1), np.float32)
    for b in range(gy):
        hit = (np.arange(n1)[:, None] // 2 == b * by + lane[None, :] % by) & (lane[None, :] < cells)
        cols[b] = hit * 0.5
        colst[b] = hit.T
    mask = ((lane[None, :] // by == np.arange(n2)[:, None] % bx) & (lane[None, :] < cells)).astype(np.float32)
    group = (np.arange(n2)[None, :] // bx == np.arange(gz)[:, None]).astype(np.float32)
    ups = []
    for offset in range(LEVELS - SWITCH - 1):
        fx, fy = bx >> offset, by >> offset
        cy = fy // 2
        matrix = np.zeros((cp, cp), np.float32)
        for i in range(fx):
            for j in range(fy):
                matrix[i * fy + j, (i // 2) * cy + j // 2] = 1.0
        ups += [matrix * 0.25, matrix.T]
    ups = np.stack(ups)
    steps = (zall - 1).bit_length()
    f32 = jnp.float32
    nl = LEVELS - SWITCH
    vm = pl.BlockSpec(memory_space=pltpu.VMEM)
    consts = [down0, down0.T.copy(), down1, cols, mask, group, ups, group.T.copy(), colst]
    solution, norms = pl.pallas_call(
        functools.partial(kernel, (gz, gy, depth, cp)),
        out_shape=(
            jax.ShapeDtypeStruct(source.shape, f32),
            jax.ShapeDtypeStruct((8, 128), f32),
        ),
        in_specs=[vm, vm, pl.BlockSpec(memory_space=pltpu.SMEM), vm] + [vm] * len(consts),
        out_specs=(vm, vm),
        scratch_shapes=[
            pltpu.VMEM((2, depth + 2, n0, n0), f32),
            pltpu.VMEM((2, depth + 2, n1, n1), f32),
            pltpu.VMEM((depth, n0, n0), f32),
            pltpu.VMEM((depth, n1, n1), f32),
            pltpu.VMEM((depth, n1, n1), f32),
            pltpu.VMEM((depth, n1, n1), f32),
            pltpu.VMEM((depth, n1, n1), f32),
            pltpu.VMEM((n0, n1), f32),
            pltpu.VMEM((depth, n1, n1), f32),
            pltpu.VMEM((gz, cp), f32),
            pltpu.VMEM((gy, gz, depth, cp), f32),
            pltpu.VMEM((gy, gz, depth, cp), f32),
            pltpu.VMEM((gy, gz, depth, cp), f32),
            pltpu.VMEM((gy, gz, depth, cp), f32),
            pltpu.VMEM((2, gy, gz, depth, cp), f32),
            pltpu.VMEM((gy, gz, depth, cp), f32),
            pltpu.VMEM((gy, gz, 8, 128), f32),
            pltpu.VMEM((zall, cp), f32),
            pltpu.VMEM((nl, zall, cp), f32),
            pltpu.VMEM((nl, 2 * steps + 1, zall, cp), f32),
            pltpu.VMEM((nl, zall, cp), f32),
            pltpu.VMEM((2, zall, cp), f32),
            pltpu.VMEM((2, 4, zall, cp), f32),
            pltpu.VMEM((zall, cp), f32),
            pltpu.VMEM((CYCLES, 8, n0), f32),
            pltpu.SemaphoreType.DMA((2, 2, 2)),
            pltpu.SemaphoreType.DMA((2, 2, 2)),
            pltpu.SemaphoreType.DMA((2, 4)),
            pltpu.SemaphoreType.DMA((2, 4)),
            pltpu.SemaphoreType.DMA((5, nd)),
            pltpu.SemaphoreType.DMA((5, nd)),
        ],
        compiler_params=pltpu.CompilerParams(
            has_side_effects=True, vmem_limit_bytes=64000 * 1024
        ),
    )(
        source,
        reaction,
        vertical,
        jnp.broadcast_to(vertical[:, None], (depth, cp)),
        *[jnp.asarray(c) for c in consts],
    )
    return solution, norms[:CYCLES, 0]


CROWS = 32
GROUP = 2
VMEM_LIMIT = 64000 * 1024
PAD = 8


def dot_parts(x, m, parts=2):
    total = None
    rest = x
    for k in range(parts):
        piece = rest.astype(jnp.bfloat16)
        if k + 1 < parts:
            rest = rest - piece.astype(jnp.float32)
        term = jnp.dot(piece, m, preferred_element_type=jnp.float32)
        total = term if total is None else total + term
    return total


def chain_kernel(
    dims,
    source_in, reaction_in, vertical,
    out, norms,
    source, reaction, downy, upy, up2, down3, down4, up3, up4, load,
    v0, g0, w0, d0, v1, g1, w1, d1, raw_r, raw_s, stage, turn, lines, vsend, vrecv,
    gx, cx, ex, dx, win3, win4, v2, v3, v4, g3, g4, diag, fac, mask, acc, nsend, nrecv,
    a2a_send, a2a_recv, from_sem, x_send, x_recv, w3_send, w3_recv, w4_send, w4_recv,
):
    gz, gy, depth = dims
    nd = gz * gy
    zall = nd * depth
    n0 = source.shape[1]
    n1, n2, n3, n4 = n0 // 2, n0 // 4, n0 // 8, n0 // 16
    r0, r1 = n0 // nd, n0 // 2 // nd
    nt0 = n0 // 128
    h = [COUPLING / 4.0**k for k in range(LEVELS)]
    f32 = jnp.float32
    a_me, b_me = lax.axis_index("gz"), lax.axis_index("gy")
    me = a_me * gy + b_me
    nchip = gz // 2

    def div(x, n):
        return lax.div(x, jnp.int32(n))

    def rem(x, n):
        return lax.rem(x, jnp.int32(n))

    def bend(c):
        return c + div(c, 2) - 2 * div(c, 3) if nchip == 4 else c

    def place(i):
        k, core = div(i, 2), rem(i, 2)
        b, q = div(k, nchip), rem(k, nchip)
        q = q + rem(b, 2) * (nchip - 1 - 2 * q)
        return (bend(q) * 2 + core, b)

    q_me = bend(a_me // 2)
    q_me = q_me + (b_me % 2) * (nchip - 1 - 2 * q_me)
    p = (b_me * nchip + q_me) * 2 + a_me % 2
    chip, par = p // 2, p % 2

    def loop(lo, hi, body):
        def step(i, c):
            body(i)
            return c
        lax.fori_loop(lo, hi, step, 0)

    def remote(src, dst, ss, rs, to):
        return pltpu.make_async_remote_copy(
            src_ref=src, dst_ref=dst, send_sem=ss, recv_sem=rs, device_id=to, device_id_type=MESH
        )

    def target(k):
        return rem(p + nd + (div(k, 2) + rem(k, 2)) * (1 - 2 * rem(k, 2)), nd)

    def flat(i):
        a, b = place(i)
        return a * gy + b

    def spread(kind, src_of, dst_mine, whole, each=None):
        def start(k):
            t = target(k)
            sem = a2a_recv.at[kind] if each is None else from_sem.at[me]
            remote(src_of(t), dst_mine, a2a_send.at[kind], sem, place(t)).start()

        def wait_all(recv):
            copy = remote(whole, whole, a2a_send.at[kind], a2a_recv.at[kind], place(p))
            copy.wait_recv() if recv else copy.wait_send()

        def landed(s):
            if each is None:
                wait_all(True)
            else:
                r = each(s)
                remote(r, r, a2a_send.at[kind], from_sem.at[s], place(p)).wait_recv()

        return lambda lo=1, hi=nd: loop(lo, hi, start), lambda: wait_all(False), landed

    def piece(ref, t):
        return ref.at[:, pl.ds(r0 * t, r0), :]

    def zrows(ref, s):
        return ref.at[pl.ds(depth * s, depth)]

    zrest = pl.ds(0, depth * (nd - 1))
    rest = pl.ds(0, nd - 1)
    start_v, done_v, landed_v = spread(0, lambda t: vsend, vrecv.at[me], vrecv.at[rest])
    start_r, done_r, landed_r = spread(1, lambda t: piece(reaction, t), zrows(raw_r, me), raw_r.at[zrest])
    start_s, done_s, landed_s = spread(
        2, lambda t: piece(source, t), zrows(raw_s, me), raw_s.at[zrest], lambda s: zrows(raw_s, s))
    start_o, done_o, landed_o = spread(
        3, lambda t: zrows(stage, flat(t)), piece(out, p), stage.at[zrest], lambda s: zrows(stage, s))
    start_n, done_n, landed_n = spread(4, lambda t: nsend, nrecv.at[me], nrecv.at[rest])

    load_r = pltpu.make_async_copy(reaction_in, reaction, load.at[0])
    load_s = pltpu.make_async_copy(source_in, source, load.at[1])
    load_r.start()
    load_s.start()
    barrier = pltpu.get_barrier_semaphore()

    def greet(k):
        pl.semaphore_signal(barrier, inc=1, device_id=place(target(nd - k)), device_id_type=MESH)

    loop(1, nd, greet)
    for i in range(depth):
        vsend[i : i + 1, :] = jnp.full((1, 128), vertical[i], f32)
    pl.semaphore_wait(barrier, nd - 1)
    load_r.wait()
    start_r()
    start_v()
    load_s.wait()
    start_s()

    def fill(ref, at, value):
        shape = ref.shape[-2:]
        row = lax.broadcasted_iota(jnp.int32, shape, 0)
        col = lax.broadcasted_iota(jnp.int32, shape, 1)
        hit, scale = value(row, col)
        ref[at] = jnp.where(hit, scale, 0.0).astype(jnp.bfloat16)

    fill(downy, ..., lambda r, c: (r // 2 == c, 0.25))
    fill(upy, ..., lambda r, c: (r == c // 2, 1.0))
    for i in range(r1 // 2):
        fill(up2, i, lambda r, c: (r == n2 * i + c // 2, 1.0))
    fill(down3, ..., lambda r, c: (r % n2 // 2 == c % n3, 0.25))
    fill(down4, 0, lambda r, c: ((r >= 3 * n3) & ((r - 3 * n3) // 2 == c % n4), 0.25))
    fill(down4, 1, lambda r, c: ((r < n3) & (r // 2 == c % n4), 0.25))
    fill(up3, 0, lambda r, c: (r == 3 * n3 + c % n2 // 2, 1.0))
    fill(up3, 1, lambda r, c: (r == c % n2 // 2, 1.0))
    for t in range(2):
        fill(up4, t, lambda r, c: (r == n4 * (4 + (4 * t + c // n3 + 5) // 2 - 4) + c % n3 // 2, 1.0))

    first, last = p == 0, p == nd - 1

    def xchg(kind, lo_src, lo_dst, hi_src, hi_dst):
        def down():
            return remote(lo_src, hi_dst, x_send.at[kind, 0], x_recv.at[kind, 0], place((p + nd - 1) % nd))

        def up():
            return remote(hi_src, lo_dst, x_send.at[kind, 1], x_recv.at[kind, 1], place((p + 1) % nd))

        def begin(sides=(0, 1)):
            if 0 in sides:
                @pl.when(jnp.logical_not(first))
                def _():
                    down().start()

            if 1 in sides:
                @pl.when(jnp.logical_not(last))
                def _():
                    up().start()

        def end():
            @pl.when(jnp.logical_not(first))
            def _():
                down().wait_send()
                up().wait_recv()

            @pl.when(jnp.logical_not(last))
            def _():
                up().wait_send()
                down().wait_recv()

        return begin, end

    def planes0(m, dep):
        def at(lo):
            return v0.at[m, pl.ds(lo, dep), pl.ds(PAD, zall), :]
        return xchg(m, at(2), at(2 - dep), at(2 + r0 - dep), at(2 + r0))

    def row1(kind, far):
        return xchg(kind, g1.at[2 + far], g1.at[1 - far], g1.at[r1 + 1 - far], g1.at[r1 + 2 + far])

    def planes1(ref, kind):
        return xchg(kind, ref.at[pl.ds(2, 2)], ref.at[pl.ds(0, 2)],
                    ref.at[pl.ds(r1, 2)], ref.at[pl.ds(r1 + 2, 2)])

    def far0(m):
        def at(x):
            return v0.at[m, x, pl.ds(PAD, zall), :]
        return xchg(11, at(3), at(0), at(r0), at(r0 + 3))

    def norm0():
        def at(m, x):
            return v0.at[m, x, pl.ds(PAD, zall), :]
        return xchg(1, at(2, 2), at(1, 0), at(2, r0 + 1), at(1, r0 + 3))

    def rows1():
        def at(x):
            return v1.at[0, x, pl.ds(PAD, zall), :]
        return xchg(12, at(2), at(1), at(r1 + 1), at(r1 + 2))

    def far1():
        def at(x):
            return v1.at[1, x, pl.ds(PAD, zall), :]
        return xchg(13, at(3), at(0), at(r1), at(r1 + 3))

    def blocks(ref, kind):
        return xchg(kind, ref.at[1], ref.at[0], ref.at[1], ref.at[2])

    def halo_d0():
        return xchg(5, d0.at[1], d0.at[0], d0.at[r0], d0.at[r0 + 1])

    offs3 = [(o, c) for o in (-2, 2, -1, 1, 0) for c in range(2)]

    def window3(kind):
        buf = win3.at[kind]

        def out_of(o, c):
            slot = par + 3 - 2 * o
            return remote(buf.at[3 + par], buf.at[slot], w3_send.at[4 + 2 * o + c], w3_recv.at[kind // CYCLES, slot],
                          place((2 * (chip + o) + c + nd) % nd))

        def goes(o, c):
            there = jnp.logical_and(chip + o >= 0, chip + o < nd // 2)
            if o == 0:
                return par != c
            if o == -2:
                return jnp.logical_and(there, par == 0)
            if o == 2:
                return jnp.logical_and(there, par == 1)
            return there

        def begin():
            for o, c in offs3:
                @pl.when(goes(o, c))
                def _(o=o, c=c):
                    out_of(o, c).start()

        def end():
            for o, c in offs3:
                @pl.when(goes(o, c))
                def _(o=o, c=c):
                    out_of(o, c).wait_send()
            for q in range(8):
                row = 2 * chip - 3 + q
                inside = jnp.logical_and(row >= 0, row < nd)
                if q in (3, 4):
                    inside = par != q - 3

                @pl.when(inside)
                def _(q=q):
                    remote(buf.at[q], buf.at[q], w3_send.at[0], w3_recv.at[kind // CYCLES, q], place(p)).wait_recv()

        return begin, end

    offs4 = [-4, 4, -3, 3, -2, 2, -1, 1]

    def window4(kind):
        buf = win4.at[kind]

        def each(fn):
            for o in offs4:
                @pl.when(jnp.logical_and(chip + o >= 0, chip + o < nd // 2))
                def _(o=o):
                    fn(o)

        def out_of(o):
            return remote(buf.at[4], buf.at[4 - o], w4_send.at[4 + o], w4_recv.at[kind // CYCLES, 4 - o],
                          place((p + 2 * o + nd) % nd))

        def begin():
            each(lambda o: out_of(o).start())

        def end():
            def fn(o):
                out_of(o).wait_send()
                remote(buf.at[4 + o], buf.at[4 + o], w4_send.at[4 + o], w4_recv.at[kind // CYCLES, 4 + o],
                       place(p)).wait_recv()
            each(fn)

        return begin, end

    zpad = jnp.zeros((PAD, n0), f32)
    for m in range(3):
        def zero0(x, m=m):
            v0[m, x, 0:PAD, :] = zpad
            v0[m, x, PAD + zall : 2 * PAD + zall, :] = zpad
        loop(0, r0 + 4, zero0)

        def zero1(x, m=m):
            v1[m, x, 0:PAD, :] = zpad[:, :n1]
            v1[m, x, PAD + zall : 2 * PAD + zall, :] = zpad[:, :n1]
        loop(0, r1 + 4, zero1)

    tile0 = jnp.zeros((zall, 128), f32)
    plane0 = jnp.zeros((zall, n0), f32)

    def blank(lo0, x0, lo1, b):
        for q in range(2):
            for m in range(3):
                v0[m, lo0 + q, PAD : PAD + zall, :] = plane0
            v1[1, lo1 + q, PAD : PAD + zall, :] = tile0
            g1[lo1 + q] = tile0
            d1[lo1 + q] = tile0
            w1[lo1 + q] = tile0
        d0[x0] = plane0
        w0[x0] = plane0
        for k in range(CYCLES):
            gx[k, b] = tile0
            cx[k, b] = tile0
            ex[k, b] = tile0
        dx[b] = tile0

    @pl.when(first)
    def _():
        blank(0, 0, 0, 0)

    @pl.when(last)
    def _():
        blank(r0 + 2, r0 + 1, r1 + 2, 2)

    for k in range(CYCLES + 1):
        for q in range(8):
            @pl.when(jnp.logical_or(2 * chip - 3 + q < 0, 2 * chip - 3 + q >= nd))
            def _(q=q, k=k):
                win3[k, q] = jnp.zeros((n3 * zall // 128, 128), f32)
        for o in offs4:
            @pl.when(jnp.logical_or(chip + o < 0, chip + o >= nd // 2))
            def _(o=o, k=k):
                win4[k, 4 + o] = jnp.zeros((n4 * zall // 128, 128), f32)
    for q in range(2):
        v3[q, 0] = tile0
        v3[q, 3] = tile0
        v4[q, 0] = tile0
        v4[q, 3] = tile0
    v4[1, 2] = tile0
    acc[...] = jnp.zeros_like(acc)

    lane = lax.broadcasted_iota(jnp.int32, (zall, 128), 1)
    rows = lax.broadcasted_iota(jnp.int32, (zall, 128), 0)

    for t in range(3):
        good = [p > 0, None, p < nd - 1][t]
        one = jnp.ones((zall, 128), f32)
        mask[t] = one if good is None else one * good.astype(f32)
    for t in range(2):
        row = 2 * chip - 3 + 4 * t + lane // n3
        mask[3 + t] = jnp.where((row >= 0) & (row < nd), 1.0, 0.0)
        row = chip - 4 + 8 * t + lane // n4
        mask[5 + t] = jnp.where((row >= 0) & (row < nd // 2) & (row < chip + 5), 1.0, 0.0)

    def pack(rep, width):
        k = 128 // width
        zb = zall // k
        part = lane[:zb]
        got = rep[0:zb]
        for j in range(1, k):
            got = jnp.where(part // width == j, rep[zb * j : zb * (j + 1)], got)
        return got

    def unpack(slots, width):
        k = 128 // width
        zb = zall // k
        part = lane[:zb] // width
        parts = []
        for j in range(k):
            got = jnp.zeros((zb, 128), f32)
            for s, x in enumerate(slots):
                turn = (width * (s - j)) % 128
                x = x if turn == 0 else pltpu.roll(x, turn, 1)
                got = jnp.where(part == s, x, got)
            parts.append(got)
        return parts

    def unpack3(kind, dest, add=None):
        for t in range(2):
            slots = [win3[kind, 4 * t + k] for k in range(4)]
            zb = zall // 4
            for j, x in enumerate(unpack(slots, n3)):
                if add is not None:
                    x = x + add(j * zb, zb)
                dest[t, j * zb : (j + 1) * zb] = x

    def unpack4(kind, dest, add=None):
        for t in range(2):
            slots = [win4[kind, r] for r in range(8 * t, min(8 * t + 8, 9))]
            zb = zall // 8
            for j, x in enumerate(unpack(slots, n4)):
                if add is not None:
                    x = x + add(j * zb, zb)
                dest[t, j * zb : (j + 1) * zb] = x

    rawr = raw_r.reshape(zall * r0, n0)
    raws = raw_s.reshape(zall * r0, n0)
    staged = stage.reshape(zall * r0, n0)

    def unfold(raw, j):
        at = pl.ds(pl.multiple_of(PAD * r0 * j, PAD * r0), PAD * r0)
        for t in range(nt0):
            turn[t, at, :] = raw[at, 128 * t : 128 * (t + 1)]
    raw_r[pl.ds(depth * me, depth)] = reaction[:, pl.ds(r0 * p, r0), :]
    raw_s[pl.ds(depth * me, depth)] = source[:, pl.ds(r0 * p, r0), :]
    vrecv[me] = vsend[...]
    group = PAD // depth

    def each_rows(landed, body):
        def step(i):
            j = (me // group + i) % (zall // PAD)
            for k in range(group if landed is not None else 0):
                s = group * j + k

                @pl.when(s != me)
                def _():
                    landed(s)
            body(j)
        loop(0, zall // PAD, step)

    landed_v(None)
    for s in range(nd):
        lines[depth * s : depth * (s + 1), :] = vrecv[s]

    def take_r(j):
        z = pl.multiple_of(PAD * j, PAD)
        unfold(rawr, j)
        for x in range(r0):
            for t in range(nt0):
                d0[x + 1, pl.ds(z, PAD), 128 * t : 128 * (t + 1)] = turn[
                    t, pl.ds(PAD * r0 * j + x, PAD, stride=r0), :]

    landed_r(None)
    each_rows(None, take_r)

    def shrink_r(i):
        for r in range(0, zall, CROWS):
            at = pl.ds(r, CROWS)
            a, b = d0[2 * i + 1, at, :], d0[2 * i + 2, at, :]
            got = dot_parts(a + b, downy[...], 3)
            vert = lines[at, :]
            base = 2.0 * vert + 4.0 * h[1]
            w1[i + 2, at, :] = got
            d = base + got
            d1[i + 2, at, :] = d
            base = jnp.concatenate([2.0 * vert + 4.0 * h[0]] * nt0, axis=1)
            for k, x in ((1, a), (2, b)):
                x = base + x
                d0[2 * i + k, at, :] = x
                w0[2 * i + k, at, :] = DAMPING / x

    loop(0, r1, shrink_r)
    begin_d0, end_d0 = halo_d0()
    begin_d0()
    begin_d1, end_d1 = planes1(d1, 6)
    begin_d1()
    rx2 = dot_parts(jnp.concatenate([w1[2] + w1[3], w1[4] + w1[5]], axis=1), downy[...], 3)
    dx[1] = rx2
    begin_dx, end_dx = blocks(dx, 7)
    begin_dx()
    rx3 = dot_parts(rx2, down3[...], 3)
    win3[CYCLES, 3 + par] = pack(rx3, n3)
    begin_w3, end_w3 = window3(CYCLES)
    begin_w3()
    begin_w4, end_w4 = window4(CYCLES)
    loop(2, r1 + 2, lambda x: w1.__setitem__(x, DAMPING / d1[x]))

    def take_s(j):
        z = pl.multiple_of(PAD * j, PAD)
        unfold(raws, j)
        for x in range(r0):
            for t in range(nt0):
                cut = slice(128 * t, 128 * (t + 1))
                got = turn[t, pl.ds(PAD * r0 * j + x, PAD, stride=r0), :]
                g0[x + 1, pl.ds(z, PAD), cut] = got
                v0[0, x + 2, pl.ds(z + PAD, PAD), cut] = w0[x + 1, pl.ds(z, PAD), cut] * got

    each_rows(landed_s, take_s)

    ns = (zall - 1).bit_length()

    def factors(f):
        vert = lines[...]
        a = jnp.where(rows == 0, 0.0, -vert)
        c = jnp.where(rows == zall - 1, 0.0, -vert)
        b = diag[f]
        for k in range(ns):
            s = 1 << k
            inv = 1.0 / b
            alpha = -a * pltpu.roll(inv, s, 0)
            gamma = -c * pltpu.roll(inv, zall - s, 0)
            b = b + alpha * pltpu.roll(c, s, 0) + gamma * pltpu.roll(a, zall - s, 0)
            a = alpha * pltpu.roll(a, s, 0)
            c = gamma * pltpu.roll(c, zall - s, 0)
            fac[f, 2 * k] = alpha
            fac[f, 2 * k + 1] = gamma
        fac[f, 2 * ns] = mask[f] / b

    def solve(f, right):
        for k in range(ns):
            s = 1 << k
            right = (
                right
                + fac[f, 2 * k] * pltpu.roll(right, s, 0)
                + fac[f, 2 * k + 1] * pltpu.roll(right, zall - s, 0)
            )
        return right * fac[f, 2 * ns]

    def near(v, q, b, width):
        t = v[q, b]
        below = pltpu.roll(jnp.where(lane >= 128 - width, v[q, b - 1], t), width, 1)
        above = pltpu.roll(jnp.where(lane < width, v[q, b + 1], t), 128 - width, 1)
        inrow = lane % width
        left = jnp.where(inrow == 0, 0.0, pltpu.roll(t, 1, 1))
        right = jnp.where(inrow == width - 1, 0.0, pltpu.roll(t, 127, 1))
        return (below + above) + (left + right)

    edge = lax.broadcasted_iota(jnp.int32, (CROWS, 128), 1)
    level0 = (v0, g0, w0, d0, nt0, h[0], 1)
    level1 = (v1, g1, w1, d1, 1, h[1], 2)

    def stencil(level, m, x, r):
        v, g, w, d, nt, weight, go = level
        centre, turn_r, turn_l = [], [], []
        for t in range(nt):
            cut = slice(128 * t, 128 * (t + 1))
            c = v[m, x + 2, PAD + r : PAD + r + CROWS, cut]
            centre.append(c)
            turn_r.append(pltpu.roll(c, 1, 1))
            turn_l.append(pltpu.roll(c, 127, 1))
        vert = lines[r : r + CROWS, :]
        got = []
        for t in range(nt):
            cut = slice(128 * t, 128 * (t + 1))
            left = jnp.where(edge == 0, turn_r[t - 1] if t else 0.0, turn_r[t])
            right = jnp.where(edge == 127, turn_l[t + 1] if t + 1 < nt else 0.0, turn_l[t])
            side = (v[m, x + 1, PAD + r : PAD + r + CROWS, cut] + v[m, x + 3, PAD + r : PAD + r + CROWS, cut]) + (left + right)
            if weight != 1.0:
                side = weight * side
            ends = v[m, x + 2, PAD + r - 1 : PAD + r - 1 + CROWS, cut] + v[m, x + 2, PAD + r + 1 : PAD + r + 1 + CROWS, cut]
            got.append(g[x + go, r : r + CROWS, cut] + side + vert * ends)
        return centre, got

    def sweep_plane(level, m, q, x, record=None, put=None):
        v, g, w, d, nt, weight, go = level
        for lo in range(0, zall, GROUP * CROWS):
            new = []
            for r in range(lo, lo + GROUP * CROWS, CROWS):
                centre, got = stencil(level, m, x, r)
                for t in range(nt):
                    cut = slice(128 * t, 128 * (t + 1))
                    wt = w[x + go, r : r + CROWS, cut]
                    if record is None:
                        value = (1.0 - DAMPING) * centre[t] + wt * got[t]
                    else:
                        res = got[t] - d[x + go, r : r + CROWS, cut] * centre[t]
                        value = centre[t] + wt * res
                        acc[record] += (res * res).reshape(CROWS // 8, 8, 128).sum(axis=0)
                    new.append((r, t, value))
            for r, t, value in new:
                v[q, x + 2, PAD + r : PAD + r + CROWS, 128 * t : 128 * (t + 1)] = value
                if put is not None:
                    for e in range(0, CROWS, 8):
                        put(x, r + e, t, value[e : e + 8])

    def residual(level, m, x, r):
        v, g, w, d, nt, weight, go = level
        centre, got = stencil(level, m, x, r)
        res = [
            got[t] - d[x + go, r : r + CROWS, 128 * t : 128 * (t + 1)] * centre[t] for t in range(nt)]
        return res

    def sweeps(level, m, q, xs, record=None, put=None):
        lo, hi, fn = xs
        loop(lo, hi, lambda i: sweep_plane(level, m, q, fn(i), record, put))

    def restrict0(m, lo, hi, fn):
        def body(i):
            i = fn(i)
            for r in range(0, zall, CROWS):
                a = residual(level0, m, 2 * i, r)
                b = residual(level0, m, 2 * i + 1, r)
                both = jnp.concatenate([s + t for s, t in zip(a, b)], axis=1)
                g1[i + 2, r : r + CROWS, :] = dot_parts(both, downy[...])
        loop(lo, hi, body)

    def same(i):
        return i

    def pair0(m, q, then, record=None, hook=None, put=None, restrict=False, fix=None):
        if fix is None:
            end = planes0(m, 2)[1]
        else:
            end = rows1()[1]
            far0(fix)[1]()
            correct0(fix, m, 0, r1, same)
        if hook is not None:
            hook[0]()
        sweeps(level0, m, 1, (1, r0 - 1, same), record)
        if restrict:
            restrict0(1, 1, r1 - 1, same)
            row1(3, 1)[0]()
        else:
            sweeps(level0, 1, q, (2, r0 - 2, same), None, put)
        end()
        if hook is not None:
            hook[1]()
        for side in range(2):
            if fix is not None:
                correct0(fix, m, 0, 1, lambda i: r1 if side else -1)
            sweep_plane(level0, m, 1, r0 if side else -1)
            sweep_plane(level0, m, 1, r0 - 1 if side else 0, record)
            if restrict:
                restrict0(1, 0, 1, lambda i: r1 - 1 if side else 0)
            else:
                for k in range(2):
                    sweep_plane(level0, 1, q, r0 - 2 + k if side else k, None, put)
            then((side,))

    def halo_factors():
        end_dx()
        for t in range(3):
            diag[t] = 2.0 * lines[...] + 4.0 * h[2] + dx[t]
        loop(0, 3, factors)
        for k in range(2 * ns + 1):
            fac[7, k] = jnp.where(lane >= n2, fac[0, k], fac[2, k])
        end_w3()
        unpack3(CYCLES, g3)
        win4[CYCLES, 4] = pack(
            dot_parts(g3[0], down4[0], 3) + dot_parts(g3[1], down4[1], 3), n4)
        begin_w4()

    def window_factors():
        def add(level):
            return lambda r, n: 2.0 * lines[r : r + n, :] + 4.0 * h[level]
        for t in range(2):
            diag[3 + t] = 2.0 * lines[...] + 4.0 * h[3] + g3[t]
        loop(3, 5, factors)
        end_w4()
        unpack4(CYCLES, diag.at[pl.ds(5, 2)], add(4))
        loop(5, 7, factors)

    def halo_level0():
        end_d0()
        for x, inside in ((0, jnp.logical_not(first)), (r0 + 1, jnp.logical_not(last))):
            @pl.when(inside)
            def _(x=x):
                w0[x] = DAMPING / d0[x]
            g0[x] = v0[0, x + 1, PAD : PAD + zall, :] * d0[x] * (1.0 / DAMPING)

    def halo_level1():
        end_d1()
        for x, inside in ((0, jnp.logical_not(first)), (r1 + 2, jnp.logical_not(last))):
            @pl.when(inside)
            def _(x=x):
                for q in range(2):
                    w1[x + q] = DAMPING / d1[x + q]

    def coarse(cycle, m):
        end = row1(10, 0)[1]
        far0(m)[0]()
        if cycle == 0:
            window_factors()
        loop(2, r1 + 2, lambda x: v1.__setitem__((0, x, pl.ds(PAD, zall)), w1[x] * g1[x]))
        row1(3, 1)[1]()
        end()
        if cycle == 0:
            halo_level1()
        for x in (0, 1, r1 + 2, r1 + 3):
            v1[0, x, PAD : PAD + zall] = w1[x] * g1[x]
        for x in range(-1, r1 + 1):
            sweep_plane(level1, 0, 1, x)

        pairs = []
        for i in range(r1 // 2):
            cuts = []
            for r in range(0, zall, CROWS):
                a = residual(level1, 1, 2 * i, r)[0]
                b = residual(level1, 1, 2 * i + 1, r)[0]
                cuts.append(a + b)
            pairs.append(jnp.concatenate(cuts, axis=0))
        gx[cycle, 1] = dot_parts(jnp.concatenate(pairs, axis=1), downy[...])
        e2 = lines2(cycle, far1()[0])
        ex[cycle, 1] = e2
        begin, end = blocks(ex.at[cycle], 4)
        begin()

        for i in range(r1 // 2):
            e = dot_parts(e2, up2[i])
            for x in (2 * i, 2 * i + 1):
                v1[2, x + 2, PAD : PAD + zall] = v1[1, x + 2, PAD : PAD + zall] + e
        far1()[1]()
        for x in range(1, r1 - 1):
            sweep_plane(level1, 2, 1, x)
        end()
        for side in range(2):
            e = dot_parts(ex[cycle, 2], up2[0]) if side else dot_parts(ex[cycle, 0], up2[r1 // 2 - 1])
            for x in (r1 + 2, r1 + 3) if side else (0, 1):
                v1[2, x, PAD : PAD + zall] = v1[1, x, PAD : PAD + zall] + e
            for x in (r1 - 1, r1) if side else (-1, 0):
                sweep_plane(level1, 2, 1, x)
            sweep_plane(level1, 1, 0, r1 - 1 if side else 0)
            rows1()[0]((side,))
        for x in range(1, r1 - 1):
            sweep_plane(level1, 1, 0, x)

    def lines_sweep(v, q, s, lo, hi, right, f, weight, width):
        for b in range(lo, hi):
            v[s, b] = solve(f + b - 1, right[b - 1] + weight * near(v, q, b, width))

    def line_residual(v, q, b, right, f, weight, width):
        values = v[q, b]
        before = jnp.where(rows == 0, 0.0, pltpu.roll(values, 1, 0))
        after = jnp.where(rows == zall - 1, 0.0, pltpu.roll(values, zall - 1, 0))
        return right[b - 1] + weight * near(v, q, b, width) + lines[...] * (before + after) - diag[f + b - 1] * values

    def beside(t):
        inrow = lane % n2
        return jnp.where(inrow == 0, 0.0, pltpu.roll(t, 1, 1)) + jnp.where(inrow == n2 - 1, 0.0, pltpu.roll(t, 127, 1))

    def pair2(left, own, right, right_own, right_rim):
        upper = lane >= n2
        rim = jnp.where(upper, left, right)
        far = jnp.where(upper, right, left)
        new = solve(1, right_own + h[2] * (beside(own) + pltpu.roll(own + rim, n2, 1)))
        return new, solve(7, right_rim + h[2] * (beside(rim) + pltpu.roll(own + far, n2, 1)))

    def lines2(cycle, after):
        right = gx.at[cycle]
        begin, end = blocks(right, 8)
        begin()
        after()
        v2[1] = solve(1, right[1])
        end()
        for b in (0, 2):
            v2[b] = solve(b, right[b])
        right_rim = jnp.where(lane >= n2, right[0], right[2])
        v2[3], v2[4] = pair2(v2[0], v2[1], v2[2], right[1], right_rim)
        own = v2[3]
        before = jnp.where(rows == 0, 0.0, pltpu.roll(own, 1, 0))
        after = jnp.where(rows == zall - 1, 0.0, pltpu.roll(own, zall - 1, 0))
        around = beside(own) + pltpu.roll(own + v2[4], n2, 1)
        res = right[1] + h[2] * around + lines[...] * (before + after) - diag[1] * own
        win3[cycle, 3 + par] = pack(dot_parts(res, down3[...]), n3)
        e3 = lines3(cycle)
        cx[cycle, 1] = v2[3] + dot_parts(e3, up3[par])
        begin, end = blocks(cx.at[cycle], 9)
        begin()
        end()
        v2[0], v2[1] = pair2(cx[cycle, 0], cx[cycle, 1], cx[cycle, 2], right[1], jnp.where(lane >= n2, right[0], right[2]))
        return solve(1, right[1] + h[2] * (beside(v2[0]) + pltpu.roll(v2[0] + v2[1], n2, 1)))

    def lines3(cycle):
        begin, end = window3(cycle)
        begin()
        end()
        unpack3(cycle, g3)
        for b in range(1, 3):
            v3[0, b] = solve(3 + b - 1, g3[b - 1])
        lines_sweep(v3, 0, 1, 1, 3, g3, 3, h[3], n3)
        both = None
        for t in range(2):
            part = dot_parts(line_residual(v3, 1, t + 1, g3, 3, h[3], n3), down4[t])
            both = part if both is None else both + part
        win4[cycle, 4] = pack(both, n4)
        e4 = lines4(cycle)
        for t in range(2):
            v3[0, t + 1] = v3[1, t + 1] + dot_parts(e4, up4[t])
        lines_sweep(v3, 0, 1, 1, 3, g3, 3, h[3], n3)
        return solve(3 + par, g3[par] + h[3] * near(v3, 1, 1 + par, n3))

    def lines4(cycle):
        begin, end = window4(cycle)
        begin()
        end()
        unpack4(cycle, g4)
        for b in range(1, 3):
            v4[0, b] = solve(5 + b - 1, g4[b - 1])
        q = 0
        for k in range(1, COARSE - 1):
            v4[1 - q, 1] = solve(5, g4[0] + h[4] * near(v4, q, 1, n4))
            q = 1 - q
        return solve(5, g4[0] + h[4] * near(v4, q, 1, n4))

    def correct0(m, q, lo, hi, fn):
        def body(i):
            i = fn(i)
            for r in range(0, zall, 2 * CROWS):
                cut = slice(PAD + r, PAD + r + 2 * CROWS)
                e = dot_parts(v1[0, i + 2, cut, :], upy[...])
                for x in (2 * i + 2, 2 * i + 3):
                    v0[q, x, cut, :] = v0[m, x, cut, :] + e
        loop(lo, hi, body)

    def put(x, z, t, value):
        turn[t, pl.ds(z * r0 + x, 8, stride=r0), :] = value

    def fold(j):
        at = pl.ds(pl.multiple_of(PAD * r0 * j, PAD * r0), PAD * r0)
        for t in range(nt0):
            staged[at, 128 * t : 128 * (t + 1)] = turn[t, at, :]

    planes0(0, 2)[0]()
    pair0(0, 1, row1(10, 0)[0], hook=(halo_factors, halo_level0), restrict=True)
    coarse(0, 1)
    pair0(2, 0, planes0(0, 2)[0], fix=1)
    pair0(0, 2, planes0(2, 1)[0], record=0)
    end = planes0(2, 1)[1]
    restrict0(2, 1, r1 - 1, same)
    row1(3, 1)[0]()
    end()
    for side in range(2):
        restrict0(2, 0, 1, lambda i: r1 - 1 if side else 0)
        row1(10, 0)[0]((side,))
    coarse(1, 2)
    pair0(0, 2, norm0()[0], put=put, fix=2)
    loop(0, zall // PAD, fold)
    end = norm0()[1]
    start_o(1, nd * 7 // 8)
    keep = pltpu.make_async_copy(zrows(stage, me), piece(out, p), load.at[2])
    keep.start()

    def last_norm(x):
        for r in range(0, zall, CROWS):
            for res in residual(level0, 2, x, r):
                acc[CYCLES - 1] += (res * res).reshape(CROWS // 8, 8, 128).sum(axis=0)

    loop(1, r0 - 1, last_norm)
    end()
    for x, y in ((1, 0), (r0 + 2, r0 + 3)):
        v0[2, x, PAD : PAD + zall, :] = v0[1, y, PAD : PAD + zall, :]
    loop(0, 2, lambda i: last_norm(i * (r0 - 1)))
    ridx = lax.broadcasted_iota(jnp.int32, (8, 128), 0)
    part = jnp.zeros((8, 128), f32)
    for k in range(CYCLES):
        part = jnp.where(ridx == k, jnp.sum(acc[k]), part)
    nsend[...] = part
    start_n()
    start_o(nd * 7 // 8, nd)
    total = part
    done_v()
    done_r()
    done_s()

    def finish(s):
        @pl.when(s != me)
        def _():
            landed_o(s)
    loop(0, nd, finish)
    landed_n(None)
    nrecv[me] = part
    total = jnp.sum(nrecv[...], axis=0)
    for k in range(CYCLES):
        norms[k] = total[k, 0] * (1.0 / (zall * n0 * n0))
    keep.wait()
    done_o()
    done_n()


def chain_shards(gz, gy, source, vertical, reaction):
    depth, n0 = source.shape[0], source.shape[1]
    nd = gz * gy
    zall = nd * depth
    n1, n2, n3, n4 = n0 // 2, n0 // 4, n0 // 8, n0 // 16
    r0, r1 = n0 // nd, n1 // nd
    f32 = jnp.float32
    bf16 = jnp.bfloat16

    sm = pl.BlockSpec(memory_space=pltpu.SMEM)
    ns = (zall - 1).bit_length()
    dma = pltpu.SemaphoreType.DMA
    solution, norms = pl.pallas_call(
        functools.partial(chain_kernel, (gz, gy, depth)),
        out_shape=(
            pltpu.VMEM(source.shape, f32),
            pltpu.SMEM((CYCLES,), f32),
        ),
        in_specs=[pl.BlockSpec(memory_space=pltpu.HBM)] * 2 + [sm],
        out_specs=(pl.BlockSpec(memory_space=pltpu.VMEM), sm),
        scratch_shapes=[
            pltpu.VMEM(source.shape, f32),
            pltpu.VMEM(source.shape, f32),
            pltpu.VMEM((n0, n1), bf16),
            pltpu.VMEM((n1, n0), bf16),
            pltpu.VMEM((r1 // 2, 128, n1), bf16),
            pltpu.VMEM((128, 128), bf16),
            pltpu.VMEM((2, 128, 128), bf16),
            pltpu.VMEM((2, 128, 128), bf16),
            pltpu.VMEM((2, 128, 128), bf16),
            pltpu.SemaphoreType.DMA((3,)),
            pltpu.VMEM((3, r0 + 4, zall + 2 * PAD, n0), f32),
            pltpu.VMEM((r0 + 2, zall, n0), f32),
            pltpu.VMEM((r0 + 2, zall, n0), f32),
            pltpu.VMEM((r0 + 2, zall, n0), f32),
            pltpu.VMEM((3, r1 + 4, zall + 2 * PAD, n1), f32),
            pltpu.VMEM((r1 + 4, zall, n1), f32),
            pltpu.VMEM((r1 + 4, zall, n1), f32),
            pltpu.VMEM((r1 + 4, zall, n1), f32),
            pltpu.VMEM((zall, r0, n0), f32),
            pltpu.VMEM((zall, r0, n0), f32),
            pltpu.VMEM((zall, r0, n0), f32),
            pltpu.VMEM((n0 // 128, zall * r0, 128), f32),
            pltpu.VMEM((zall, 128), f32),
            pltpu.VMEM((depth, 128), f32),
            pltpu.VMEM((nd, depth, 128), f32),
            pltpu.VMEM((CYCLES, 3, zall, 128), f32),
            pltpu.VMEM((CYCLES, 3, zall, 128), f32),
            pltpu.VMEM((CYCLES, 3, zall, 128), f32),
            pltpu.VMEM((3, zall, 128), f32),
            pltpu.VMEM((CYCLES + 1, 8, n3 * zall // 128, 128), f32),
            pltpu.VMEM((CYCLES + 1, 9, n4 * zall // 128, 128), f32),
            pltpu.VMEM((5, zall, 128), f32),
            pltpu.VMEM((2, 4, zall, 128), f32),
            pltpu.VMEM((2, 4, zall, 128), f32),
            pltpu.VMEM((2, zall, 128), f32),
            pltpu.VMEM((2, zall, 128), f32),
            pltpu.VMEM((7, zall, 128), f32),
            pltpu.VMEM((8, 2 * ns + 1, zall, 128), f32),
            pltpu.VMEM((7, zall, 128), f32),
            pltpu.VMEM((CYCLES, 8, 128), f32),
            pltpu.VMEM((8, 128), f32),
            pltpu.VMEM((nd, 8, 128), f32),
            dma((5,)),
            dma((5,)),
            dma((nd,)),
            dma((14, 2)),
            dma((14, 2)),
            dma((10,)),
            dma((2, 8)),
            dma((9,)),
            dma((2, 9)),
        ],
        compiler_params=pltpu.CompilerParams(
            has_side_effects=True, vmem_limit_bytes=VMEM_LIMIT, collective_id=0
        ),
    )(source, reaction, vertical)
    return solution, norms


def shards_of(gz, gy, source, vertical, reaction):
    depth, n0 = source.shape[0], source.shape[1]
    nd = gz * gy
    fits = (
        gz % 2 == 0 and n0 % (8 * nd) == 0 and n0 // nd == 8 and n0 % 256 == 0 and n0 // 4 * 2 == 128
        and PAD % depth == 0 and nd * depth % 128 == 0 and (LEVELS, SWITCH, SWEEPS, COARSE, CYCLES) == (5, 2, 2, 4, 2)
    )
    return (chain_shards if fits else shards)(gz, gy, source, vertical, reaction)


def solution(mesh):
    return jax.shard_map(
        functools.partial(shards_of, mesh.shape["gz"], mesh.shape["gy"]),
        mesh=mesh,
        in_specs=(P(("gz", "gy"), None, None), P(("gz", "gy")), P(("gz", "gy"), None, None)),
        out_specs=(P(("gz", "gy"), None, None), P()),
        check_vma=False,
    )
```
